256 devices in a mesh: rows: 256 (over z, y, x, core).
Axes of the slice: x: 4, y: 4, z: 8, core: 2. Of those that a mesh axis runs over, the one named last changes fastest.
Arguments:
- wave_fn: float32 [512, 3, 3, 512], P('rows')
- left_env: bfloat16 [32, 512, 512], P(None, 'rows')
- op_pair: bfloat16 [32, 9, 9], replicated
- right_env: bfloat16 [32, 512, 512], replicated
Outputs:
- output 1: float32 [7, 512, 3, 3, 512], P(None, 'rows')
- output 2: float32 [6], replicated
- output 3: float32 [6], replicated
All inputs are finite; a program needn't handle non-finite values.
Results may differ from the reference program's by a relative error of at most 0.0127079.
Values are sent between devices in bfloat16 or wider.
A program may use at most 768 MiB of HBM per device.

```python
import jax
import jax.numpy as jnp
from jax import lax

BOND_DIM = 512
PHYS_DIM = 3
NUM_TERMS = 32
NUM_STEPS = 6


def sym_noise(rng_key, num_mats, mat_size):
    raw_draw = jax.random.normal(rng_key, (num_mats, mat_size, mat_size), jnp.float32)
    return (raw_draw + jnp.swapaxes(raw_draw, 1, 2)) * (0.5 ** 0.5) * mat_size ** -0.5


def setup_inputs(seed: int = 0) -> dict:
    key_list = jax.random.split(jax.random.key(seed), 7)
    pair_dim = PHYS_DIM * PHYS_DIM
    shift_left = jax.random.uniform(key_list[0], (NUM_TERMS, 1, 1), jnp.float32, 0.3, 0.9)
    shift_pair = jax.random.uniform(key_list[1], (NUM_TERMS, 1, 1), jnp.float32, 0.3, 0.9)
    shift_right = jax.random.uniform(key_list[2], (NUM_TERMS, 1, 1), jnp.float32, 0.3, 0.9)
    left_env = sym_noise(key_list[3], NUM_TERMS, BOND_DIM) + shift_left * jnp.eye(BOND_DIM, dtype=jnp.float32)
    op_pair = (sym_noise(key_list[4], NUM_TERMS, pair_dim) + shift_pair * jnp.eye(pair_dim, dtype=jnp.float32)) * NUM_TERMS ** -0.5
    right_env = sym_noise(key_list[5], NUM_TERMS, BOND_DIM) + shift_right * jnp.eye(BOND_DIM, dtype=jnp.float32)
    wave_fn = jax.random.normal(key_list[6], (BOND_DIM, PHYS_DIM, PHYS_DIM, BOND_DIM), jnp.float32)
    return {"wave_fn": wave_fn, "left_env": left_env.astype(jnp.bfloat16), "op_pair": op_pair.astype(jnp.bfloat16), "right_env": right_env.astype(jnp.bfloat16)}


def matvec(vec_in, left_env, op_pair, right_env):
    pair_dim = PHYS_DIM * PHYS_DIM
    flat_in = vec_in.astype(jnp.bfloat16).reshape(BOND_DIM, pair_dim * BOND_DIM)

    def add_term(acc_sum, term_ops):
        left_k, pair_k, right_k = term_ops
        left_out = jnp.dot(left_k, flat_in, preferred_element_type=jnp.float32).astype(jnp.bfloat16)
        left_out = left_out.reshape(BOND_DIM, pair_dim, BOND_DIM)
        mid_out = jnp.einsum("qr,arc->aqc", pair_k.astype(jnp.float32), left_out.astype(jnp.float32)).astype(jnp.bfloat16)
        part_out = jnp.dot(mid_out.reshape(BOND_DIM * pair_dim, BOND_DIM), right_k.T, preferred_element_type=jnp.float32)
        return acc_sum + part_out, None

    start_sum = jnp.zeros((BOND_DIM * pair_dim, BOND_DIM), jnp.float32)
    sigma_all = lax.scan(add_term, start_sum, (left_env, op_pair, right_env))[0]
    return sigma_all.reshape(BOND_DIM, PHYS_DIM, PHYS_DIM, BOND_DIM)


def reference(wave_fn, left_env, op_pair, right_env):
    vec_count = BOND_DIM * BOND_DIM * PHYS_DIM * PHYS_DIM
    first_vec = wave_fn / jnp.sqrt(jnp.sum(wave_fn * wave_fn) / vec_count)

    def lanczos_step(carry_in, unused):
        prev_vec, cur_vec, beta_prev = carry_in
        sigma_all = matvec(cur_vec, left_env, op_pair, right_env)
        alpha_val = jnp.sum(sigma_all * cur_vec) / vec_count
        resid_vec = sigma_all - alpha_val * cur_vec - beta_prev * prev_vec
        beta_val = jnp.sqrt(jnp.sum(resid_vec * resid_vec) / vec_count)
        next_vec = resid_vec / beta_val
        return (cur_vec, next_vec, beta_val), (next_vec, alpha_val, beta_val)

    start_carry = (jnp.zeros_like(first_vec), first_vec, jnp.zeros((), jnp.float32))
    later_vecs, alphas, betas = lax.scan(lanczos_step, start_carry, None, length=NUM_STEPS)[1]
    return jnp.concatenate([first_vec[None], later_vecs], axis=0), alphas, betas
```

```python
import functools

import jax
import jax.numpy as jnp
from jax import lax
from jax.experimental import pallas as pl
from jax.experimental.pallas import tpu as pltpu
from jax.sharding import PartitionSpec as P

NUM_STEPS = 6
ROW = "rows"
NY, NX, NC = 4, 4, 2
NS = NY * NX
PAIR = 9
BW = 32
BLK = 72
MESH = pl.DeviceIdType.MESH
F32, BF16 = jnp.float32, jnp.bfloat16
OFFSETS = sorted(
    [(dy, dx) for dy in range(NY) for dx in range(NX) if (dy, dx) != (0, 0)],
    key=lambda o: (-(min(o[0], NY - o[0]) + min(o[1], NX - o[1])), o),
)


def place():
    me = lax.axis_index(ROW)
    return me // (NS * NC), (me // (NX * NC)) % NY, (me // NC) % NX, me % NC


def device(z, y, x, core):
    return ((z * NY + y) * NX + x) * NC + core


def rcopy(src, dst, send_sem, recv_sem, dev):
    return pltpu.make_async_remote_copy(
        src_ref=src, dst_ref=dst, send_sem=send_sem, recv_sem=recv_sem, device_id=(dev,), device_id_type=MESH
    )


def enter(devs):
    barrier = pltpu.get_barrier_semaphore()
    for dev in devs:
        pl.semaphore_signal(barrier, inc=1, device_id=(dev,), device_id_type=MESH)
    pl.semaphore_wait(barrier, len(devs))


def plane_peers(z, y, x, core):
    out = []
    for dy, dx in OFFSETS:
        py, px = (y + dy) % NY, (x + dx) % NX
        out.append((py * NX + px, device(z, py, px, core)))
    return out


def head_kernel(psi_ref, left_ref, psi_out, left_out, p_ss, p_rs, l_ss, l_rs):
    z, y, x, core = place()
    j = y * NX + x
    peers = plane_peers(z, y, x, core)
    enter([dev for _, dev in peers])
    for pj, dev in peers:
        rcopy(psi_ref.at[pj], psi_out.at[j], p_ss.at[pj], p_rs.at[j], dev).start()
    for pj, dev in peers:
        rcopy(left_ref, left_out.at[j], l_ss.at[pj], l_rs.at[j], dev).start()
    psi_out[pl.ds(j, 1)] = psi_ref[pl.ds(j, 1)]
    left_out[pl.ds(j, 1)] = left_ref[...][None]
    for pj, dev in peers:
        rcopy(psi_ref.at[pj], psi_out.at[pj], p_ss.at[pj], p_rs.at[pj], dev).wait()
        rcopy(left_ref, left_out.at[pj], l_ss.at[pj], l_rs.at[pj], dev).wait()


def tail_kernel(vec_ref, vec_out, v_ss, v_rs):
    z, y, x, core = place()
    j = y * NX + x
    peers = plane_peers(z, y, x, core)
    enter([dev for _, dev in peers])
    for pj, dev in peers:
        rcopy(vec_ref.at[pj], vec_out.at[j], v_ss.at[pj], v_rs.at[j], dev).start()
    vec_out[pl.ds(j, 1)] = vec_ref[pl.ds(j, 1)]
    for pj, dev in peers:
        rcopy(vec_ref.at[pj], vec_out.at[pj], v_ss.at[pj], v_rs.at[pj], dev).wait()


def swap4(a, b, c, d):
    lane = lax.broadcasted_iota(jnp.int32, a.shape, 1)
    low = lane < 64
    even = (lane // 32) % 2 == 0
    a, c = jnp.where(low, a, pltpu.roll(c, 64, 1)), jnp.where(low, pltpu.roll(a, 64, 1), c)
    b, d = jnp.where(low, b, pltpu.roll(d, 64, 1)), jnp.where(low, pltpu.roll(b, 64, 1), d)
    a, b = jnp.where(even, a, pltpu.roll(b, 32, 1)), jnp.where(even, pltpu.roll(a, 96, 1), b)
    c, d = jnp.where(even, c, pltpu.roll(d, 32, 1)), jnp.where(even, pltpu.roll(c, 96, 1), d)
    return a, b, c, d


def fold(val):
    return jnp.sum(val.reshape(BLK // 8, 8, 128), axis=0)


def total(val):
    one = jnp.sum(jnp.sum(val, axis=0, keepdims=True), axis=1, keepdims=True)
    return jnp.broadcast_to(one, (1, 128))


def main_kernel(
    nz, count, psi_ref, lt_ref, r2_ref, wv_ref, vout_ref, ab_ref,
    gbuf, vb, ut, xt, y2, sbuf, rbuf, abuf, asend,
    g_ss, d_ss, g_rs, r_ss, r_rs, a_ss, a_rs,
):
    ng = nz * NC
    terms = lt_ref.shape[1] // BW
    z, y, x, core = place()
    i, j = core * nz + z, y * NX + x
    peers = plane_peers(z, y, x, core)
    mate = device(z, y, x, 1 - core)
    zs = [((z + dz) % nz, dz) for dz in sorted(range(1, nz), key=lambda dz: (min(dz, nz - dz), dz))]
    enter([dev for _, dev in peers] + [device(pz, y, x, core) for pz, _ in zs] + [mate])

    vb[...] = jnp.zeros_like(vb)
    gbuf[0, pl.ds(i, 1)] = psi_ref[...][None]

    def gather(par):
        own = gbuf.at[par, i]
        for pz, dz in reversed(zs):
            rcopy(own, own, g_ss.at[dz], g_rs.at[par, i], device(pz, y, x, core)).start()
        rcopy(own, own, g_ss.at[0], g_rs.at[par, i], mate).start()
        for pz, dz in zs:
            slot = core * nz + pz
            ref = gbuf.at[par, slot]
            rcopy(ref, ref, g_ss.at[dz], g_rs.at[par, slot], mate).wait_recv()
            rcopy(ref, ref, d_ss.at[dz], g_rs.at[par, slot], mate).start()
        for dz in range(nz):
            slot = (1 - core) * nz + (z + dz) % nz
            ref = gbuf.at[par, slot]
            rcopy(ref, ref, g_ss.at[0], g_rs.at[par, slot], mate).wait_recv()
        rcopy(own, own, g_ss.at[0], g_rs.at[par, i], mate).wait_send()
        for pz, dz in zs:
            ref = gbuf.at[par, core * nz + pz]
            rcopy(own, own, g_ss.at[dz], g_rs.at[par, i], mate).wait_send()
            rcopy(ref, ref, d_ss.at[dz], g_rs.at[par, i], mate).wait_send()

    def scalars(par, beta_prev):
        zero = jnp.zeros((8, 128), F32)

        def first(s, acc):
            w, v, vp = gbuf[par, s], vb[1 - par, s], vb[par, s]
            return (
                acc[0] + fold(w * v),
                acc[1] + fold((w - beta_prev * vp) * v),
                acc[2] + fold(v * v),
            )

        m, yv, nn = [total(val) for val in lax.fori_loop(0, ng, first, (zero, zero, zero))]
        some = nn > 0.0
        p = jnp.where(some, yv / jnp.where(some, nn, 1.0), 0.0)

        def second(s, acc):
            w, v, vp = gbuf[par, s], vb[1 - par, s], vb[par, s]
            e = w - p * v - beta_prev * vp
            return acc[0] + fold(e * e), acc[1] + fold(e * v)

        ee, ev = [total(val) for val in lax.fori_loop(0, ng, second, (zero, zero))]
        row = lax.broadcasted_iota(jnp.int32, (8, 128), 0)
        tile = jnp.where(row == 0, m, jnp.where(row == 1, p, jnp.where(row == 2, nn, jnp.where(row == 3, ee, ev))))
        asend[...] = tile
        for pj, dev in peers:
            rcopy(asend, abuf.at[j], a_ss.at[pj], a_rs.at[j], dev).start()
        abuf[pl.ds(j, 1)] = tile[None]
        for pj, dev in peers:
            rcopy(asend, abuf.at[pj], a_ss.at[pj], a_rs.at[pj], dev).wait()
        alpha = abuf[0, 0:1]
        for s in range(1, NS):
            alpha = alpha + abuf[s, 0:1]
        alpha = alpha / count
        square = jnp.zeros((1, 128), F32)
        for s in range(NS):
            off = abuf[s, 1:2] - alpha
            square = square + (abuf[s, 3:4] + 2.0 * (off * abuf[s, 4:5]) + (off * abuf[s, 2:3]) * off)
        return alpha, jnp.sqrt(square / count)

    def left_and_mix(par):
        for grp in range(ng // 4):
            lanes = slice(grp * 128, grp * 128 + 128)
            for t in range(2):
                outs = swap4(*[vb[par, grp * 4 + ii, t * 32 : t * 32 + 32] for ii in range(4)])
                for k in range(4):
                    q = 4 * t + k
                    ut[q * 32 : q * 32 + 32, lanes] = outs[k].astype(BF16)
            outs = swap4(*[vb[par, grp * 4 + ii, 64:72] for ii in range(4)])
            ut[256:272, lanes] = jnp.concatenate(outs[:2], axis=0).astype(BF16)
            ut[272:288, lanes] = jnp.concatenate(outs[2:], axis=0).astype(BF16)
        width = 256
        for part in range(terms * BW // width):
            cols = slice(part * width, part * width + width)
            xt[:, cols] = jnp.dot(ut[...], lt_ref[:, cols], preferred_element_type=F32)

        def mix(grp, carry):
            lanes = pl.ds(pl.multiple_of(grp * 128, 128), 128)
            xs = [xt[r * 32 : r * 32 + 32, lanes].astype(BF16).astype(F32) for r in range(PAIR)]

            def one(q):
                acc = wv_ref[q * PAIR : q * PAIR + 1, lanes] * xs[0]
                for r in range(1, PAIR):
                    acc = acc + wv_ref[q * PAIR + r : q * PAIR + r + 1, lanes] * xs[r]
                return acc

            rows = [pl.ds(pl.multiple_of(grp * 128 + k * 32, 32), 32) for k in range(4)]
            for t in range(2):
                outs = swap4(*[one(4 * t + k) for k in range(4)])
                for k in range(4):
                    y2[rows[k], t * 128 : t * 128 + 128] = outs[k].astype(BF16)
            last = one(8)
            for k in range(4):
                moved = last if k == 0 else pltpu.roll(last, 128 - 32 * k, 1)
                y2[rows[k], 256:384] = moved.astype(BF16)
            return carry

        lax.fori_loop(0, terms * BW // 128, mix, 0)

    def right_and_scatter(nxt):
        grp = lax.broadcasted_iota(jnp.int32, (8, 128), 1) // 32
        for dy in (2, 1, 3, 0):
            py = (y + dy) % NY
            part = jnp.dot(
                r2_ref[pl.ds(pl.multiple_of(py * 128, 128), 128), :], y2[...], preferred_element_type=F32
            )
            for px in range(NX):
                pj = py * NX + px
                rows = part[px * 32 : px * 32 + 32]
                packed = rows[0:8, 256:384]
                for t in range(1, 4):
                    packed = jnp.where(grp == t, pltpu.roll(rows[8 * t : 8 * t + 8, 256:384], 32 * t, 1), packed)
                sbuf[pj, 0:32] = rows[:, 0:128]
                sbuf[pj, 32:64] = rows[:, 128:256]
                sbuf[pj, 64:72] = packed
                send = rcopy(sbuf.at[pj], rbuf.at[j], r_ss.at[pj], r_rs.at[j], device(z, py, px, core))
                if dy:
                    send.start()
                else:

                    @pl.when(px != x)
                    def _():
                        send.start()

        rbuf[pl.ds(j, 1)] = sbuf[pl.ds(j, 1)]
        for pj, dev in reversed(peers):
            rcopy(sbuf.at[pj], rbuf.at[pj], r_ss.at[pj], r_rs.at[pj], dev).wait()
        w = rbuf[0]
        for s in range(1, NS):
            w = w + rbuf[s]
        gbuf[nxt, pl.ds(i, 1)] = w[None]

    def step(t, beta_prev):
        par = t % 2
        gather(par)
        alpha, beta = scalars(par, beta_prev)
        ab_ref[0, pl.ds(t, 1)] = alpha
        ab_ref[1, pl.ds(t, 1)] = beta

        def update(s, carry):
            w, v, vp = gbuf[par, s], vb[1 - par, s], vb[par, s]
            vb[par, pl.ds(s, 1)] = ((w - alpha * v - beta_prev * vp) / beta)[None]
            return carry

        lax.fori_loop(0, ng, update, 0)
        vout_ref[pl.ds(t, 1)] = vb[par, pl.ds(i, 1)]

        @pl.when(t < NUM_STEPS)
        def _():
            left_and_mix(par)
            right_and_scatter(1 - par)

        return jnp.where(t == 0, jnp.zeros_like(beta), beta)

    lax.fori_loop(0, NUM_STEPS + 1, step, jnp.zeros((1, 128), F32))


def vmem(n):
    return [pl.BlockSpec(memory_space=pltpu.VMEM)] * n


def dma(*shape):
    return pltpu.SemaphoreType.DMA(shape)


def solution(mesh):
    nz = mesh.shape[ROW] // (NS * NC)
    ng = nz * NC

    def local_run(wave_rows, left_rows, op_pair, right_env):
        terms, rows, left_dim = left_rows.shape
        right_dim = right_env.shape[1]
        count = left_dim * right_dim * PAIR
        j = (lax.axis_index(ROW) // NC) % NS

        psi = wave_rows.reshape(rows, PAIR, NS, BW).transpose(2, 0, 1, 3).reshape(NS, rows * PAIR * BW)
        psi = jnp.pad(psi, ((0, 0), (0, 1024 - psi.shape[1]))).reshape(NS, 8, 128)
        left = left_rows.reshape(terms, rows, nz, NS, NC, rows).transpose(0, 1, 4, 2, 3, 5).reshape(terms * rows, left_dim)
        psi, left = pl.pallas_call(
            head_kernel,
            out_shape=(jax.ShapeDtypeStruct((NS, 8, 128), F32), jax.ShapeDtypeStruct((NS, terms * rows, left_dim), BF16)),
            in_specs=vmem(2),
            out_specs=tuple(vmem(2)),
            scratch_shapes=[dma(NS), dma(NS), dma(NS), dma(NS)],
            compiler_params=pltpu.CompilerParams(collective_id=0, has_side_effects=True),
            name="head",
        )(psi, left)
        psi = psi.reshape(NS, 1024)[:, : rows * PAIR * BW].reshape(NS, rows, PAIR, BW)
        psi = psi.transpose(2, 3, 0, 1).reshape(PAIR, BW, BW)
        main = psi[:8].reshape(2, 4, BW, BW).transpose(0, 2, 1, 3).reshape(64, 128)
        last = psi[8].reshape(4, 8, BW).transpose(1, 0, 2).reshape(8, 128)
        psi = jnp.concatenate([main, last], axis=0)
        lt = left.reshape(NS, terms, rows, left_dim).transpose(3, 1, 0, 2).reshape(left_dim, terms * BW)
        r2 = lax.dynamic_slice_in_dim(right_env, j * BW, BW, axis=1)
        r2 = r2.transpose(2, 0, 1).reshape(right_dim, terms * BW)
        wv = jnp.repeat(op_pair.astype(F32).transpose(1, 2, 0).reshape(PAIR * PAIR, terms), BW, axis=1)

        vblk, ab = pl.pallas_call(
            functools.partial(main_kernel, nz, float(count)),
            out_shape=(jax.ShapeDtypeStruct((NUM_STEPS + 1, BLK, 128), F32), jax.ShapeDtypeStruct((2, 8, 128), F32)),
            in_specs=vmem(4),
            out_specs=tuple(vmem(2)),
            scratch_shapes=[
                pltpu.VMEM((2, ng, BLK, 128), F32),
                pltpu.VMEM((2, ng, BLK, 128), F32),
                pltpu.VMEM((PAIR * BW, left_dim), BF16),
                pltpu.VMEM((PAIR * BW, terms * BW), F32),
                pltpu.VMEM((terms * BW, 384), BF16),
                pltpu.VMEM((NS, BLK, 128), F32),
                pltpu.VMEM((NS, BLK, 128), F32),
                pltpu.VMEM((NS, 8, 128), F32),
                pltpu.VMEM((8, 128), F32),
                dma(nz), dma(nz), dma(2, ng), dma(NS), dma(NS), dma(NS), dma(NS),
            ],
            compiler_params=pltpu.CompilerParams(
                collective_id=1, has_side_effects=True, vmem_limit_bytes=48 * 1024 * 1024
            ),
            name="lanczos",
        )(psi, lt, r2, wv)

        nv = NUM_STEPS + 1
        main = vblk[:, :64].reshape(nv, 2, BW, 4, NS, rows).transpose(4, 0, 5, 1, 3, 2).reshape(NS, nv, rows, 8, BW)
        last = vblk[:, 64:].reshape(nv, 8, 4, NS, rows).transpose(3, 0, 4, 2, 1).reshape(NS, nv, rows, 1, BW)
        vecs = jnp.concatenate([main, last], axis=3).reshape(NS, nv * rows * PAIR * BW)
        vecs = jnp.pad(vecs, ((0, 0), (0, 4096 - vecs.shape[1]))).reshape(NS, 32, 128)
        vecs = pl.pallas_call(
            tail_kernel,
            out_shape=jax.ShapeDtypeStruct((NS, 32, 128), F32),
            in_specs=vmem(1),
            out_specs=vmem(1)[0],
            scratch_shapes=[dma(NS), dma(NS)],
            compiler_params=pltpu.CompilerParams(collective_id=2, has_side_effects=True),
            name="tail",
        )(vecs)
        vecs = vecs.reshape(NS, 4096)[:, : nv * rows * PAIR * BW].reshape(NS, nv, rows, PAIR, BW)
        vecs = vecs.transpose(1, 2, 3, 0, 4).reshape(nv, rows, 3, 3, right_dim)
        return vecs, ab[0, 1 : NUM_STEPS + 1, 0], ab[1, 1 : NUM_STEPS + 1, 0]

    return jax.shard_map(
        local_run,
        mesh=mesh,
        in_specs=(P(ROW), P(None, ROW), P(), P()),
        out_specs=(P(None, ROW), P(), P()),
        check_vma=False,
    )
```

```python
import functools

import jax
import jax.numpy as jnp
from jax import lax
from jax.experimental import pallas as pl
from jax.experimental.pallas import tpu as pltpu
from jax.sharding import PartitionSpec as P

NUM_STEPS = 6
ROW = "rows"
NY, NX, NC = 4, 4, 2
NS = NY * NX
PAIR = 9
BW = 32
BLK = 72
MESH = pl.DeviceIdType.MESH
F32, BF16 = jnp.float32, jnp.bfloat16
OFFSETS = sorted(
    [(dy, dx) for dy in range(NY) for dx in range(NX) if (dy, dx) != (0, 0)],
    key=lambda o: (-(min(o[0], NY - o[0]) + min(o[1], NX - o[1])), o),
)


def place():
    me = lax.axis_index(ROW)
    return me // (NS * NC), (me // (NX * NC)) % NY, (me // NC) % NX, me % NC


def device(z, y, x, core):
    return ((z * NY + y) * NX + x) * NC + core


def rcopy(src, dst, send_sem, recv_sem, dev):
    return pltpu.make_async_remote_copy(
        src_ref=src, dst_ref=dst, send_sem=send_sem, recv_sem=recv_sem, device_id=(dev,), device_id_type=MESH
    )


def enter(devs):
    barrier = pltpu.get_barrier_semaphore()
    for dev in devs:
        pl.semaphore_signal(barrier, inc=1, device_id=(dev,), device_id_type=MESH)
    pl.semaphore_wait(barrier, len(devs))


def plane_peers(z, y, x, core):
    out = []
    for dy, dx in OFFSETS:
        py, px = (y + dy) % NY, (x + dx) % NX
        out.append((py * NX + px, device(z, py, px, core)))
    return out


def swap4(a, b, c, d):
    lane = lax.broadcasted_iota(jnp.int32, a.shape, 1)
    low = lane < 64
    even = (lane // 32) % 2 == 0
    a, c = jnp.where(low, a, pltpu.roll(c, 64, 1)), jnp.where(low, pltpu.roll(a, 64, 1), c)
    b, d = jnp.where(low, b, pltpu.roll(d, 64, 1)), jnp.where(low, pltpu.roll(b, 64, 1), d)
    a, b = jnp.where(even, a, pltpu.roll(b, 32, 1)), jnp.where(even, pltpu.roll(a, 96, 1), b)
    c, d = jnp.where(even, c, pltpu.roll(d, 32, 1)), jnp.where(even, pltpu.roll(c, 96, 1), d)
    return a, b, c, d


def fold(val):
    return jnp.sum(val.reshape(BLK // 8, 8, 128), axis=0)


def total(val):
    one = jnp.sum(jnp.sum(val, axis=0, keepdims=True), axis=1, keepdims=True)
    return jnp.broadcast_to(one, (1, 128))


def block(main, last):
    return jnp.concatenate([main[0], main[1], last], axis=0)


def pack_last(rows):
    grp = lax.broadcasted_iota(jnp.int32, (8, 128), 1) // 32
    packed = rows[0:8]
    for t in range(1, 4):
        packed = jnp.where(grp == t, pltpu.roll(rows[8 * t : 8 * t + 8], 32 * t, 1), packed)
    return packed


def unpack_last(tile):
    return jnp.concatenate([tile if t == 0 else pltpu.roll(tile, 128 - 32 * t, 1) for t in range(4)], axis=0)


def rows5(vals):
    row = lax.broadcasted_iota(jnp.int32, (8, 128), 0)
    tile = vals[4]
    for k in (3, 2, 1, 0):
        tile = jnp.where(row == k, vals[k], tile)
    return jnp.broadcast_to(tile, (8, 128))


def ratio(num, den):
    some = den > 0.0
    return jnp.where(some, num / jnp.where(some, den, 1.0), 0.0)


def main_kernel(
    nz, count, psi_ref, left_ref, op_ref, right_ref, vec_ref, alpha_ref, beta_ref,
    gbuf, vb, ut, xt, y2, sbuf, rbuf, abuf, asend, cbuf, lt, r2, wv, lf, lsend, lrecv, rt, psend, precv, osend, orecv, mt,
    g_ss, d_ss, g_rs, r_ss, r_rs, a_ss, a_rs, c_ss, c_rs, l_ss, l_rs, p_ss, p_rs, o_ss, o_rs, rt_sem,
):
    ng = nz * NC
    terms = left_ref.shape[0]
    left_dim = left_ref.shape[2]
    z, y, x, core = place()
    i, j = core * nz + z, y * NX + x
    peers = plane_peers(z, y, x, core)
    mate = device(z, y, x, 1 - core)
    zs = [((z + dz) % nz, dz) for dz in sorted(range(1, nz), key=lambda dz: (min(dz, nz - dz), dz))]
    line = [(core, pz, dz) for pz, dz in zs] + [(1 - core, pz, nz + dz) for pz, dz in zs] + [(1 - core, z, nz)]

    load_right = pltpu.make_async_copy(right_ref.at[:, pl.ds(pl.multiple_of(j * BW, BW), BW), :], rt, rt_sem)
    load_right.start()
    enter([dev for _, dev in peers] + [device(pz, y, x, pc) for pc, pz, _ in line])

    def start_gather(par):
        own = gbuf.at[par, i]
        for pz, dz in reversed(zs):
            rcopy(own, own, g_ss.at[dz], g_rs.at[par, i], device(pz, y, x, core)).start()
        rcopy(own, own, g_ss.at[0], g_rs.at[par, i], mate).start()

    def relay(par, some):
        for pz, dz in some:
            slot = core * nz + pz
            ref = gbuf.at[par, slot]
            rcopy(ref, ref, g_ss.at[dz], g_rs.at[par, slot], mate).wait_recv()
            rcopy(ref, ref, d_ss.at[dz], g_rs.at[par, slot], mate).start()

    def finish_gather(par):
        for dz in range(nz):
            slot = (1 - core) * nz + (z + dz) % nz
            ref = gbuf.at[par, slot]
            rcopy(ref, ref, g_ss.at[0], g_rs.at[par, slot], mate).wait_recv()
        own = gbuf.at[par, i]
        rcopy(own, own, g_ss.at[0], g_rs.at[par, i], mate).wait_send()
        for pz, dz in zs:
            ref = gbuf.at[par, core * nz + pz]
            rcopy(own, own, g_ss.at[dz], g_rs.at[par, i], mate).wait_send()
            rcopy(ref, ref, d_ss.at[dz], g_rs.at[par, i], mate).wait_send()

    def start_line(par, vals):
        cbuf[par, pl.ds(i, 1)] = rows5(vals)[None]
        own = cbuf.at[par, i]
        for pc, pz, k in line:
            rcopy(own, own, c_ss.at[k], c_rs.at[par, i], device(pz, y, x, pc)).start()

    def finish_line(par):
        own = cbuf.at[par, i]
        for pc, pz, k in line:
            slot = pc * nz + pz
            rcopy(own, cbuf.at[par, slot], c_ss.at[k], c_rs.at[par, slot], mate).wait()
        alpha = cbuf[par, 0, 0:1]
        for s in range(1, ng):
            alpha = alpha + cbuf[par, s, 0:1]
        alpha = alpha / count
        square = jnp.zeros((1, 128), F32)
        for s in range(ng):
            off = cbuf[par, s, 1:2] - alpha
            square = square + (cbuf[par, s, 3:4] + 2.0 * (off * cbuf[par, s, 4:5]) + (off * cbuf[par, s, 2:3]) * off)
        return alpha, jnp.sqrt(square / count)

    def start_plane(par, beta_prev):
        w, v, vp = gbuf[par, i], vb[1 - par, i], vb[par, i]
        rest = w - beta_prev * vp
        m, yv, nn = total(fold(w * v)), total(fold(rest * v)), total(fold(v * v))
        p = ratio(yv, nn)
        e = rest - p * v
        tile = rows5([m, p, nn, total(fold(e * e)), total(fold(e * v))])
        asend[...] = tile
        for pj, dev in peers:
            rcopy(asend, abuf.at[j], a_ss.at[pj], a_rs.at[j], dev).start()
        abuf[pl.ds(j, 1)] = tile[None]

    def finish_plane():
        for pj, dev in peers:
            rcopy(asend, abuf.at[pj], a_ss.at[pj], a_rs.at[pj], dev).wait()
        zero = jnp.zeros((1, 128), F32)
        m, nn, pn, ee, ev = zero, zero, zero, zero, zero
        for s in range(NS):
            m, nn, pn = m + abuf[s, 0:1], nn + abuf[s, 2:3], pn + abuf[s, 1:2] * abuf[s, 2:3]
        p = ratio(pn, nn)
        for s in range(NS):
            off = abuf[s, 1:2] - p
            ee = ee + (abuf[s, 3:4] + 2.0 * (off * abuf[s, 4:5]) + (off * abuf[s, 2:3]) * off)
            ev = ev + (abuf[s, 4:5] + off * abuf[s, 2:3])
        return [m, p, nn, ee, ev]

    early, final = (osend, orecv, o_ss, o_rs), (psend, precv, p_ss, p_rs)

    def start_out(par, bufs):
        send, recv, ss, rs = bufs
        blk = vb[par, i]
        last = unpack_last(blk[64:72])
        mt[...] = jnp.concatenate([blk[:64], last, jnp.zeros((32, 128), F32)], axis=0).T
        for pj in range(NS):
            for k in range(4):
                send[pj, 2 * k : 2 * k + 2] = mt[k * 32 + 2 * pj : k * 32 + 2 * pj + 2]
        for pj, dev in peers:
            rcopy(send.at[pj], recv.at[j], ss.at[pj], rs.at[j], dev).start()
        recv[pl.ds(j, 1)] = send[pl.ds(j, 1)]

    def finish_out(num, bufs):
        send, recv, ss, rs = bufs
        for pj, dev in peers:
            rcopy(send.at[pj], recv.at[pj], ss.at[pj], rs.at[pj], dev).wait()
        for grp in range(NS // 4):
            outs = swap4(*[recv[grp * 4 + k] for k in range(4)])
            lanes = slice(grp * 128, grp * 128 + 128)
            for t in range(2):
                for k in range(4):
                    vec_ref[num, 4 * t + k, :, lanes] = outs[t][2 * k : 2 * k + 2]
            vec_ref[num, 8, :, lanes] = outs[2][0:2]

    def update(par, alpha, beta_prev, beta, first, size):
        def body(s, carry):
            w, v, vp = gbuf[par, s], vb[1 - par, s], vb[par, s]
            vb[par, pl.ds(s, 1)] = ((w - alpha * v - beta_prev * vp) / beta)[None]
            return carry

        lax.fori_loop(first, first + size, body, 0)

    def left_and_mix(par):
        for grp in range(ng // 4):
            lanes = slice(grp * 128, grp * 128 + 128)
            for t in range(2):
                outs = swap4(*[vb[par, grp * 4 + ii, t * 32 : t * 32 + 32] for ii in range(4)])
                for k in range(4):
                    q = 4 * t + k
                    ut[q * 32 : q * 32 + 32, lanes] = outs[k].astype(BF16)
            outs = swap4(*[vb[par, grp * 4 + ii, 64:72] for ii in range(4)])
            ut[256:272, lanes] = jnp.concatenate(outs[:2], axis=0).astype(BF16)
            ut[272:288, lanes] = jnp.concatenate(outs[2:], axis=0).astype(BF16)
        width = 256
        for part in range(terms * BW // width):
            cols = slice(part * width, part * width + width)
            xt[:, cols] = jnp.dot(ut[...], lt[:, cols], preferred_element_type=F32)

        def mix(grp, carry):
            lanes = pl.ds(pl.multiple_of(grp * 128, 128), 128)
            xs = [xt[r * 32 : r * 32 + 32, lanes].astype(BF16).astype(F32) for r in range(PAIR)]

            def one(q):
                acc = wv[q * 16 : q * 16 + 1, lanes] * xs[0]
                for r in range(1, PAIR):
                    acc = acc + wv[q * 16 + r : q * 16 + r + 1, lanes] * xs[r]
                return acc

            rows = [pl.ds(pl.multiple_of(grp * 128 + k * 32, 32), 32) for k in range(4)]
            for t in range(2):
                outs = swap4(*[one(4 * t + k) for k in range(4)])
                for k in range(4):
                    y2[rows[k], t * 128 : t * 128 + 128] = outs[k].astype(BF16)
            last = one(8)
            for k in range(4):
                moved = last if k == 0 else pltpu.roll(last, 128 - 32 * k, 1)
                y2[rows[k], 256:384] = moved.astype(BF16)
            return carry

        lax.fori_loop(0, terms * BW // 128, mix, 0)

    def right_and_scatter(nxt):
        for dy in (2, 1, 3, 0):
            py = (y + dy) % NY
            part = jnp.dot(
                r2[pl.ds(pl.multiple_of(py * 128, 128), 128), :], y2[...], preferred_element_type=F32
            )
            for px in range(NX):
                pj = py * NX + px
                rows = part[px * 32 : px * 32 + 32]
                sbuf[pj, 0:32] = rows[:, 0:128]
                sbuf[pj, 32:64] = rows[:, 128:256]
                sbuf[pj, 64:72] = pack_last(rows[:, 256:384])
                send = rcopy(sbuf.at[pj], rbuf.at[j], r_ss.at[pj], r_rs.at[j], device(z, py, px, core))
                if dy:
                    send.start()
                else:

                    @pl.when(px != x)
                    def _():
                        send.start()

        rbuf[pl.ds(j, 1)] = sbuf[pl.ds(j, 1)]
        for pj, dev in reversed(peers):
            rcopy(sbuf.at[pj], rbuf.at[pj], r_ss.at[pj], r_rs.at[pj], dev).wait()
        w = rbuf[0]
        for s in range(1, NS):
            w = w + rbuf[s]
        gbuf[nxt, pl.ds(i, 1)] = w[None]

    norm = jnp.zeros((1, 128), F32)
    for grp in range(NS // 4):
        lanes = slice(grp * 128, grp * 128 + 128)
        for q in range(PAIR):
            norm = norm + jnp.sum(psi_ref[q, :, lanes] * psi_ref[q, :, lanes], axis=0, keepdims=True)
    norm = jnp.broadcast_to(jnp.sum(norm, axis=1, keepdims=True), (8, 128))
    for t in range(3):
        mt[8 * t : 8 * t + 8] = jnp.zeros((8, 128), F32)
    for grp in range(NS // 4):
        lanes = slice(grp * 128, grp * 128 + 128)
        for q in range(PAIR):
            mt[2 * q : 2 * q + 2] = psi_ref[q, :, lanes]
        outs = swap4(mt[0:8], mt[8:16], mt[16:24], norm)
        for k in range(4):
            psend[grp * 4 + k] = outs[k]
    for pj, dev in peers:
        rcopy(psend.at[pj], precv.at[j], p_ss.at[pj], p_rs.at[j], dev).start()
    precv[pl.ds(j, 1)] = psend[pl.ds(j, 1)]

    for k in range(terms):
        lf[2 * k : 2 * k + 2] = left_ref[k].astype(F32)
    row = lax.broadcasted_iota(jnp.int32, (left_dim, left_dim), 0)
    col = lax.broadcasted_iota(jnp.int32, (left_dim, left_dim), 1)
    goal = ((row >> 1) & 1) * (nz * BW) + (row >> 6) * BW + ((row >> 2) & 15) * 2 + (row & 1)
    perm = jnp.where(goal == col, 1.0, 0.0).astype(BF16)
    lsend[...] = jnp.dot(lf[...].astype(BF16), perm, preferred_element_type=F32).astype(BF16)
    for pj, dev in peers:
        rcopy(lsend, lrecv.at[j], l_ss.at[pj], l_rs.at[j], dev).start()
    lrecv[pl.ds(j, 1)] = lsend[...][None]

    term = lax.broadcasted_iota(jnp.int32, (terms, terms * BW), 0)
    lane = lax.broadcasted_iota(jnp.int32, (terms, terms * BW), 1)
    spread = jnp.where((lane >> 5) == term, 1.0, 0.0).astype(BF16)
    for q in range(PAIR):
        wv[q * 16 : q * 16 + PAIR] = jnp.dot(op_ref[q], spread, preferred_element_type=F32)
    vb[...] = jnp.zeros_like(vb)

    for pj, dev in peers:
        rcopy(psend.at[pj], precv.at[pj], p_ss.at[pj], p_rs.at[pj], dev).wait()
    square = precv[0, 0:1]
    for s in range(1, NS):
        square = square + precv[s, 0:1]
    square = jnp.where(lax.broadcasted_iota(jnp.int32, (1, 128), 1) >= 96, square, 0.0)
    square = square + pltpu.roll(square, 64, 1)
    square = square + pltpu.roll(square, 32, 1)
    for s in range(NS):
        for k in range(4):
            mt[k * 32 + 2 * s : k * 32 + 2 * s + 2] = precv[s, 2 * k : 2 * k + 2]
    flat = mt[...].T
    gbuf[0, pl.ds(i, 1)] = block((flat[0:32], flat[32:64]), pack_last(flat[64:96]))[None]
    start_gather(0)
    zero = jnp.zeros((1, 128), F32)
    start_line(0, [zero, zero, zero, square, zero])

    load_right.wait()
    for part in range(terms * BW // 128):
        rows = rt[part * 4 : part * 4 + 4].reshape(128, rt.shape[2])
        r2[:, part * 128 : part * 128 + 128] = rows.T

    relay(0, zs)
    for pj, dev in peers:
        rcopy(lsend, lrecv.at[pj], l_ss.at[pj], l_rs.at[pj], dev).wait()
    mine = lrecv[...].reshape(NS * terms * 2, left_dim)
    width = 256
    row = lax.broadcasted_iota(jnp.int32, (NS * terms * 2, width), 0)
    col = lax.broadcasted_iota(jnp.int32, (NS * terms * 2, width), 1)
    shift = terms.bit_length()
    goal = ((row & (2 * terms - 1)) >> 1) * BW + (row >> shift) * 2 + (row & 1)
    for part in range(terms * BW // width):
        perm = jnp.where(goal == col + part * width, 1.0, 0.0).astype(BF16)
        lt[:, part * width : part * width + width] = lax.dot_general(
            mine, perm, (((0,), (0,)), ((), ())), preferred_element_type=F32
        ).astype(BF16)
    finish_gather(0)
    alpha, beta = finish_line(0)
    update(0, zero, zero, beta, 0, ng)
    left_and_mix(0)
    right_and_scatter(1)

    def step(t, beta_prev):
        par = t % 2
        start_gather(par)
        start_plane(par, beta_prev)
        start_out(1 - par, early)
        relay(par, zs[:4])
        start_line(par, finish_plane())
        finish_out(t - 1, early)
        relay(par, zs[4:])
        finish_gather(par)
        alpha, beta = finish_line(par)
        alpha_ref[t - 1] = alpha[0, 0]
        beta_ref[t - 1] = beta[0, 0]
        update(par, alpha, beta_prev, beta, 0, ng)
        left_and_mix(par)
        right_and_scatter(1 - par)
        return beta

    beta_prev = lax.fori_loop(1, NUM_STEPS, step, zero)
    par = NUM_STEPS % 2
    start_plane(par, beta_prev)
    start_out(1 - par, early)
    start_line(par, finish_plane())
    finish_out(NUM_STEPS - 1, early)
    alpha, beta = finish_line(par)
    alpha_ref[NUM_STEPS - 1] = alpha[0, 0]
    beta_ref[NUM_STEPS - 1] = beta[0, 0]
    update(par, alpha, beta_prev, beta, i, 1)
    start_out(par, final)
    finish_out(NUM_STEPS, final)


def vmem(n):
    return [pl.BlockSpec(memory_space=pltpu.VMEM)] * n


def dma(*shape):
    return pltpu.SemaphoreType.DMA(shape)


def solution(mesh):
    nz = mesh.shape[ROW] // (NS * NC)
    ng = nz * NC

    def local_run(wave_rows, left_rows, op_pair, right_env):
        terms, rows, left_dim = left_rows.shape
        right_dim = right_env.shape[1]
        count = left_dim * right_dim * PAIR
        nv = NUM_STEPS + 1
        smem = pl.BlockSpec(memory_space=pltpu.SMEM)
        vecs, alpha, beta = pl.pallas_call(
            functools.partial(main_kernel, nz, float(count)),
            out_shape=(
                jax.ShapeDtypeStruct((nv, PAIR, rows, right_dim), F32),
                jax.ShapeDtypeStruct((NUM_STEPS,), F32),
                jax.ShapeDtypeStruct((NUM_STEPS,), F32),
            ),
            in_specs=vmem(3) + [pl.BlockSpec(memory_space=pl.ANY)],
            out_specs=(vmem(1)[0], smem, smem),
            scratch_shapes=[
                pltpu.VMEM((2, ng, BLK, 128), F32),
                pltpu.VMEM((2, ng, BLK, 128), F32),
                pltpu.VMEM((PAIR * BW, left_dim), BF16),
                pltpu.VMEM((PAIR * BW, terms * BW), F32),
                pltpu.VMEM((terms * BW, 384), BF16),
                pltpu.VMEM((NS, BLK, 128), F32),
                pltpu.VMEM((NS, BLK, 128), F32),
                pltpu.VMEM((NS, 8, 128), F32),
                pltpu.VMEM((8, 128), F32),
                pltpu.VMEM((2, ng, 8, 128), F32),
                pltpu.VMEM((left_dim, terms * BW), BF16),
                pltpu.VMEM((right_dim, terms * BW), BF16),
                pltpu.VMEM((PAIR * 16, terms * BW), F32),
                pltpu.VMEM((terms * rows, left_dim), F32),
                pltpu.VMEM((terms * rows, left_dim), BF16),
                pltpu.VMEM((NS, terms * rows, left_dim), BF16),
                pltpu.VMEM((terms, BW, right_dim), BF16),
                pltpu.VMEM((NS, 8, 128), F32),
                pltpu.VMEM((NS, 8, 128), F32),
                pltpu.VMEM((NS, 8, 128), F32),
                pltpu.VMEM((NS, 8, 128), F32),
                pltpu.VMEM((128, 128), F32),
                dma(nz), dma(nz), dma(2, ng), dma(NS), dma(NS), dma(NS), dma(NS), dma(ng), dma(2, ng),
                dma(NS), dma(NS), dma(NS), dma(NS), dma(NS), dma(NS), pltpu.SemaphoreType.DMA,
            ],
            compiler_params=pltpu.CompilerParams(
                collective_id=0, has_side_effects=True, vmem_limit_bytes=56 * 1024 * 1024
            ),
            name="lanczos",
        )(
            wave_rows.transpose(1, 2, 0, 3).reshape(PAIR, rows, right_dim),
            left_rows,
            op_pair.transpose(1, 2, 0),
            right_env,
        )
        vecs = vecs.reshape(nv, 3, 3, rows, right_dim).transpose(0, 3, 1, 2, 4)
        return vecs, alpha, beta

    return jax.shard_map(
        local_run,
        mesh=mesh,
        in_specs=(P(ROW), P(None, ROW), P(), P()),
        out_specs=(P(None, ROW), P(), P()),
        check_vma=False,
    )
```

```python
import functools

import jax
import jax.numpy as jnp
from jax import lax
from jax.experimental import pallas as pl
from jax.experimental.pallas import tpu as pltpu
from jax.sharding import PartitionSpec as P

NUM_STEPS = 6
ROW = "rows"
NY, NX, NC = 4, 4, 2
NS = NY * NX
PAIR = 9
BW = 32
BLK = 72
HALVES = (slice(0, 32), slice(32, 72))
LANES = 128
TILE, ROWVEC = (8, LANES), (1, LANES)
PAIRED, QUAD = range(2), range(4)
MESH = pl.DeviceIdType.MESH
F32, BF16 = jnp.float32, jnp.bfloat16
OFFSETS = sorted(
    [(dy, dx) for dy in range(NY) for dx in range(NX) if (dy, dx) != (0, 0)],
    key=lambda o: (-(min(o[0], NY - o[0]) + min(o[1], NX - o[1])), o),
)


def span(k, width):
    return slice(k * width, k * width + width)


GROUPS = [(k, span(k, LANES)) for k in QUAD]
ROW0, ROW1, ROW2, ROW3, ROW4 = [span(k, 1) for k in range(5)]


def place():
    me = lax.axis_index(ROW)
    return me // (NS * NC), (me // (NX * NC)) % NY, (me // NC) % NX, me % NC


def device(z, y, x, core):
    return ((z * NY + y) * NX + x) * NC + core


def rcopy(src, dst, send_sem, recv_sem, dev):
    return pltpu.make_async_remote_copy(
        src_ref=src, dst_ref=dst, send_sem=send_sem, recv_sem=recv_sem, device_id=(dev,), device_id_type=MESH
    )


def knock(devs):
    for dev in devs:
        pl.semaphore_signal(pltpu.get_barrier_semaphore(), inc=1, device_id=(dev,), device_id_type=MESH)


def enter(devs):
    pl.semaphore_wait(pltpu.get_barrier_semaphore(), len(devs))


def plane_peers(z, y, x, core):
    out = []
    for dy, dx in OFFSETS:
        py, px = (y + dy) % NY, (x + dx) % NX
        out.append((py * NX + px, device(z, py, px, core)))
    return out


def swap4(a, b, c, d):
    lane = lax.broadcasted_iota(jnp.int32, a.shape, 1)
    low = lane < 64
    even = (lane // 32) % 2 == 0
    a, c = jnp.where(low, a, pltpu.roll(c, 64, 1)), jnp.where(low, pltpu.roll(a, 64, 1), c)
    b, d = jnp.where(low, b, pltpu.roll(d, 64, 1)), jnp.where(low, pltpu.roll(b, 64, 1), d)
    a, b = jnp.where(even, a, pltpu.roll(b, 32, 1)), jnp.where(even, pltpu.roll(a, 96, 1), b)
    c, d = jnp.where(even, c, pltpu.roll(d, 32, 1)), jnp.where(even, pltpu.roll(c, 96, 1), d)
    return a, b, c, d


def fold(val):
    return jnp.sum(val.reshape(BLK // 8, *TILE), axis=0)


def total(val):
    one = jnp.sum(jnp.sum(val, axis=0, keepdims=True), axis=1, keepdims=True)
    return jnp.broadcast_to(one, ROWVEC)


def block(main, last):
    return jnp.concatenate([main[0], main[1], last], axis=0)


def pack_last(rows):
    grp = lax.broadcasted_iota(jnp.int32, TILE, 1) // 32
    packed = rows[0:8]
    for t in range(1, 4):
        packed = jnp.where(grp == t, pltpu.roll(rows[span(t, 8)], 32 * t, 1), packed)
    return packed


def unpack_last(tile):
    return jnp.concatenate([tile if t == 0 else pltpu.roll(tile, 128 - 32 * t, 1) for t in QUAD], axis=0)


def rows5(vals):
    row = lax.broadcasted_iota(jnp.int32, TILE, 0)
    tile = vals[4]
    for k in (3, 2, 1, 0):
        tile = jnp.where(row == k, vals[k], tile)
    return jnp.broadcast_to(tile, TILE)


def ratio(num, den):
    some = den > 0.0
    return jnp.where(some, num / jnp.where(some, den, 1.0), 0.0)


def main_kernel(
    nz, count, psi_ref, left_ref, op_ref, right_ref, vec_ref, ab_ref,
    gbuf, vb, ut, xt, y2, sbuf, rbuf, abuf, asend, cbuf, lt, r2, wv, lf, lsend, lrecv, rt, psend, precv, osend, orecv, mt,
    g_ss, d_ss, g_rs, r_ss, r_rs, a_ss, a_rs, c_ss, c_rs, l_ss, l_rs, p_ss, p_rs, o_ss, o_rs, rt_sem,
):
    ng = nz * NC
    terms = left_ref.shape[0]
    left_dim = left_ref.shape[2]
    z, y, x, core = place()
    i, j = core * nz + z, y * NX + x
    peers = plane_peers(z, y, x, core)
    mate = device(z, y, x, 1 - core)
    zs = [((z + dz) % nz, dz) for dz in sorted(range(1, nz), key=lambda dz: (min(dz, nz - dz), dz))]
    line = [(core, pz, dz) for pz, dz in zs] + [(1 - core, pz, nz + dz) for pz, dz in zs] + [(1 - core, z, nz)]

    load_right = pltpu.make_async_copy(right_ref.at[:, pl.ds(pl.multiple_of(j * BW, BW), BW), :], rt, rt_sem)
    load_right.start()
    others = [dev for _, dev in peers] + [device(pz, y, x, pc) for pc, pz, _ in line]
    knock(others)

    def start_gather(par, half):
        own = gbuf.at[par, i, HALVES[half]]
        for pz, dz in reversed(zs):
            rcopy(own, own, g_ss.at[half, dz], g_rs.at[2 * par + half, i], device(pz, y, x, core)).start()
        rcopy(own, own, g_ss.at[half, 0], g_rs.at[2 * par + half, i], mate).start()

    def relay(par, half):
        for pz, dz in zs:
            slot = core * nz + pz
            ref = gbuf.at[par, slot, HALVES[half]]
            rcopy(ref, ref, g_ss.at[half, dz], g_rs.at[2 * par + half, slot], mate).wait_recv()
            rcopy(ref, ref, d_ss.at[half, dz], g_rs.at[2 * par + half, slot], mate).start()

    def finish_gather(par):
        for half in PAIRED:
            for dz in range(nz):
                slot = (1 - core) * nz + (z + dz) % nz
                ref = gbuf.at[par, slot, HALVES[half]]
                rcopy(ref, ref, g_ss.at[half, 0], g_rs.at[2 * par + half, slot], mate).wait_recv()
        for half in PAIRED:
            own = gbuf.at[par, i, HALVES[half]]
            rcopy(own, own, g_ss.at[half, 0], g_rs.at[2 * par + half, i], mate).wait_send()
            for pz, dz in zs:
                ref = gbuf.at[par, core * nz + pz, HALVES[half]]
                rcopy(own, own, g_ss.at[half, dz], g_rs.at[2 * par + half, i], mate).wait_send()
                rcopy(ref, ref, d_ss.at[half, dz], g_rs.at[2 * par + half, i], mate).wait_send()

    def start_line(par, vals):
        cbuf[par, pl.ds(i, 1)] = rows5(vals)[None]
        own = cbuf.at[par, i]
        for pc, pz, k in line:
            rcopy(own, own, c_ss.at[k], c_rs.at[par, i], device(pz, y, x, pc)).start()

    def finish_line(par):
        own = cbuf.at[par, i]
        for pc, pz, k in line:
            slot = pc * nz + pz
            rcopy(own, cbuf.at[par, slot], c_ss.at[k], c_rs.at[par, slot], mate).wait()
        alpha = cbuf[par, 0, ROW0]
        for s in range(1, ng):
            alpha = alpha + cbuf[par, s, ROW0]
        alpha = alpha / count
        square = jnp.zeros(ROWVEC, F32)
        for s in range(ng):
            off = cbuf[par, s, ROW1] - alpha
            square = square + (cbuf[par, s, ROW3] + 2.0 * (off * cbuf[par, s, ROW4]) + (off * cbuf[par, s, ROW2]) * off)
        return alpha, jnp.sqrt(square / count)

    def start_plane(par, beta_prev):
        w, v, vp = gbuf[par, i], vb[1 - par, i], vb[par, i]
        rest = w - beta_prev * vp
        m, yv, nn = total(fold(w * v)), total(fold(rest * v)), total(fold(v * v))
        p = ratio(yv, nn)
        e = rest - p * v
        tile = rows5([m, p, nn, total(fold(e * e)), total(fold(e * v))])
        asend[...] = tile
        for pj, dev in peers:
            rcopy(asend, abuf.at[j], a_ss.at[pj], a_rs.at[j], dev).start()
        abuf[pl.ds(j, 1)] = tile[None]

    def finish_plane():
        for pj, dev in peers:
            rcopy(asend, abuf.at[pj], a_ss.at[pj], a_rs.at[pj], dev).wait()
        zero = jnp.zeros(ROWVEC, F32)
        m, nn, pn, ee, ev = zero, zero, zero, zero, zero
        for s in range(NS):
            m, nn, pn = m + abuf[s, ROW0], nn + abuf[s, ROW2], pn + abuf[s, ROW1] * abuf[s, ROW2]
        p = ratio(pn, nn)
        for s in range(NS):
            off = abuf[s, ROW1] - p
            ee = ee + (abuf[s, ROW3] + 2.0 * (off * abuf[s, ROW4]) + (off * abuf[s, ROW2]) * off)
            ev = ev + (abuf[s, ROW4] + off * abuf[s, ROW2])
        return [m, p, nn, ee, ev]

    def start_out(par):
        blk = gbuf[par, i]
        last = unpack_last(blk[64:72])
        mt[...] = jnp.concatenate([blk[:64], last, jnp.zeros((32, 128), F32)], axis=0).T
        for pj in range(NS):
            for k in QUAD:
                osend[pj, span(k, 2)] = mt[span(k * NS + pj, 2)]
        for pj, dev in peers:
            rcopy(osend.at[pj], orecv.at[j], o_ss.at[pj], o_rs.at[j], dev).start()
        orecv[pl.ds(j, 1)] = osend[pl.ds(j, 1)]

    def finish_out(num):
        for pj, dev in peers:
            rcopy(osend.at[pj], orecv.at[pj], o_ss.at[pj], o_rs.at[pj], dev).wait()
        for grp, lanes in GROUPS:
            outs = swap4(*[orecv[grp * 4 + k] for k in QUAD])
            for t in PAIRED:
                for k in QUAD:
                    vec_ref[num, 4 * t + k, :, lanes] = outs[t][span(k, 2)]
            vec_ref[num, 8, :, lanes] = outs[2][0:2]

    def own_rows(num, alpha, beta_prev, beta):
        older = num - 2 if isinstance(num, int) else jnp.maximum(num - 2, 0)
        for grp, lanes in GROUPS:
            for q in range(PAIR):
                w, v, vp = vec_ref[num, q, :, lanes], vec_ref[num - 1, q, :, lanes], vec_ref[older, q, :, lanes]
                vec_ref[num, q, :, lanes] = (w - alpha * v - beta_prev * vp) / beta

    def update(par, alpha, beta_prev, beta, first, size):
        def body(s, carry):
            w, v, vp = gbuf[par, s], vb[1 - par, s], vb[par, s]
            vb[par, pl.ds(s, 1)] = ((w - alpha * v - beta_prev * vp) / beta)[None]
            return carry

        lax.fori_loop(first, first + size, body, 0)

    def left(par):
        for grp in range(ng // 4):
            lanes = span(grp, LANES)
            for t in PAIRED:
                outs = swap4(*[vb[par, grp * 4 + ii, span(t, BW)] for ii in QUAD])
                for k in QUAD:
                    q = 4 * t + k
                    ut[span(q, BW), lanes] = outs[k].astype(BF16)
            outs = swap4(*[vb[par, grp * 4 + ii, 64:72] for ii in QUAD])
            ut[256:272, lanes] = jnp.concatenate(outs[:2], axis=0).astype(BF16)
            ut[272:288, lanes] = jnp.concatenate(outs[2:], axis=0).astype(BF16)
        width = 256
        for part in range(terms * BW // width):
            cols = span(part, width)
            whole = jnp.dot(ut[...], lt[:, cols], preferred_element_type=F32)
            xt[:, cols] = whole.astype(BF16).astype(F32)

    def mix(half):
        def body(grp, carry):
            lanes = pl.ds(pl.multiple_of(grp * 128, 128), 128)
            xs = [xt[span(r, BW), lanes] for r in range(PAIR)]

            def one(q):
                acc = wv[q * 16 : q * 16 + 1, lanes] * xs[0]
                for r in range(1, PAIR):
                    acc = acc + wv[q * 16 + r : q * 16 + r + 1, lanes] * xs[r]
                return acc

            rows = [pl.ds(pl.multiple_of(grp * 128 + k * 32, 32), 32) for k in QUAD]
            outs = swap4(*[one(4 * half + k) for k in QUAD])
            for k in QUAD:
                y2[rows[k], span(half, LANES)] = outs[k].astype(BF16)
            if half:
                last = one(8)
                for k in QUAD:
                    moved = last if k == 0 else pltpu.roll(last, 128 - 32 * k, 1)
                    y2[rows[k], 256:384] = moved.astype(BF16)
            return carry

        lax.fori_loop(0, terms * BW // 128, body, 0)

    def start_scatter(half):
        cols = slice(0, 128) if half == 0 else slice(128, 384)
        for dy in (2, 1, 3, 0):
            py = (y + dy) % NY
            part = jnp.dot(
                r2[pl.ds(pl.multiple_of(py * 128, 128), 128), :], y2[:, cols], preferred_element_type=F32
            )
            for px in range(NX):
                pj = py * NX + px
                rows = part[span(px, BW)]
                if half == 0:
                    sbuf[pj, 0:32] = rows
                else:
                    sbuf[pj, 32:64] = rows[:, 0:128]
                    sbuf[pj, 64:72] = pack_last(rows[:, 128:256])
                send = rcopy(
                    sbuf.at[pj, HALVES[half]], rbuf.at[j, HALVES[half]],
                    r_ss.at[half, pj], r_rs.at[half, j], device(z, py, px, core),
                )
                if dy:
                    send.start()
                else:

                    @pl.when(px != x)
                    def _():
                        send.start()

        rbuf[pl.ds(j, 1), HALVES[half]] = sbuf[pl.ds(j, 1), HALVES[half]]

    def finish_scatter(nxt, half):
        for pj, dev in reversed(peers):
            rcopy(
                sbuf.at[pj, HALVES[half]], rbuf.at[pj, HALVES[half]], r_ss.at[half, pj], r_rs.at[half, pj], dev
            ).wait()
        w = rbuf[0, HALVES[half]]
        for s in range(1, NS):
            w = w + rbuf[s, HALVES[half]]
        gbuf[nxt, pl.ds(i, 1), HALVES[half]] = w[None]

    def product(par, nxt, more, between):
        left(par)
        for half in PAIRED:
            mix(half)
            start_scatter(half)
        between()
        for half in PAIRED:
            finish_scatter(nxt, half)
            if more is True:
                start_gather(nxt, half)
            else:

                @pl.when(more)
                def _(half=half):
                    start_gather(nxt, half)

    norm = jnp.zeros(ROWVEC, F32)
    for grp, lanes in GROUPS:
        for q in range(PAIR):
            norm = norm + jnp.sum(psi_ref[q, :, lanes] * psi_ref[q, :, lanes], axis=0, keepdims=True)
    norm = jnp.broadcast_to(jnp.sum(norm, axis=1, keepdims=True), TILE)
    for t in range(3):
        mt[span(t, 8)] = jnp.zeros(TILE, F32)
    for grp, lanes in GROUPS:
        for q in range(PAIR):
            mt[span(q, 2)] = psi_ref[q, :, lanes]
        outs = swap4(mt[0:8], mt[8:16], mt[16:24], norm)
        for k in QUAD:
            psend[grp * 4 + k] = outs[k]
    enter(others)
    for pj, dev in peers:
        rcopy(psend.at[pj], precv.at[j], p_ss.at[pj], p_rs.at[j], dev).start()
    precv[pl.ds(j, 1)] = psend[pl.ds(j, 1)]

    for k in range(terms):
        lf[span(k, 2)] = left_ref[k].astype(F32)
    row = lax.broadcasted_iota(jnp.int32, (left_dim, left_dim), 0)
    col = lax.broadcasted_iota(jnp.int32, (left_dim, left_dim), 1)
    goal = ((row >> 1) & 1) * (nz * BW) + (row >> 6) * BW + ((row >> 2) & 15) * 2 + (row & 1)
    perm = jnp.where(goal == col, 1.0, 0.0).astype(BF16)
    lsend[...] = jnp.dot(lf[...].astype(BF16), perm, preferred_element_type=F32).astype(BF16)
    for pj, dev in peers:
        rcopy(lsend, lrecv.at[j], l_ss.at[pj], l_rs.at[j], dev).start()
    lrecv[pl.ds(j, 1)] = lsend[...][None]

    term = lax.broadcasted_iota(jnp.int32, (terms, terms * BW), 0)
    lane = lax.broadcasted_iota(jnp.int32, (terms, terms * BW), 1)
    spread = jnp.where((lane >> 5) == term, 1.0, 0.0).astype(BF16)
    for q in range(PAIR):
        wv[q * 16 : q * 16 + PAIR] = jnp.dot(op_ref[q], spread, preferred_element_type=F32)
    vb[...] = jnp.zeros_like(vb)

    for pj, dev in peers:
        rcopy(psend.at[pj], precv.at[pj], p_ss.at[pj], p_rs.at[pj], dev).wait()
    square = precv[0, ROW0]
    for s in range(1, NS):
        square = square + precv[s, ROW0]
    square = jnp.where(lax.broadcasted_iota(jnp.int32, ROWVEC, 1) >= 96, square, 0.0)
    square = square + pltpu.roll(square, 64, 1)
    square = square + pltpu.roll(square, 32, 1)
    for s in range(NS):
        for k in QUAD:
            mt[span(k * NS + s, 2)] = precv[s, span(k, 2)]
    flat = mt[...].T
    gbuf[0, pl.ds(i, 1)] = block((flat[span(0, BW)], flat[span(1, BW)]), pack_last(flat[span(2, BW)]))[None]
    start_gather(0, 0)
    start_gather(0, 1)
    zero = jnp.zeros(ROWVEC, F32)
    start_line(0, [zero, zero, zero, square, zero])

    load_right.wait()
    for part in range(terms * BW // 128):
        rows = rt[span(part, 4)].reshape(128, rt.shape[2])
        r2[:, span(part, LANES)] = rows.T

    relay(0, 0)
    relay(0, 1)
    for pj, dev in peers:
        rcopy(lsend, lrecv.at[pj], l_ss.at[pj], l_rs.at[pj], dev).wait()
    mine = lrecv[...].reshape(NS * terms * 2, left_dim)
    width = 256
    row = lax.broadcasted_iota(jnp.int32, (NS * terms * 2, width), 0)
    col = lax.broadcasted_iota(jnp.int32, (NS * terms * 2, width), 1)
    shift = terms.bit_length()
    goal = ((row & (2 * terms - 1)) >> 1) * BW + (row >> shift) * 2 + (row & 1)
    for part in range(terms * BW // width):
        perm = jnp.where(goal == col + part * width, 1.0, 0.0).astype(BF16)
        lt[:, span(part, width)] = lax.dot_general(
            mine, perm, (((0,), (0,)), ((), ())), preferred_element_type=F32
        ).astype(BF16)
    finish_gather(0)
    alpha, beta = finish_line(0)
    update(0, zero, zero, beta, 0, ng)

    def first_rows():
        for grp, lanes in GROUPS:
            for q in range(PAIR):
                vec_ref[0, q, :, lanes] = psi_ref[q, :, lanes] / beta

    product(0, 1, True, first_rows)

    def step(t, beta_prev):
        par = t % 2
        start_plane(par, beta_prev)
        start_out(par)
        relay(par, 0)
        start_line(par, finish_plane())
        relay(par, 1)
        finish_out(t)
        finish_gather(par)
        alpha, beta = finish_line(par)
        update(par, alpha, beta_prev, beta, 0, ng)

        def rest():
            ab_ref[0, t - 1] = alpha[0, 0]
            ab_ref[1, t - 1] = beta[0, 0]
            own_rows(t, alpha, beta_prev, beta)

        product(par, 1 - par, t < NUM_STEPS - 1, rest)
        return beta

    beta_prev = lax.fori_loop(1, NUM_STEPS, step, zero)
    par = NUM_STEPS % 2
    start_plane(par, beta_prev)
    start_out(par)
    start_line(par, finish_plane())
    finish_out(NUM_STEPS)
    alpha, beta = finish_line(par)
    ab_ref[0, NUM_STEPS - 1] = alpha[0, 0]
    ab_ref[1, NUM_STEPS - 1] = beta[0, 0]
    own_rows(NUM_STEPS, alpha, beta_prev, beta)


def vmem(n):
    return [pl.BlockSpec(memory_space=pltpu.VMEM)] * n


def dma(*shape):
    return pltpu.SemaphoreType.DMA(shape)


def solution(mesh):
    nz = mesh.shape[ROW] // (NS * NC)
    ng = nz * NC

    def local_run(wave_rows, left_rows, op_pair, right_env):
        terms, rows, left_dim = left_rows.shape
        right_dim = right_env.shape[1]
        count = left_dim * right_dim * PAIR
        nv = NUM_STEPS + 1
        smem = pl.BlockSpec(memory_space=pltpu.SMEM)
        vecs, ab = pl.pallas_call(
            functools.partial(main_kernel, nz, float(count)),
            out_shape=(
                jax.ShapeDtypeStruct((nv, PAIR, rows, right_dim), F32),
                jax.ShapeDtypeStruct((2, NUM_STEPS), F32),
            ),
            in_specs=vmem(3) + [pl.BlockSpec(memory_space=pl.ANY)],
            out_specs=(vmem(1)[0], smem),
            scratch_shapes=[
                pltpu.VMEM((2, ng, BLK, LANES), F32),
                pltpu.VMEM((2, ng, BLK, LANES), F32),
                pltpu.VMEM((PAIR * BW, left_dim), BF16),
                pltpu.VMEM((PAIR * BW, terms * BW), F32),
                pltpu.VMEM((terms * BW, 384), BF16),
                pltpu.VMEM((NS, BLK, LANES), F32),
                pltpu.VMEM((NS, BLK, LANES), F32),
                pltpu.VMEM((NS, *TILE), F32),
                pltpu.VMEM(TILE, F32),
                pltpu.VMEM((2, ng, *TILE), F32),
                pltpu.VMEM((left_dim, terms * BW), BF16),
                pltpu.VMEM((right_dim, terms * BW), BF16),
                pltpu.VMEM((PAIR * 16, terms * BW), F32),
                pltpu.VMEM((terms * rows, left_dim), F32),
                pltpu.VMEM((terms * rows, left_dim), BF16),
                pltpu.VMEM((NS, terms * rows, left_dim), BF16),
                pltpu.VMEM((terms, BW, right_dim), BF16),
                pltpu.VMEM((NS, *TILE), F32),
                pltpu.VMEM((NS, *TILE), F32),
                pltpu.VMEM((NS, *TILE), F32),
                pltpu.VMEM((NS, *TILE), F32),
                pltpu.VMEM((128, 128), F32),
                dma(2, nz), dma(2, nz), dma(4, ng), dma(2, NS), dma(2, NS), dma(NS), dma(NS), dma(ng), dma(2, ng),
                dma(NS), dma(NS), dma(NS), dma(NS), dma(NS), dma(NS), pltpu.SemaphoreType.DMA,
            ],
            compiler_params=pltpu.CompilerParams(
                collective_id=0, has_side_effects=True, vmem_limit_bytes=56 * 1024 * 1024
            ),
            name="lanczos",
        )(
            wave_rows.transpose(1, 2, 0, 3).reshape(PAIR, rows, right_dim),
            left_rows,
            op_pair.transpose(1, 2, 0),
            right_env,
        )
        vecs = vecs.reshape(nv, 3, 3, rows, right_dim).transpose(0, 3, 1, 2, 4)
        return vecs, ab[0], ab[1]

    return jax.shard_map(
        local_run,
        mesh=mesh,
        in_specs=(P(ROW), P(None, ROW), P(), P()),
        out_specs=(P(None, ROW), P(), P()),
        check_vma=False,
    )
```

```python
import functools

import jax
import jax.numpy as jnp
from jax import lax
from jax.experimental import pallas as pl
from jax.experimental.pallas import tpu as pltpu
from jax.sharding import PartitionSpec as P

NUM_STEPS = 6
ROW = "rows"
NY, NX, NC = 4, 4, 2
NS = NY * NX
PAIR = 9
BW = 32
BLK = 72
HALVES = (slice(0, 32), slice(32, 72))
LANES = 128
TILE, ROWVEC = (8, LANES), (1, LANES)
PAIRED, QUAD = range(2), range(4)
MESH = pl.DeviceIdType.MESH
F32, BF16 = jnp.float32, jnp.bfloat16
OFFSETS = sorted(
    [(dy, dx) for dy in range(NY) for dx in range(NX) if (dy, dx) != (0, 0)],
    key=lambda o: (-(min(o[0], NY - o[0]) + min(o[1], NX - o[1])), o),
)


def span(k, width):
    return slice(k * width, k * width + width)


GROUPS = [(k, span(k, LANES)) for k in QUAD]
ROW0, ROW1, ROW2, ROW3, ROW4 = [span(k, 1) for k in range(5)]


def place():
    me = lax.axis_index(ROW)
    return me // (NS * NC), (me // (NX * NC)) % NY, (me // NC) % NX, me % NC


def device(z, y, x, core):
    return ((z * NY + y) * NX + x) * NC + core


def rcopy(src, dst, send_sem, recv_sem, dev):
    return pltpu.make_async_remote_copy(
        src_ref=src, dst_ref=dst, send_sem=send_sem, recv_sem=recv_sem, device_id=(dev,), device_id_type=MESH
    )


def knock(devs):
    for dev in devs:
        pl.semaphore_signal(pltpu.get_barrier_semaphore(), inc=1, device_id=(dev,), device_id_type=MESH)


def enter(devs):
    pl.semaphore_wait(pltpu.get_barrier_semaphore(), len(devs))


def plane_peers(z, y, x, core):
    out = []
    for dy, dx in OFFSETS:
        py, px = (y + dy) % NY, (x + dx) % NX
        out.append((py * NX + px, device(z, py, px, core)))
    return out


def swap4(a, b, c, d):
    lane = lax.broadcasted_iota(jnp.int32, a.shape, 1)
    low = lane < 64
    even = (lane // 32) % 2 == 0
    a, c = jnp.where(low, a, pltpu.roll(c, 64, 1)), jnp.where(low, pltpu.roll(a, 64, 1), c)
    b, d = jnp.where(low, b, pltpu.roll(d, 64, 1)), jnp.where(low, pltpu.roll(b, 64, 1), d)
    a, b = jnp.where(even, a, pltpu.roll(b, 32, 1)), jnp.where(even, pltpu.roll(a, 96, 1), b)
    c, d = jnp.where(even, c, pltpu.roll(d, 32, 1)), jnp.where(even, pltpu.roll(c, 96, 1), d)
    return a, b, c, d


def fold(val):
    return jnp.sum(val.reshape(BLK // 8, *TILE), axis=0)


def total(val):
    one = jnp.sum(jnp.sum(val, axis=0, keepdims=True), axis=1, keepdims=True)
    return jnp.broadcast_to(one, ROWVEC)


def block(main, last):
    return jnp.concatenate([main[0], main[1], last], axis=0)


def pack_last(rows):
    grp = lax.broadcasted_iota(jnp.int32, TILE, 1) // 32
    packed = rows[0:8]
    for t in range(1, 4):
        packed = jnp.where(grp == t, pltpu.roll(rows[span(t, 8)], 32 * t, 1), packed)
    return packed


def unpack_last(tile):
    return jnp.concatenate([tile if t == 0 else pltpu.roll(tile, 128 - 32 * t, 1) for t in QUAD], axis=0)


def rows5(vals):
    row = lax.broadcasted_iota(jnp.int32, TILE, 0)
    tile = vals[4]
    for k in (3, 2, 1, 0):
        tile = jnp.where(row == k, vals[k], tile)
    return jnp.broadcast_to(tile, TILE)


def ratio(num, den):
    some = den > 0.0
    return jnp.where(some, num / jnp.where(some, den, 1.0), 0.0)


def main_kernel(
    nz, count, psi_ref, left_ref, op_ref, right_ref, vec_ref, ab_ref,
    gbuf, vb, ut, xt, y2, sbuf, rbuf, abuf, asend, cbuf, lt, r2, wv, lf, lsend, lrecv, rt, psend, precv, osend, orecv, mt,
    g_ss, d_ss, g_rs, r_ss, r_rs, a_ss, a_rs, c_ss, c_rs, l_ss, l_rs, p_ss, p_rs, o_ss, o_rs, rt_sem,
):
    ng = nz * NC
    terms = left_ref.shape[0]
    left_dim = left_ref.shape[2]
    z, y, x, core = place()
    i, j = core * nz + z, y * NX + x
    peers = plane_peers(z, y, x, core)
    mate = device(z, y, x, 1 - core)
    zs = [((z + dz) % nz, dz) for dz in sorted(range(1, nz), key=lambda dz: (min(dz, nz - dz), dz))]
    line = [(core, pz, dz) for pz, dz in zs] + [(1 - core, pz, nz + dz) for pz, dz in zs] + [(1 - core, z, nz)]

    load_right = pltpu.make_async_copy(right_ref.at[:, pl.ds(pl.multiple_of(j * BW, BW), BW), :], rt, rt_sem)
    load_right.start()
    others = [dev for _, dev in peers] + [device(pz, y, x, pc) for pc, pz, _ in line]
    knock(others)

    def start_gather(par, half):
        own = gbuf.at[par, i, HALVES[half]]
        for pz, dz in reversed(zs):
            rcopy(own, own, g_ss.at[half, dz], g_rs.at[2 * par + half, i], device(pz, y, x, core)).start()
        rcopy(own, own, g_ss.at[half, 0], g_rs.at[2 * par + half, i], mate).start()

    def relay(par, half):
        for pz, dz in zs:
            slot = core * nz + pz
            ref = gbuf.at[par, slot, HALVES[half]]
            rcopy(ref, ref, g_ss.at[half, dz], g_rs.at[2 * par + half, slot], mate).wait_recv()
            rcopy(ref, ref, d_ss.at[half, dz], g_rs.at[2 * par + half, slot], mate).start()

    def finish_gather(par):
        for half in PAIRED:
            for dz in range(nz):
                slot = (1 - core) * nz + (z + dz) % nz
                ref = gbuf.at[par, slot, HALVES[half]]
                rcopy(ref, ref, g_ss.at[half, 0], g_rs.at[2 * par + half, slot], mate).wait_recv()
    def drain_gather(par):
        for half in PAIRED:
            own = gbuf.at[par, i, HALVES[half]]
            rcopy(own, own, g_ss.at[half, 0], g_rs.at[2 * par + half, i], mate).wait_send()
            for pz, dz in zs:
                ref = gbuf.at[par, core * nz + pz, HALVES[half]]
                rcopy(own, own, g_ss.at[half, dz], g_rs.at[2 * par + half, i], mate).wait_send()
                rcopy(ref, ref, d_ss.at[half, dz], g_rs.at[2 * par + half, i], mate).wait_send()

    def start_line(par, vals):
        cbuf[par, pl.ds(i, 1)] = rows5(vals)[None]
        own = cbuf.at[par, i]
        for pc, pz, k in line:
            rcopy(own, own, c_ss.at[k], c_rs.at[par, i], device(pz, y, x, pc)).start()

    def finish_line(par):
        own = cbuf.at[par, i]
        for pc, pz, k in line:
            slot = pc * nz + pz
            rcopy(own, cbuf.at[par, slot], c_ss.at[k], c_rs.at[par, slot], mate).wait()
        alpha = cbuf[par, 0, ROW0]
        for s in range(1, ng):
            alpha = alpha + cbuf[par, s, ROW0]
        alpha = alpha / count
        square = jnp.zeros(ROWVEC, F32)
        for s in range(ng):
            off = cbuf[par, s, ROW1] - alpha
            square = square + (cbuf[par, s, ROW3] + 2.0 * (off * cbuf[par, s, ROW4]) + (off * cbuf[par, s, ROW2]) * off)
        return alpha, jnp.sqrt(square / count)

    def start_plane(par, beta_prev):
        w, v, vp = gbuf[par, i], vb[1 - par, i], vb[par, i]
        rest = w - beta_prev * vp
        m, yv, nn = total(fold(w * v)), total(fold(rest * v)), total(fold(v * v))
        p = ratio(yv, nn)
        e = rest - p * v
        tile = rows5([m, p, nn, total(fold(e * e)), total(fold(e * v))])
        asend[...] = tile
        for pj, dev in peers:
            rcopy(asend, abuf.at[j], a_ss.at[pj], a_rs.at[j], dev).start()
        abuf[pl.ds(j, 1)] = tile[None]

    def finish_plane():
        for pj, dev in peers:
            rcopy(asend, abuf.at[pj], a_ss.at[pj], a_rs.at[pj], dev).wait()
        zero = jnp.zeros(ROWVEC, F32)
        m, nn, pn, ee, ev = zero, zero, zero, zero, zero
        for s in range(NS):
            m, nn, pn = m + abuf[s, ROW0], nn + abuf[s, ROW2], pn + abuf[s, ROW1] * abuf[s, ROW2]
        p = ratio(pn, nn)
        for s in range(NS):
            off = abuf[s, ROW1] - p
            ee = ee + (abuf[s, ROW3] + 2.0 * (off * abuf[s, ROW4]) + (off * abuf[s, ROW2]) * off)
            ev = ev + (abuf[s, ROW4] + off * abuf[s, ROW2])
        return [m, p, nn, ee, ev]

    def start_out(par):
        blk = gbuf[par, i]
        last = unpack_last(blk[64:72])
        mt[...] = jnp.concatenate([blk[:64], last, jnp.zeros((32, 128), F32)], axis=0).T
        for pj in range(NS):
            for k in QUAD:
                osend[pj, span(k, 2)] = mt[span(k * NS + pj, 2)]
        for pj, dev in peers:
            rcopy(osend.at[pj], orecv.at[j], o_ss.at[pj], o_rs.at[j], dev).start()
        orecv[pl.ds(j, 1)] = osend[pl.ds(j, 1)]

    def finish_out(num):
        for pj, dev in peers:
            rcopy(osend.at[pj], orecv.at[pj], o_ss.at[pj], o_rs.at[pj], dev).wait()
        for grp, lanes in GROUPS:
            outs = swap4(*[orecv[grp * 4 + k] for k in QUAD])
            for t in PAIRED:
                for k in QUAD:
                    vec_ref[num, 4 * t + k, :, lanes] = outs[t][span(k, 2)]
            vec_ref[num, 8, :, lanes] = outs[2][0:2]

    def own_rows(num, alpha, beta_prev, beta):
        older = num - 2 if isinstance(num, int) else jnp.maximum(num - 2, 0)
        for grp, lanes in GROUPS:
            for q in range(PAIR):
                w, v, vp = vec_ref[num, q, :, lanes], vec_ref[num - 1, q, :, lanes], vec_ref[older, q, :, lanes]
                vec_ref[num, q, :, lanes] = (w - alpha * v - beta_prev * vp) / beta

    def update(par, alpha, beta_prev, beta, first, size):
        def body(s, carry):
            w, v, vp = gbuf[par, s], vb[1 - par, s], vb[par, s]
            vb[par, pl.ds(s, 1)] = ((w - alpha * v - beta_prev * vp) / beta)[None]
            return carry

        lax.fori_loop(first, first + size, body, 0, unroll=4 if size > 1 else 1)

    def left_and_mix(par):
        for grp in range(ng // 4):
            lanes = span(grp, LANES)
            for t in PAIRED:
                outs = swap4(*[vb[par, grp * 4 + ii, span(t, BW)] for ii in QUAD])
                for k in QUAD:
                    q = 4 * t + k
                    ut[span(q, BW), lanes] = outs[k].astype(BF16)
            outs = swap4(*[vb[par, grp * 4 + ii, 64:72] for ii in QUAD])
            ut[256:272, lanes] = jnp.concatenate(outs[:2], axis=0).astype(BF16)
            ut[272:288, lanes] = jnp.concatenate(outs[2:], axis=0).astype(BF16)
        width = 256
        for part in range(terms * BW // width):
            cols = span(part, width)
            whole = jnp.dot(ut[...], lt[:, cols], preferred_element_type=F32).astype(BF16).astype(F32)
            xt[:, cols] = whole
            for sub in range(width // LANES):
                grp = part * (width // LANES) + sub
                mix(0, [whole[span(r, BW), span(sub, LANES)] for r in range(PAIR)], span(grp, LANES), grp * LANES)

    def mix(half, xs, lanes, first):
        def one(q):
            acc = wv[q * 16 : q * 16 + 1, lanes] * xs[0]
            for r in range(1, PAIR):
                acc = acc + wv[q * 16 + r : q * 16 + r + 1, lanes] * xs[r]
            return acc

        rows = [pl.ds(first + k * BW, BW) for k in QUAD]
        outs = swap4(*[one(4 * half + k) for k in QUAD])
        for k in QUAD:
            y2[rows[k], span(half, LANES)] = outs[k].astype(BF16)
        if half:
            last = one(8)
            for k in QUAD:
                moved = last if k == 0 else pltpu.roll(last, LANES - BW * k, 1)
                y2[rows[k], 2 * LANES :] = moved.astype(BF16)

    def mix_rest():
        def body(grp, carry):
            first = pl.multiple_of(grp * LANES, LANES)
            lanes = pl.ds(first, LANES)
            mix(1, [xt[span(r, BW), lanes] for r in range(PAIR)], lanes, first)
            return carry

        lax.fori_loop(0, terms * BW // LANES, body, 0, unroll=2)

    def start_scatter(half):
        cols = slice(0, 128) if half == 0 else slice(128, 384)
        for dy in (2, 1, 3, 0):
            py = (y + dy) % NY
            part = jnp.dot(
                r2[pl.ds(pl.multiple_of(py * 128, 128), 128), :], y2[:, cols], preferred_element_type=F32
            )
            for px in range(NX):
                pj = py * NX + px
                rows = part[span(px, BW)]
                if half == 0:
                    sbuf[pj, 0:32] = rows
                else:
                    sbuf[pj, 32:64] = rows[:, 0:128]
                    sbuf[pj, 64:72] = pack_last(rows[:, 128:256])
                send = rcopy(
                    sbuf.at[pj, HALVES[half]], rbuf.at[j, HALVES[half]],
                    r_ss.at[half, pj], r_rs.at[half, j], device(z, py, px, core),
                )
                if dy:
                    send.start()
                else:

                    @pl.when(px != x)
                    def _():
                        send.start()

        rbuf[pl.ds(j, 1), HALVES[half]] = sbuf[pl.ds(j, 1), HALVES[half]]

    def finish_scatter(nxt, half):
        for pj, dev in reversed(peers):
            rcopy(
                sbuf.at[pj, HALVES[half]], rbuf.at[pj, HALVES[half]], r_ss.at[half, pj], r_rs.at[half, pj], dev
            ).wait()
        w = rbuf[0, HALVES[half]]
        for s in range(1, NS):
            w = w + rbuf[s, HALVES[half]]
        gbuf[nxt, pl.ds(i, 1), HALVES[half]] = w[None]

    def product(par, nxt, more, between):
        left_and_mix(par)
        start_scatter(0)
        mix_rest()
        start_scatter(1)
        drain_gather(par)
        between()
        for half in PAIRED:
            finish_scatter(nxt, half)
            if more is True:
                start_gather(nxt, half)
            else:

                @pl.when(more)
                def _(half=half):
                    start_gather(nxt, half)

    norm = jnp.zeros(ROWVEC, F32)
    for grp, lanes in GROUPS:
        for q in range(PAIR):
            norm = norm + jnp.sum(psi_ref[q, :, lanes] * psi_ref[q, :, lanes], axis=0, keepdims=True)
    norm = jnp.broadcast_to(jnp.sum(norm, axis=1, keepdims=True), TILE)
    for t in range(3):
        mt[span(t, 8)] = jnp.zeros(TILE, F32)
    for grp, lanes in GROUPS:
        for q in range(PAIR):
            mt[span(q, 2)] = psi_ref[q, :, lanes]
        outs = swap4(mt[0:8], mt[8:16], mt[16:24], norm)
        for k in QUAD:
            psend[grp * 4 + k] = outs[k]
    enter(others)
    for pj, dev in peers:
        rcopy(psend.at[pj], precv.at[j], p_ss.at[pj], p_rs.at[j], dev).start()
    precv[pl.ds(j, 1)] = psend[pl.ds(j, 1)]

    for k in range(terms):
        lf[span(k, 2)] = left_ref[k].astype(F32)
    row = lax.broadcasted_iota(jnp.int32, (left_dim, left_dim), 0)
    col = lax.broadcasted_iota(jnp.int32, (left_dim, left_dim), 1)
    goal = ((row >> 1) & 1) * (nz * BW) + (row >> 6) * BW + ((row >> 2) & 15) * 2 + (row & 1)
    perm = jnp.where(goal == col, 1.0, 0.0).astype(BF16)
    lsend[...] = jnp.dot(lf[...].astype(BF16), perm, preferred_element_type=F32).astype(BF16)
    for pj, dev in peers:
        rcopy(lsend, lrecv.at[j], l_ss.at[pj], l_rs.at[j], dev).start()
    lrecv[pl.ds(j, 1)] = lsend[...][None]

    term = lax.broadcasted_iota(jnp.int32, (terms, terms * BW), 0)
    lane = lax.broadcasted_iota(jnp.int32, (terms, terms * BW), 1)
    spread = jnp.where((lane >> 5) == term, 1.0, 0.0).astype(BF16)
    for q in range(PAIR):
        wv[q * 16 : q * 16 + PAIR] = jnp.dot(op_ref[q], spread, preferred_element_type=F32)
    vb[...] = jnp.zeros_like(vb)

    for pj, dev in peers:
        rcopy(psend.at[pj], precv.at[pj], p_ss.at[pj], p_rs.at[pj], dev).wait()
    square = precv[0, ROW0]
    for s in range(1, NS):
        square = square + precv[s, ROW0]
    square = jnp.where(lax.broadcasted_iota(jnp.int32, ROWVEC, 1) >= 96, square, 0.0)
    square = square + pltpu.roll(square, 64, 1)
    square = square + pltpu.roll(square, 32, 1)
    for s in range(NS):
        for k in QUAD:
            mt[span(k * NS + s, 2)] = precv[s, span(k, 2)]
    flat = mt[...].T
    gbuf[0, pl.ds(i, 1)] = block((flat[span(0, BW)], flat[span(1, BW)]), pack_last(flat[span(2, BW)]))[None]
    start_gather(0, 0)
    start_gather(0, 1)
    zero = jnp.zeros(ROWVEC, F32)
    start_line(0, [zero, zero, zero, square, zero])

    load_right.wait()
    for part in range(terms * BW // 128):
        rows = rt[span(part, 4)].reshape(128, rt.shape[2])
        r2[:, span(part, LANES)] = rows.T

    relay(0, 0)
    relay(0, 1)
    for pj, dev in peers:
        rcopy(lsend, lrecv.at[pj], l_ss.at[pj], l_rs.at[pj], dev).wait()
    mine = lrecv[...].reshape(NS * terms * 2, left_dim)
    width = 256
    row = lax.broadcasted_iota(jnp.int32, (NS * terms * 2, width), 0)
    col = lax.broadcasted_iota(jnp.int32, (NS * terms * 2, width), 1)
    shift = terms.bit_length()
    goal = ((row & (2 * terms - 1)) >> 1) * BW + (row >> shift) * 2 + (row & 1)
    for part in range(terms * BW // width):
        perm = jnp.where(goal == col + part * width, 1.0, 0.0).astype(BF16)
        lt[:, span(part, width)] = lax.dot_general(
            mine, perm, (((0,), (0,)), ((), ())), preferred_element_type=F32
        ).astype(BF16)
    finish_gather(0)
    alpha, beta = finish_line(0)
    update(0, zero, zero, beta, 0, ng)

    def first_rows():
        for grp, lanes in GROUPS:
            for q in range(PAIR):
                vec_ref[0, q, :, lanes] = psi_ref[q, :, lanes] / beta

    product(0, 1, True, first_rows)

    def step(t, beta_prev):
        par = t % 2
        start_plane(par, beta_prev)
        start_out(par)
        relay(par, 0)
        start_line(par, finish_plane())
        relay(par, 1)
        finish_out(t)
        finish_gather(par)
        alpha, beta = finish_line(par)
        update(par, alpha, beta_prev, beta, 0, ng)

        def rest():
            ab_ref[0, t - 1] = alpha[0, 0]
            ab_ref[1, t - 1] = beta[0, 0]
            own_rows(t, alpha, beta_prev, beta)

        product(par, 1 - par, t < NUM_STEPS - 1, rest)
        return beta

    beta_prev = lax.fori_loop(1, NUM_STEPS, step, zero)
    par = NUM_STEPS % 2
    start_plane(par, beta_prev)
    start_out(par)
    start_line(par, finish_plane())
    finish_out(NUM_STEPS)
    alpha, beta = finish_line(par)
    ab_ref[0, NUM_STEPS - 1] = alpha[0, 0]
    ab_ref[1, NUM_STEPS - 1] = beta[0, 0]
    own_rows(NUM_STEPS, alpha, beta_prev, beta)


def vmem(n):
    return [pl.BlockSpec(memory_space=pltpu.VMEM)] * n


def dma(*shape):
    return pltpu.SemaphoreType.DMA(shape)


def solution(mesh):
    nz = mesh.shape[ROW] // (NS * NC)
    ng = nz * NC

    def local_run(wave_rows, left_rows, op_pair, right_env):
        terms, rows, left_dim = left_rows.shape
        right_dim = right_env.shape[1]
        count = left_dim * right_dim * PAIR
        nv = NUM_STEPS + 1
        smem = pl.BlockSpec(memory_space=pltpu.SMEM)
        vecs, ab = pl.pallas_call(
            functools.partial(main_kernel, nz, float(count)),
            out_shape=(
                jax.ShapeDtypeStruct((nv, PAIR, rows, right_dim), F32),
                jax.ShapeDtypeStruct((2, NUM_STEPS), F32),
            ),
            in_specs=vmem(3) + [pl.BlockSpec(memory_space=pl.ANY)],
            out_specs=(vmem(1)[0], smem),
            scratch_shapes=[
                pltpu.VMEM((2, ng, BLK, LANES), F32),
                pltpu.VMEM((2, ng, BLK, LANES), F32),
                pltpu.VMEM((PAIR * BW, left_dim), BF16),
                pltpu.VMEM((PAIR * BW, terms * BW), F32),
                pltpu.VMEM((terms * BW, 384), BF16),
                pltpu.VMEM((NS, BLK, LANES), F32),
                pltpu.VMEM((NS, BLK, LANES), F32),
                pltpu.VMEM((NS, *TILE), F32),
                pltpu.VMEM(TILE, F32),
                pltpu.VMEM((2, ng, *TILE), F32),
                pltpu.VMEM((left_dim, terms * BW), BF16),
                pltpu.VMEM((right_dim, terms * BW), BF16),
                pltpu.VMEM((PAIR * 16, terms * BW), F32),
                pltpu.VMEM((terms * rows, left_dim), F32),
                pltpu.VMEM((terms * rows, left_dim), BF16),
                pltpu.VMEM((NS, terms * rows, left_dim), BF16),
                pltpu.VMEM((terms, BW, right_dim), BF16),
                pltpu.VMEM((NS, *TILE), F32),
                pltpu.VMEM((NS, *TILE), F32),
                pltpu.VMEM((NS, *TILE), F32),
                pltpu.VMEM((NS, *TILE), F32),
                pltpu.VMEM((128, 128), F32),
                dma(2, nz), dma(2, nz), dma(4, ng), dma(2, NS), dma(2, NS), dma(NS), dma(NS), dma(ng), dma(2, ng),
                dma(NS), dma(NS), dma(NS), dma(NS), dma(NS), dma(NS), pltpu.SemaphoreType.DMA,
            ],
            compiler_params=pltpu.CompilerParams(
                collective_id=0, has_side_effects=True, vmem_limit_bytes=56 * 1024 * 1024
            ),
            name="lanczos",
        )(
            wave_rows.transpose(1, 2, 0, 3).reshape(PAIR, rows, right_dim),
            left_rows,
            op_pair.transpose(1, 2, 0),
            right_env,
        )
        vecs = vecs.reshape(nv, 3, 3, rows, right_dim).transpose(0, 3, 1, 2, 4)
        return vecs, ab[0], ab[1]

    return jax.shard_map(
        local_run,
        mesh=mesh,
        in_specs=(P(ROW), P(None, ROW), P(), P()),
        out_specs=(P(None, ROW), P(), P()),
        check_vma=False,
    )
```

```python
import functools

import jax
import jax.numpy as jnp
from jax import lax
from jax.experimental import pallas as pl
from jax.experimental.pallas import tpu as pltpu
from jax.sharding import PartitionSpec as P

NUM_STEPS = 6
ROW = "rows"
NY, NX, NC = 4, 4, 2
NS = NY * NX
PAIR = 9
BW = 32
BLK = 72
HALVES = (slice(0, 32), slice(32, 72))
LANES = 128
TILE, ROWVEC = (8, LANES), (1, LANES)
PAIRED, QUAD = range(2), range(4)
MESH = pl.DeviceIdType.MESH
F32, BF16 = jnp.float32, jnp.bfloat16
OFFSETS = sorted(
    [(dy, dx) for dy in range(NY) for dx in range(NX) if (dy, dx) != (0, 0)],
    key=lambda o: (-(min(o[0], NY - o[0]) + min(o[1], NX - o[1])), o),
)


def span(k, width):
    return slice(k * width, k * width + width)


GROUPS = [(k, span(k, LANES)) for k in QUAD]
ROW0, ROW1, ROW2, ROW3, ROW4 = [span(k, 1) for k in range(5)]


def place():
    me = lax.axis_index(ROW)
    return me // (NS * NC), (me // (NX * NC)) % NY, (me // NC) % NX, me % NC


def device(z, y, x, core):
    return ((z * NY + y) * NX + x) * NC + core


def rcopy(src, dst, send_sem, recv_sem, dev):
    return pltpu.make_async_remote_copy(
        src_ref=src, dst_ref=dst, send_sem=send_sem, recv_sem=recv_sem, device_id=(dev,), device_id_type=MESH
    )


def knock(devs):
    for dev in devs:
        pl.semaphore_signal(pltpu.get_barrier_semaphore(), inc=1, device_id=(dev,), device_id_type=MESH)


def enter(devs):
    pl.semaphore_wait(pltpu.get_barrier_semaphore(), len(devs))


def plane_peers(z, y, x, core):
    out = []
    for dy, dx in OFFSETS:
        py, px = (y + dy) % NY, (x + dx) % NX
        out.append((py * NX + px, device(z, py, px, core)))
    return out


def swap4(a, b, c, d):
    lane = lax.broadcasted_iota(jnp.int32, a.shape, 1)
    low = lane < 64
    even = (lane // 32) % 2 == 0
    a, c = jnp.where(low, a, pltpu.roll(c, 64, 1)), jnp.where(low, pltpu.roll(a, 64, 1), c)
    b, d = jnp.where(low, b, pltpu.roll(d, 64, 1)), jnp.where(low, pltpu.roll(b, 64, 1), d)
    a, b = jnp.where(even, a, pltpu.roll(b, 32, 1)), jnp.where(even, pltpu.roll(a, 96, 1), b)
    c, d = jnp.where(even, c, pltpu.roll(d, 32, 1)), jnp.where(even, pltpu.roll(c, 96, 1), d)
    return a, b, c, d


def fold(val):
    return jnp.sum(val.reshape(BLK // 8, *TILE), axis=0)


def total(val):
    one = jnp.sum(jnp.sum(val, axis=0, keepdims=True), axis=1, keepdims=True)
    return jnp.broadcast_to(one, ROWVEC)


def block(main, last):
    return jnp.concatenate([main[0], main[1], last], axis=0)


def pack_last(rows):
    grp = lax.broadcasted_iota(jnp.int32, TILE, 1) // 32
    packed = rows[0:8]
    for t in range(1, 4):
        packed = jnp.where(grp == t, pltpu.roll(rows[span(t, 8)], 32 * t, 1), packed)
    return packed


def unpack_last(tile):
    return jnp.concatenate([tile if t == 0 else pltpu.roll(tile, 128 - 32 * t, 1) for t in QUAD], axis=0)


def rows5(vals):
    row = lax.broadcasted_iota(jnp.int32, TILE, 0)
    tile = vals[4]
    for k in (3, 2, 1, 0):
        tile = jnp.where(row == k, vals[k], tile)
    return jnp.broadcast_to(tile, TILE)


def ratio(num, den):
    some = den > 0.0
    return jnp.where(some, num / jnp.where(some, den, 1.0), 0.0)


def main_kernel(
    nz, count, psi_ref, left_ref, op_ref, right_ref, vec_ref, ab_ref,
    gbuf, vb, ut, xt, y2, sbuf, rbuf, abuf, asend, cbuf, lt, r2, wv, lf, lsend, lrecv, rt, psend, precv, osend, orecv, mt,
    g_ss, d_ss, g_rs, r_ss, r_rs, a_ss, a_rs, c_ss, c_rs, l_ss, l_rs, p_ss, p_rs, o_ss, o_rs, rt_sem,
):
    ng = nz * NC
    terms = left_ref.shape[0]
    left_dim = left_ref.shape[2]
    z, y, x, core = place()
    i, j = core * nz + z, y * NX + x
    peers = plane_peers(z, y, x, core)
    mate = device(z, y, x, 1 - core)
    zs = [((z + dz) % nz, dz) for dz in sorted(range(1, nz), key=lambda dz: (min(dz, nz - dz), dz))]
    line = [(core, pz, dz) for pz, dz in zs] + [(1 - core, pz, nz + dz) for pz, dz in zs] + [(1 - core, z, nz)]

    load_right = pltpu.make_async_copy(right_ref.at[:, pl.ds(pl.multiple_of(j * BW, BW), BW), :], rt, rt_sem)
    load_right.start()
    others = [dev for _, dev in peers] + [device(pz, y, x, pc) for pc, pz, _ in line]
    knock(others)

    def start_gather(par, half):
        own = gbuf.at[par, i, HALVES[half]]
        for pz, dz in reversed(zs):
            rcopy(own, own, g_ss.at[half, dz], g_rs.at[2 * par + half, i], device(pz, y, x, core)).start()
        rcopy(own, own, g_ss.at[half, 0], g_rs.at[2 * par + half, i], mate).start()

    def relay(par, half):
        for pz, dz in zs:
            slot = core * nz + pz
            ref = gbuf.at[par, slot, HALVES[half]]
            rcopy(ref, ref, g_ss.at[half, dz], g_rs.at[2 * par + half, slot], mate).wait_recv()
            rcopy(ref, ref, d_ss.at[half, dz], g_rs.at[2 * par + half, slot], mate).start()

    def finish_gather(par):
        for half in PAIRED:
            for dz in range(nz):
                slot = (1 - core) * nz + (z + dz) % nz
                ref = gbuf.at[par, slot, HALVES[half]]
                rcopy(ref, ref, g_ss.at[half, 0], g_rs.at[2 * par + half, slot], mate).wait_recv()
    def drain_gather(par):
        for half in PAIRED:
            own = gbuf.at[par, i, HALVES[half]]
            rcopy(own, own, g_ss.at[half, 0], g_rs.at[2 * par + half, i], mate).wait_send()
            for pz, dz in zs:
                ref = gbuf.at[par, core * nz + pz, HALVES[half]]
                rcopy(own, own, g_ss.at[half, dz], g_rs.at[2 * par + half, i], mate).wait_send()
                rcopy(ref, ref, d_ss.at[half, dz], g_rs.at[2 * par + half, i], mate).wait_send()

    def start_line(par, vals):
        lane = lax.broadcasted_iota(jnp.int32, ROWVEC, 1)
        line_row = vals[4]
        for k in reversed(QUAD):
            line_row = jnp.where(lane == k, vals[k], line_row)
        cbuf[par, pl.ds(i, 1)] = line_row[None]
        own = cbuf.at[par, i]
        for pc, pz, k in line:
            rcopy(own, own, c_ss.at[k], c_rs.at[par, i], device(pz, y, x, pc)).start()

    def finish_line(par):
        own = cbuf.at[par, i]
        for pc, pz, k in line:
            slot = pc * nz + pz
            rcopy(own, cbuf.at[par, slot], c_ss.at[k], c_rs.at[par, slot], mate).wait()
        rows = jnp.concatenate([cbuf[par, s] for s in range(ng)], axis=0)
        lane = lax.broadcasted_iota(jnp.int32, rows.shape, 1)
        m, p, nn, ee, ev = [jnp.sum(jnp.where(lane == k, rows, 0.0), axis=1, keepdims=True) for k in range(5)]
        alpha = jnp.sum(m, axis=0, keepdims=True) / count
        off = p - alpha
        square = jnp.sum(ee + 2.0 * (off * ev) + (off * nn) * off, axis=0, keepdims=True)
        return jnp.broadcast_to(alpha, ROWVEC), jnp.broadcast_to(jnp.sqrt(square / count), ROWVEC)

    def start_plane(par, beta_prev):
        w, v, vp = gbuf[par, i], vb[1 - par, i], vb[par, i]
        rest = w - beta_prev * vp
        m, yv, nn = total(fold(w * v)), total(fold(rest * v)), total(fold(v * v))
        p = ratio(yv, nn)
        e = rest - p * v
        tile = rows5([m, p, nn, total(fold(e * e)), total(fold(e * v))])
        asend[...] = tile
        for pj, dev in peers:
            rcopy(asend, abuf.at[j], a_ss.at[pj], a_rs.at[j], dev).start()
        abuf[pl.ds(j, 1)] = tile[None]

    def finish_plane():
        for pj, dev in peers:
            rcopy(asend, abuf.at[pj], a_ss.at[pj], a_rs.at[pj], dev).wait()
        zero = jnp.zeros(ROWVEC, F32)
        m, nn, pn, ee, ev = zero, zero, zero, zero, zero
        for s in range(NS):
            m, nn, pn = m + abuf[s, ROW0], nn + abuf[s, ROW2], pn + abuf[s, ROW1] * abuf[s, ROW2]
        p = ratio(pn, nn)
        for s in range(NS):
            off = abuf[s, ROW1] - p
            ee = ee + (abuf[s, ROW3] + 2.0 * (off * abuf[s, ROW4]) + (off * abuf[s, ROW2]) * off)
            ev = ev + (abuf[s, ROW4] + off * abuf[s, ROW2])
        return [m, p, nn, ee, ev]

    def start_out(par):
        blk = gbuf[par, i]
        last = unpack_last(blk[64:72])
        mt[...] = jnp.concatenate([blk[:64], last, jnp.zeros((32, 128), F32)], axis=0).T
        for pj in range(NS):
            for k in QUAD:
                osend[pj, span(k, 2)] = mt[span(k * NS + pj, 2)]
        for pj, dev in peers:
            rcopy(osend.at[pj], orecv.at[j], o_ss.at[pj], o_rs.at[j], dev).start()
        orecv[pl.ds(j, 1)] = osend[pl.ds(j, 1)]

    def finish_out(num):
        for pj, dev in peers:
            rcopy(osend.at[pj], orecv.at[pj], o_ss.at[pj], o_rs.at[pj], dev).wait()
        for grp, lanes in GROUPS:
            outs = swap4(*[orecv[grp * 4 + k] for k in QUAD])
            for t in PAIRED:
                for k in QUAD:
                    vec_ref[num, 4 * t + k, :, lanes] = outs[t][span(k, 2)]
            vec_ref[num, 8, :, lanes] = outs[2][0:2]

    def own_rows(num, alpha, beta_prev, beta):
        older = num - 2 if isinstance(num, int) else jnp.maximum(num - 2, 0)
        for grp, lanes in GROUPS:
            for q in range(PAIR):
                w, v, vp = vec_ref[num, q, :, lanes], vec_ref[num - 1, q, :, lanes], vec_ref[older, q, :, lanes]
                vec_ref[num, q, :, lanes] = (w - alpha * v - beta_prev * vp) / beta

    def update(par, alpha, beta_prev, beta, first, size):
        def body(s, carry):
            w, v, vp = gbuf[par, s], vb[1 - par, s], vb[par, s]
            vb[par, pl.ds(s, 1)] = ((w - alpha * v - beta_prev * vp) / beta)[None]
            return carry

        lax.fori_loop(first, first + size, body, 0, unroll=4 if size > 1 else 1)

    def left_and_mix(par):
        for grp in range(ng // 4):
            lanes = span(grp, LANES)
            for t in PAIRED:
                outs = swap4(*[vb[par, grp * 4 + ii, span(t, BW)] for ii in QUAD])
                for k in QUAD:
                    q = 4 * t + k
                    ut[span(q, BW), lanes] = outs[k].astype(BF16)
            outs = swap4(*[vb[par, grp * 4 + ii, 64:72] for ii in QUAD])
            ut[256:272, lanes] = jnp.concatenate(outs[:2], axis=0).astype(BF16)
            ut[272:288, lanes] = jnp.concatenate(outs[2:], axis=0).astype(BF16)
        width = 256
        for part in range(terms * BW // width):
            cols = span(part, width)
            whole = jnp.dot(ut[...], lt[:, cols], preferred_element_type=F32).astype(BF16).astype(F32)
            xt[:, cols] = whole
            for sub in range(width // LANES):
                grp = part * (width // LANES) + sub
                mix(0, [whole[span(r, BW), span(sub, LANES)] for r in range(PAIR)], span(grp, LANES), grp * LANES)

    def mix(half, xs, lanes, first):
        def one(q):
            acc = wv[q * 16 : q * 16 + 1, lanes] * xs[0]
            for r in range(1, PAIR):
                acc = acc + wv[q * 16 + r : q * 16 + r + 1, lanes] * xs[r]
            return acc

        rows = [pl.ds(first + k * BW, BW) for k in QUAD]
        outs = swap4(*[one(4 * half + k) for k in QUAD])
        for k in QUAD:
            y2[rows[k], span(half, LANES)] = outs[k].astype(BF16)
        if half:
            last = one(8)
            for k in QUAD:
                moved = last if k == 0 else pltpu.roll(last, LANES - BW * k, 1)
                y2[rows[k], 2 * LANES :] = moved.astype(BF16)

    def mix_rest():
        def body(grp, carry):
            first = pl.multiple_of(grp * LANES, LANES)
            lanes = pl.ds(first, LANES)
            mix(1, [xt[span(r, BW), lanes] for r in range(PAIR)], lanes, first)
            return carry

        lax.fori_loop(0, terms * BW // LANES, body, 0, unroll=2)

    def start_scatter(half):
        cols = slice(0, 128) if half == 0 else slice(128, 384)
        for dy in (2, 1, 3, 0):
            py = (y + dy) % NY
            part = jnp.dot(
                r2[pl.ds(pl.multiple_of(py * 128, 128), 128), :], y2[:, cols], preferred_element_type=F32
            )
            for px in range(NX):
                pj = py * NX + px
                rows = part[span(px, BW)]
                if half == 0:
                    sbuf[pj, 0:32] = rows
                else:
                    sbuf[pj, 32:64] = rows[:, 0:128]
                    sbuf[pj, 64:72] = pack_last(rows[:, 128:256])
                send = rcopy(
                    sbuf.at[pj, HALVES[half]], rbuf.at[j, HALVES[half]],
                    r_ss.at[half, pj], r_rs.at[half, j], device(z, py, px, core),
                )
                if dy:
                    send.start()
                else:

                    @pl.when(px != x)
                    def _():
                        send.start()

        rbuf[pl.ds(j, 1), HALVES[half]] = sbuf[pl.ds(j, 1), HALVES[half]]

    def finish_scatter(nxt, half):
        for pj, dev in reversed(peers):
            rcopy(
                sbuf.at[pj, HALVES[half]], rbuf.at[pj, HALVES[half]], r_ss.at[half, pj], r_rs.at[half, pj], dev
            ).wait()
        w = rbuf[0, HALVES[half]]
        for s in range(1, NS):
            w = w + rbuf[s, HALVES[half]]
        gbuf[nxt, pl.ds(i, 1), HALVES[half]] = w[None]

    def product(par, nxt, more, between):
        left_and_mix(par)
        start_scatter(0)
        mix_rest()
        start_scatter(1)
        drain_gather(par)
        between()
        for half in PAIRED:
            finish_scatter(nxt, half)
            if more is True:
                start_gather(nxt, half)
            else:

                @pl.when(more)
                def _(half=half):
                    start_gather(nxt, half)

    norm = jnp.zeros(ROWVEC, F32)
    for grp, lanes in GROUPS:
        for q in range(PAIR):
            norm = norm + jnp.sum(psi_ref[q, :, lanes] * psi_ref[q, :, lanes], axis=0, keepdims=True)
    norm = jnp.broadcast_to(jnp.sum(norm, axis=1, keepdims=True), TILE)
    for t in range(3):
        mt[span(t, 8)] = jnp.zeros(TILE, F32)
    for grp, lanes in GROUPS:
        for q in range(PAIR):
            mt[span(q, 2)] = psi_ref[q, :, lanes]
        outs = swap4(mt[0:8], mt[8:16], mt[16:24], norm)
        for k in QUAD:
            psend[grp * 4 + k] = outs[k]
    enter(others)
    for pj, dev in peers:
        rcopy(psend.at[pj], precv.at[j], p_ss.at[pj], p_rs.at[j], dev).start()
    precv[pl.ds(j, 1)] = psend[pl.ds(j, 1)]

    for k in range(terms):
        lf[span(k, 2)] = left_ref[k].astype(F32)
    row = lax.broadcasted_iota(jnp.int32, (left_dim, left_dim), 0)
    col = lax.broadcasted_iota(jnp.int32, (left_dim, left_dim), 1)
    goal = ((row >> 1) & 1) * (nz * BW) + (row >> 6) * BW + ((row >> 2) & 15) * 2 + (row & 1)
    perm = jnp.where(goal == col, 1.0, 0.0).astype(BF16)
    lsend[...] = jnp.dot(lf[...].astype(BF16), perm, preferred_element_type=F32).astype(BF16)
    for pj, dev in peers:
        rcopy(lsend, lrecv.at[j], l_ss.at[pj], l_rs.at[j], dev).start()
    lrecv[pl.ds(j, 1)] = lsend[...][None]

    term = lax.broadcasted_iota(jnp.int32, (terms, terms * BW), 0)
    lane = lax.broadcasted_iota(jnp.int32, (terms, terms * BW), 1)
    spread = jnp.where((lane >> 5) == term, 1.0, 0.0).astype(BF16)
    for q in range(PAIR):
        wv[q * 16 : q * 16 + PAIR] = jnp.dot(op_ref[q], spread, preferred_element_type=F32)
    vb[...] = jnp.zeros_like(vb)

    for pj, dev in peers:
        rcopy(psend.at[pj], precv.at[pj], p_ss.at[pj], p_rs.at[pj], dev).wait()
    square = precv[0, ROW0]
    for s in range(1, NS):
        square = square + precv[s, ROW0]
    square = jnp.where(lax.broadcasted_iota(jnp.int32, ROWVEC, 1) >= 96, square, 0.0)
    square = square + pltpu.roll(square, 64, 1)
    square = square + pltpu.roll(square, 32, 1)
    for s in range(NS):
        for k in QUAD:
            mt[span(k * NS + s, 2)] = precv[s, span(k, 2)]
    flat = mt[...].T
    gbuf[0, pl.ds(i, 1)] = block((flat[span(0, BW)], flat[span(1, BW)]), pack_last(flat[span(2, BW)]))[None]
    start_gather(0, 0)
    start_gather(0, 1)
    zero = jnp.zeros(ROWVEC, F32)
    start_line(0, [zero, zero, zero, square, zero])

    load_right.wait()
    for part in range(terms * BW // 128):
        rows = rt[span(part, 4)].reshape(128, rt.shape[2])
        r2[:, span(part, LANES)] = rows.T

    relay(0, 0)
    for pj, dev in peers:
        rcopy(lsend, lrecv.at[pj], l_ss.at[pj], l_rs.at[pj], dev).wait()
    mine = lrecv[...].reshape(NS * terms * 2, left_dim)
    width = 256
    row = lax.broadcasted_iota(jnp.int32, (NS * terms * 2, width), 0)
    col = lax.broadcasted_iota(jnp.int32, (NS * terms * 2, width), 1)
    shift = terms.bit_length()
    goal = ((row & (2 * terms - 1)) >> 1) * BW + (row >> shift) * 2 + (row & 1)
    for part in range(terms * BW // width):
        perm = jnp.where(goal == col + part * width, 1.0, 0.0).astype(BF16)
        lt[:, span(part, width)] = lax.dot_general(
            mine, perm, (((0,), (0,)), ((), ())), preferred_element_type=F32
        ).astype(BF16)
    relay(0, 1)
    finish_gather(0)
    alpha, beta = finish_line(0)
    update(0, zero, zero, beta, 0, ng)

    def first_rows():
        for grp, lanes in GROUPS:
            for q in range(PAIR):
                vec_ref[0, q, :, lanes] = psi_ref[q, :, lanes] / beta

    product(0, 1, True, first_rows)

    def step(t, beta_prev):
        par = t % 2
        start_plane(par, beta_prev)
        start_out(par)
        relay(par, 0)
        start_line(par, finish_plane())
        relay(par, 1)
        finish_out(t)
        finish_gather(par)
        alpha, beta = finish_line(par)
        update(par, alpha, beta_prev, beta, 0, ng)

        def rest():
            ab_ref[0, t - 1] = alpha[0, 0]
            ab_ref[1, t - 1] = beta[0, 0]
            own_rows(t, alpha, beta_prev, beta)

        product(par, 1 - par, t < NUM_STEPS - 1, rest)
        return beta

    beta_prev = lax.fori_loop(1, NUM_STEPS, step, zero)
    par = NUM_STEPS % 2
    start_plane(par, beta_prev)
    start_out(par)
    start_line(par, finish_plane())
    finish_out(NUM_STEPS)
    alpha, beta = finish_line(par)
    ab_ref[0, NUM_STEPS - 1] = alpha[0, 0]
    ab_ref[1, NUM_STEPS - 1] = beta[0, 0]
    own_rows(NUM_STEPS, alpha, beta_prev, beta)


def vmem(n):
    return [pl.BlockSpec(memory_space=pltpu.VMEM)] * n


def dma(*shape):
    return pltpu.SemaphoreType.DMA(shape)


def solution(mesh):
    nz = mesh.shape[ROW] // (NS * NC)
    ng = nz * NC

    def local_run(wave_rows, left_rows, op_pair, right_env):
        terms, rows, left_dim = left_rows.shape
        right_dim = right_env.shape[1]
        count = left_dim * right_dim * PAIR
        nv = NUM_STEPS + 1
        smem = pl.BlockSpec(memory_space=pltpu.SMEM)
        vecs, ab = pl.pallas_call(
            functools.partial(main_kernel, nz, float(count)),
            out_shape=(
                jax.ShapeDtypeStruct((nv, PAIR, rows, right_dim), F32),
                jax.ShapeDtypeStruct((2, NUM_STEPS), F32),
            ),
            in_specs=vmem(3) + [pl.BlockSpec(memory_space=pl.ANY)],
            out_specs=(vmem(1)[0], smem),
            scratch_shapes=[
                pltpu.VMEM((2, ng, BLK, LANES), F32),
                pltpu.VMEM((2, ng, BLK, LANES), F32),
                pltpu.VMEM((PAIR * BW, left_dim), BF16),
                pltpu.VMEM((PAIR * BW, terms * BW), F32),
                pltpu.VMEM((terms * BW, 384), BF16),
                pltpu.VMEM((NS, BLK, LANES), F32),
                pltpu.VMEM((NS, BLK, LANES), F32),
                pltpu.VMEM((NS, *TILE), F32),
                pltpu.VMEM(TILE, F32),
                pltpu.VMEM((2, ng, *ROWVEC), F32),
                pltpu.VMEM((left_dim, terms * BW), BF16),
                pltpu.VMEM((right_dim, terms * BW), BF16),
                pltpu.VMEM((PAIR * 16, terms * BW), F32),
                pltpu.VMEM((terms * rows, left_dim), F32),
                pltpu.VMEM((terms * rows, left_dim), BF16),
                pltpu.VMEM((NS, terms * rows, left_dim), BF16),
                pltpu.VMEM((terms, BW, right_dim), BF16),
                pltpu.VMEM((NS, *TILE), F32),
                pltpu.VMEM((NS, *TILE), F32),
                pltpu.VMEM((NS, *TILE), F32),
                pltpu.VMEM((NS, *TILE), F32),
                pltpu.VMEM((128, 128), F32),
                dma(2, nz), dma(2, nz), dma(4, ng), dma(2, NS), dma(2, NS), dma(NS), dma(NS), dma(ng), dma(2, ng),
                dma(NS), dma(NS), dma(NS), dma(NS), dma(NS), dma(NS), pltpu.SemaphoreType.DMA,
            ],
            compiler_params=pltpu.CompilerParams(
                collective_id=0, has_side_effects=True, vmem_limit_bytes=56 * 1024 * 1024
            ),
            name="lanczos",
        )(
            wave_rows.transpose(1, 2, 0, 3).reshape(PAIR, rows, right_dim),
            left_rows,
            op_pair.transpose(1, 2, 0),
            right_env,
        )
        vecs = vecs.reshape(nv, 3, 3, rows, right_dim).transpose(0, 3, 1, 2, 4)
        return vecs, ab[0], ab[1]

    return jax.shard_map(
        local_run,
        mesh=mesh,
        in_specs=(P(ROW), P(None, ROW), P(), P()),
        out_specs=(P(None, ROW), P(), P()),
        check_vma=False,
    )
```

```python
import functools

import jax
import jax.numpy as jnp
from jax import lax
from jax.experimental import pallas as pl
from jax.experimental.pallas import tpu as pltpu
from jax.sharding import PartitionSpec as P

NUM_STEPS = 6
ROW = "rows"
NY, NX, NC = 4, 4, 2
NS = NY * NX
PAIR = 9
BW = 32
BLK = 72
HALVES = (slice(0, 32), slice(32, 72))
LANES = 128
TILE, ROWVEC = (8, LANES), (1, LANES)
PAIRED, QUAD = range(2), range(4)
MESH = pl.DeviceIdType.MESH
F32, BF16 = jnp.float32, jnp.bfloat16
OFFSETS = sorted(
    [(dy, dx) for dy in range(NY) for dx in range(NX) if (dy, dx) != (0, 0)],
    key=lambda o: (-(min(o[0], NY - o[0]) + min(o[1], NX - o[1])), o),
)


def span(k, width):
    return slice(k * width, k * width + width)


GROUPS = [(k, span(k, LANES)) for k in QUAD]
ROW0, ROW1, ROW2, ROW3, ROW4 = [span(k, 1) for k in range(5)]


def place():
    me = lax.axis_index(ROW)
    return me // (NS * NC), (me // (NX * NC)) % NY, (me // NC) % NX, me % NC


def device(z, y, x, core):
    return ((z * NY + y) * NX + x) * NC + core


def rcopy(src, dst, send_sem, recv_sem, dev):
    return pltpu.make_async_remote_copy(
        src_ref=src, dst_ref=dst, send_sem=send_sem, recv_sem=recv_sem, device_id=(dev,), device_id_type=MESH
    )


def knock(devs):
    for dev in devs:
        pl.semaphore_signal(pltpu.get_barrier_semaphore(), inc=1, device_id=(dev,), device_id_type=MESH)


def enter(devs):
    pl.semaphore_wait(pltpu.get_barrier_semaphore(), len(devs))


def plane_peers(z, y, x, core):
    out = []
    for dy, dx in OFFSETS:
        py, px = (y + dy) % NY, (x + dx) % NX
        out.append((py * NX + px, device(z, py, px, core)))
    return out


def swap4(a, b, c, d):
    lane = lax.broadcasted_iota(jnp.int32, a.shape, 1)
    low = lane < 64
    even = (lane // 32) % 2 == 0
    a, c = jnp.where(low, a, pltpu.roll(c, 64, 1)), jnp.where(low, pltpu.roll(a, 64, 1), c)
    b, d = jnp.where(low, b, pltpu.roll(d, 64, 1)), jnp.where(low, pltpu.roll(b, 64, 1), d)
    a, b = jnp.where(even, a, pltpu.roll(b, 32, 1)), jnp.where(even, pltpu.roll(a, 96, 1), b)
    c, d = jnp.where(even, c, pltpu.roll(d, 32, 1)), jnp.where(even, pltpu.roll(c, 96, 1), d)
    return a, b, c, d


def fold(val):
    return jnp.sum(val.reshape(BLK // 8, *TILE), axis=0)


def total(val):
    one = jnp.sum(jnp.sum(val, axis=0, keepdims=True), axis=1, keepdims=True)
    return jnp.broadcast_to(one, ROWVEC)


def block(main, last):
    return jnp.concatenate([main[0], main[1], last], axis=0)


def pack_last(rows):
    grp = lax.broadcasted_iota(jnp.int32, TILE, 1) // 32
    packed = rows[0:8]
    for t in range(1, 4):
        packed = jnp.where(grp == t, pltpu.roll(rows[span(t, 8)], 32 * t, 1), packed)
    return packed


def unpack_last(tile):
    return jnp.concatenate([tile if t == 0 else pltpu.roll(tile, 128 - 32 * t, 1) for t in QUAD], axis=0)


def rows5(vals):
    row = lax.broadcasted_iota(jnp.int32, TILE, 0)
    tile = vals[4]
    for k in (3, 2, 1, 0):
        tile = jnp.where(row == k, vals[k], tile)
    return jnp.broadcast_to(tile, TILE)


def ratio(num, den):
    some = den > 0.0
    return jnp.where(some, num / jnp.where(some, den, 1.0), 0.0)


def main_kernel(
    nz, count, psi_ref, left_ref, op_ref, right_ref, vec_ref, ab_ref,
    gbuf, vb, ut, xt, y2, sbuf, rbuf, abuf, asend, cbuf, lt, r2, wv, lf, lsend, lrecv, rt, psend, precv, osend, orecv, mt,
    g_ss, d_ss, g_rs, r_ss, r_rs, a_ss, a_rs, c_ss, c_rs, l_ss, l_rs, p_ss, p_rs, o_ss, o_rs, rt_sem,
):
    ng = nz * NC
    terms = left_ref.shape[0]
    left_dim = left_ref.shape[2]
    z, y, x, core = place()
    i, j = core * nz + z, y * NX + x
    peers = plane_peers(z, y, x, core)
    mate = device(z, y, x, 1 - core)
    zs = [((z + dz) % nz, dz) for dz in sorted(range(1, nz), key=lambda dz: (min(dz, nz - dz), dz))]
    line = [(core, pz, dz) for pz, dz in zs] + [(1 - core, pz, nz + dz) for pz, dz in zs] + [(1 - core, z, nz)]

    load_right = pltpu.make_async_copy(right_ref.at[:, pl.ds(pl.multiple_of(j * BW, BW), BW), :], rt, rt_sem)
    load_right.start()
    others = [dev for _, dev in peers] + [device(pz, y, x, pc) for pc, pz, _ in line]
    knock(others)

    def start_gather(par, half):
        own = gbuf.at[par, i, HALVES[half]]
        for pz, dz in reversed(zs):
            rcopy(own, own, g_ss.at[half, dz], g_rs.at[2 * par + half, i], device(pz, y, x, core)).start()
        rcopy(own, own, g_ss.at[half, 0], g_rs.at[2 * par + half, i], mate).start()

    def relay(par, half):
        for pz, dz in zs:
            slot = core * nz + pz
            ref = gbuf.at[par, slot, HALVES[half]]
            rcopy(ref, ref, g_ss.at[half, dz], g_rs.at[2 * par + half, slot], mate).wait_recv()
            rcopy(ref, ref, d_ss.at[half, dz], g_rs.at[2 * par + half, slot], mate).start()

    def finish_gather(par):
        for half in PAIRED:
            for dz in range(nz):
                slot = (1 - core) * nz + (z + dz) % nz
                ref = gbuf.at[par, slot, HALVES[half]]
                rcopy(ref, ref, g_ss.at[half, 0], g_rs.at[2 * par + half, slot], mate).wait_recv()
    def drain_gather(par):
        for half in PAIRED:
            own = gbuf.at[par, i, HALVES[half]]
            rcopy(own, own, g_ss.at[half, 0], g_rs.at[2 * par + half, i], mate).wait_send()
            for pz, dz in zs:
                ref = gbuf.at[par, core * nz + pz, HALVES[half]]
                rcopy(own, own, g_ss.at[half, dz], g_rs.at[2 * par + half, i], mate).wait_send()
                rcopy(ref, ref, d_ss.at[half, dz], g_rs.at[2 * par + half, i], mate).wait_send()

    def start_line(par, vals):
        lane = lax.broadcasted_iota(jnp.int32, ROWVEC, 1)
        line_row = vals[4]
        for k in reversed(QUAD):
            line_row = jnp.where(lane == k, vals[k], line_row)
        cbuf[par, pl.ds(i, 1)] = line_row[None]
        own = cbuf.at[par, i]
        for pc, pz, k in line:
            rcopy(own, own, c_ss.at[k], c_rs.at[par, i], device(pz, y, x, pc)).start()

    def finish_line(par):
        own = cbuf.at[par, i]
        for pc, pz, k in line:
            slot = pc * nz + pz
            rcopy(own, cbuf.at[par, slot], c_ss.at[k], c_rs.at[par, slot], mate).wait()
        rows = jnp.concatenate([cbuf[par, s] for s in range(ng)], axis=0)
        lane = lax.broadcasted_iota(jnp.int32, rows.shape, 1)
        m, p, nn, ee, ev = [jnp.sum(jnp.where(lane == k, rows, 0.0), axis=1, keepdims=True) for k in range(5)]
        alpha = jnp.sum(m, axis=0, keepdims=True) / count
        off = p - alpha
        square = jnp.sum(ee + 2.0 * (off * ev) + (off * nn) * off, axis=0, keepdims=True)
        return jnp.broadcast_to(alpha, ROWVEC), jnp.broadcast_to(jnp.sqrt(square / count), ROWVEC)

    def start_plane(par, beta_prev):
        w, v, vp = gbuf[par, i], vb[1 - par, i], vb[par, i]
        rest = w - beta_prev * vp
        m, yv, nn = total(fold(w * v)), total(fold(rest * v)), total(fold(v * v))
        p = ratio(yv, nn)
        e = rest - p * v
        tile = rows5([m, p, nn, total(fold(e * e)), total(fold(e * v))])
        asend[...] = tile
        for pj, dev in peers:
            rcopy(asend, abuf.at[j], a_ss.at[pj], a_rs.at[j], dev).start()
        abuf[pl.ds(j, 1)] = tile[None]

    def finish_plane():
        for pj, dev in peers:
            rcopy(asend, abuf.at[pj], a_ss.at[pj], a_rs.at[pj], dev).wait()
        zero = jnp.zeros(ROWVEC, F32)
        m, nn, pn, ee, ev = zero, zero, zero, zero, zero
        for s in range(NS):
            m, nn, pn = m + abuf[s, ROW0], nn + abuf[s, ROW2], pn + abuf[s, ROW1] * abuf[s, ROW2]
        p = ratio(pn, nn)
        for s in range(NS):
            off = abuf[s, ROW1] - p
            ee = ee + (abuf[s, ROW3] + 2.0 * (off * abuf[s, ROW4]) + (off * abuf[s, ROW2]) * off)
            ev = ev + (abuf[s, ROW4] + off * abuf[s, ROW2])
        return [m, p, nn, ee, ev]

    def start_out(par):
        blk = gbuf[par, i]
        last = unpack_last(blk[64:72])
        mt[...] = jnp.concatenate([blk[:64], last, jnp.zeros((32, 128), F32)], axis=0).T
        for pj in range(NS):
            for k in QUAD:
                osend[pj, span(k, 2)] = mt[span(k * NS + pj, 2)]
        for pj, dev in peers:
            rcopy(osend.at[pj], orecv.at[j], o_ss.at[pj], o_rs.at[j], dev).start()
        orecv[pl.ds(j, 1)] = osend[pl.ds(j, 1)]

    def finish_out(num):
        for pj, dev in peers:
            rcopy(osend.at[pj], orecv.at[pj], o_ss.at[pj], o_rs.at[pj], dev).wait()
        for grp, lanes in GROUPS:
            outs = swap4(*[orecv[grp * 4 + k] for k in QUAD])
            for t in PAIRED:
                for k in QUAD:
                    vec_ref[num, 4 * t + k, :, lanes] = outs[t][span(k, 2)]
            vec_ref[num, 8, :, lanes] = outs[2][0:2]

    def own_rows(num, alpha, beta_prev, beta):
        older = num - 2 if isinstance(num, int) else jnp.maximum(num - 2, 0)
        for grp, lanes in GROUPS:
            for q in range(PAIR):
                w, v, vp = vec_ref[num, q, :, lanes], vec_ref[num - 1, q, :, lanes], vec_ref[older, q, :, lanes]
                vec_ref[num, q, :, lanes] = (w - alpha * v - beta_prev * vp) / beta

    def update(par, alpha, beta_prev, beta, first, size):
        def body(s, carry):
            w, v, vp = gbuf[par, s], vb[1 - par, s], vb[par, s]
            vb[par, pl.ds(s, 1)] = ((w - alpha * v - beta_prev * vp) / beta)[None]
            return carry

        lax.fori_loop(first, first + size, body, 0, unroll=4 if size > 1 else 1)

    def left_and_mix(par):
        for grp in range(ng // 4):
            lanes = span(grp, LANES)
            for t in PAIRED:
                outs = swap4(*[vb[par, grp * 4 + ii, span(t, BW)] for ii in QUAD])
                for k in QUAD:
                    q = 4 * t + k
                    ut[span(q, BW), lanes] = outs[k].astype(BF16)
            outs = swap4(*[vb[par, grp * 4 + ii, 64:72] for ii in QUAD])
            ut[256:272, lanes] = jnp.concatenate(outs[:2], axis=0).astype(BF16)
            ut[272:288, lanes] = jnp.concatenate(outs[2:], axis=0).astype(BF16)
        width = 256
        for part in range(terms * BW // width):
            cols = span(part, width)
            whole = jnp.dot(ut[...], lt[:, cols], preferred_element_type=F32).astype(BF16).astype(F32)
            xt[:, cols] = whole
            for sub in range(width // LANES):
                grp = part * (width // LANES) + sub
                mix(0, grp, [whole[span(r, BW), span(sub, LANES)] for r in range(PAIR)])

    def mix(half, grp, xs):
        lanes = span(grp, LANES)
        for part in PAIRED:
            some = [x_r[span(part, 16)] for x_r in xs]

            def one(q):
                acc = wv[q * 16 : q * 16 + 1, lanes] * some[0]
                for r in range(1, PAIR):
                    acc = acc + wv[q * 16 + r : q * 16 + r + 1, lanes] * some[r]
                return acc

            rows = [span(grp * 8 + 2 * k + part, 16) for k in QUAD]
            outs = swap4(*[one(4 * half + k) for k in QUAD])
            for k in QUAD:
                y2[rows[k], span(half, LANES)] = outs[k].astype(BF16)
            if half:
                last = one(8)
                for k in QUAD:
                    moved = last if k == 0 else pltpu.roll(last, LANES - BW * k, 1)
                    y2[rows[k], 2 * LANES :] = moved.astype(BF16)

    def mix_rest():
        for grp in range(terms * BW // LANES):
            mix(1, grp, [xt[span(r, BW), span(grp, LANES)] for r in range(PAIR)])

    def start_scatter(half):
        cols = slice(0, 128) if half == 0 else slice(128, 384)
        for dy in (2, 1, 3, 0):
            py = (y + dy) % NY
            part = jnp.dot(
                r2[pl.ds(pl.multiple_of(py * 128, 128), 128), :], y2[:, cols], preferred_element_type=F32
            )
            for px in range(NX):
                pj = py * NX + px
                rows = part[span(px, BW)]
                if half == 0:
                    sbuf[pj, 0:32] = rows
                else:
                    sbuf[pj, 32:64] = rows[:, 0:128]
                    sbuf[pj, 64:72] = pack_last(rows[:, 128:256])
                send = rcopy(
                    sbuf.at[pj, HALVES[half]], rbuf.at[j, HALVES[half]],
                    r_ss.at[half, pj], r_rs.at[half, j], device(z, py, px, core),
                )
                if dy:
                    send.start()
                else:

                    @pl.when(px != x)
                    def _():
                        send.start()

        rbuf[pl.ds(j, 1), HALVES[half]] = sbuf[pl.ds(j, 1), HALVES[half]]

    def finish_scatter(nxt, half):
        for pj, dev in reversed(peers):
            rcopy(
                sbuf.at[pj, HALVES[half]], rbuf.at[pj, HALVES[half]], r_ss.at[half, pj], r_rs.at[half, pj], dev
            ).wait()
        w = rbuf[0, HALVES[half]]
        for s in range(1, NS):
            w = w + rbuf[s, HALVES[half]]
        gbuf[nxt, pl.ds(i, 1), HALVES[half]] = w[None]

    def product(par, nxt, more, between):
        left_and_mix(par)
        start_scatter(0)
        mix_rest()
        start_scatter(1)
        drain_gather(par)
        between()
        for half in PAIRED:
            finish_scatter(nxt, half)
            if more is True:
                start_gather(nxt, half)
            else:

                @pl.when(more)
                def _(half=half):
                    start_gather(nxt, half)

    norm = jnp.zeros(ROWVEC, F32)
    for grp, lanes in GROUPS:
        for q in range(PAIR):
            norm = norm + jnp.sum(psi_ref[q, :, lanes] * psi_ref[q, :, lanes], axis=0, keepdims=True)
    norm = jnp.broadcast_to(jnp.sum(norm, axis=1, keepdims=True), TILE)
    for t in range(3):
        mt[span(t, 8)] = jnp.zeros(TILE, F32)
    for grp, lanes in GROUPS:
        for q in range(PAIR):
            mt[span(q, 2)] = psi_ref[q, :, lanes]
        outs = swap4(mt[0:8], mt[8:16], mt[16:24], norm)
        for k in QUAD:
            psend[grp * 4 + k] = outs[k]
    enter(others)
    for pj, dev in peers:
        rcopy(psend.at[pj], precv.at[j], p_ss.at[pj], p_rs.at[j], dev).start()
    precv[pl.ds(j, 1)] = psend[pl.ds(j, 1)]

    for k in range(terms):
        lf[span(k, 2)] = left_ref[k].astype(F32)
    row = lax.broadcasted_iota(jnp.int32, (left_dim, left_dim), 0)
    col = lax.broadcasted_iota(jnp.int32, (left_dim, left_dim), 1)
    goal = ((row >> 1) & 1) * (nz * BW) + (row >> 6) * BW + ((row >> 2) & 15) * 2 + (row & 1)
    perm = jnp.where(goal == col, 1.0, 0.0).astype(BF16)
    lsend[...] = jnp.dot(lf[...].astype(BF16), perm, preferred_element_type=F32).astype(BF16)
    for pj, dev in peers:
        rcopy(lsend, lrecv.at[j], l_ss.at[pj], l_rs.at[j], dev).start()
    lrecv[pl.ds(j, 1)] = lsend[...][None]

    term = lax.broadcasted_iota(jnp.int32, (terms, terms * BW), 0)
    lane = lax.broadcasted_iota(jnp.int32, (terms, terms * BW), 1)
    spread = jnp.where((lane >> 5) == term, 1.0, 0.0).astype(BF16)
    for q in range(PAIR):
        wv[q * 16 : q * 16 + PAIR] = jnp.dot(op_ref[q], spread, preferred_element_type=F32)
    vb[...] = jnp.zeros_like(vb)

    for pj, dev in peers:
        rcopy(psend.at[pj], precv.at[pj], p_ss.at[pj], p_rs.at[pj], dev).wait()
    square = precv[0, ROW0]
    for s in range(1, NS):
        square = square + precv[s, ROW0]
    square = jnp.where(lax.broadcasted_iota(jnp.int32, ROWVEC, 1) >= 96, square, 0.0)
    square = square + pltpu.roll(square, 64, 1)
    square = square + pltpu.roll(square, 32, 1)
    for s in range(NS):
        for k in QUAD:
            mt[span(k * NS + s, 2)] = precv[s, span(k, 2)]
    flat = mt[...].T
    gbuf[0, pl.ds(i, 1)] = block((flat[span(0, BW)], flat[span(1, BW)]), pack_last(flat[span(2, BW)]))[None]
    start_gather(0, 0)
    start_gather(0, 1)
    zero = jnp.zeros(ROWVEC, F32)
    start_line(0, [zero, zero, zero, square, zero])

    load_right.wait()
    for part in range(terms * BW // 128):
        rows = rt[span(part, 4)].reshape(128, rt.shape[2])
        r2[:, span(part, LANES)] = rows.T

    relay(0, 0)
    relay(0, 1)
    for pj, dev in peers:
        rcopy(lsend, lrecv.at[pj], l_ss.at[pj], l_rs.at[pj], dev).wait()
    mine = lrecv[...].reshape(NS * terms * 2, left_dim)
    width = 256
    row = lax.broadcasted_iota(jnp.int32, (NS * terms * 2, width), 0)
    col = lax.broadcasted_iota(jnp.int32, (NS * terms * 2, width), 1)
    shift = terms.bit_length()
    goal = ((row & (2 * terms - 1)) >> 1) * BW + (row >> shift) * 2 + (row & 1)
    for part in range(terms * BW // width):
        perm = jnp.where(goal == col + part * width, 1.0, 0.0).astype(BF16)
        lt[:, span(part, width)] = lax.dot_general(
            mine, perm, (((0,), (0,)), ((), ())), preferred_element_type=F32
        ).astype(BF16)
    finish_gather(0)
    alpha, beta = finish_line(0)
    update(0, zero, zero, beta, 0, ng)

    def first_rows():
        for grp, lanes in GROUPS:
            for q in range(PAIR):
                vec_ref[0, q, :, lanes] = psi_ref[q, :, lanes] / beta

    product(0, 1, True, first_rows)

    def step(t, beta_prev):
        par = t % 2
        start_plane(par, beta_prev)
        start_out(par)
        relay(par, 0)
        start_line(par, finish_plane())
        relay(par, 1)
        finish_out(t)
        finish_gather(par)
        alpha, beta = finish_line(par)
        update(par, alpha, beta_prev, beta, 0, ng)

        def rest():
            ab_ref[0, t - 1] = alpha[0, 0]
            ab_ref[1, t - 1] = beta[0, 0]
            own_rows(t, alpha, beta_prev, beta)

        product(par, 1 - par, t < NUM_STEPS - 1, rest)
        return beta

    beta_prev = lax.fori_loop(1, NUM_STEPS, step, zero)
    par = NUM_STEPS % 2
    start_plane(par, beta_prev)
    start_out(par)
    start_line(par, finish_plane())
    finish_out(NUM_STEPS)
    alpha, beta = finish_line(par)
    ab_ref[0, NUM_STEPS - 1] = alpha[0, 0]
    ab_ref[1, NUM_STEPS - 1] = beta[0, 0]
    own_rows(NUM_STEPS, alpha, beta_prev, beta)


def vmem(n):
    return [pl.BlockSpec(memory_space=pltpu.VMEM)] * n


def dma(*shape):
    return pltpu.SemaphoreType.DMA(shape)


def solution(mesh):
    nz = mesh.shape[ROW] // (NS * NC)
    ng = nz * NC

    def local_run(wave_rows, left_rows, op_pair, right_env):
        terms, rows, left_dim = left_rows.shape
        right_dim = right_env.shape[1]
        count = left_dim * right_dim * PAIR
        nv = NUM_STEPS + 1
        smem = pl.BlockSpec(memory_space=pltpu.SMEM)
        vecs, ab = pl.pallas_call(
            functools.partial(main_kernel, nz, float(count)),
            out_shape=(
                jax.ShapeDtypeStruct((nv, PAIR, rows, right_dim), F32),
                jax.ShapeDtypeStruct((2, NUM_STEPS), F32),
            ),
            in_specs=vmem(3) + [pl.BlockSpec(memory_space=pl.ANY)],
            out_specs=(vmem(1)[0], smem),
            scratch_shapes=[
                pltpu.VMEM((2, ng, BLK, LANES), F32),
                pltpu.VMEM((2, ng, BLK, LANES), F32),
                pltpu.VMEM((PAIR * BW, left_dim), BF16),
                pltpu.VMEM((PAIR * BW, terms * BW), F32),
                pltpu.VMEM((terms * BW, 384), BF16),
                pltpu.VMEM((NS, BLK, LANES), F32),
                pltpu.VMEM((NS, BLK, LANES), F32),
                pltpu.VMEM((NS, *TILE), F32),
                pltpu.VMEM(TILE, F32),
                pltpu.VMEM((2, ng, *ROWVEC), F32),
                pltpu.VMEM((left_dim, terms * BW), BF16),
                pltpu.VMEM((right_dim, terms * BW), BF16),
                pltpu.VMEM((PAIR * 16, terms * BW), F32),
                pltpu.VMEM((terms * rows, left_dim), F32),
                pltpu.VMEM((terms * rows, left_dim), BF16),
                pltpu.VMEM((NS, terms * rows, left_dim), BF16),
                pltpu.VMEM((terms, BW, right_dim), BF16),
                pltpu.VMEM((NS, *TILE), F32),
                pltpu.VMEM((NS, *TILE), F32),
                pltpu.VMEM((NS, *TILE), F32),
                pltpu.VMEM((NS, *TILE), F32),
                pltpu.VMEM((128, 128), F32),
                dma(2, nz), dma(2, nz), dma(4, ng), dma(2, NS), dma(2, NS), dma(NS), dma(NS), dma(ng), dma(2, ng),
                dma(NS), dma(NS), dma(NS), dma(NS), dma(NS), dma(NS), pltpu.SemaphoreType.DMA,
            ],
            compiler_params=pltpu.CompilerParams(
                collective_id=0, has_side_effects=True, vmem_limit_bytes=56 * 1024 * 1024
            ),
            name="lanczos",
        )(
            wave_rows.transpose(1, 2, 0, 3).reshape(PAIR, rows, right_dim),
            left_rows,
            op_pair.transpose(1, 2, 0),
            right_env,
        )
        vecs = vecs.reshape(nv, 3, 3, rows, right_dim).transpose(0, 3, 1, 2, 4)
        return vecs, ab[0], ab[1]

    return jax.shard_map(
        local_run,
        mesh=mesh,
        in_specs=(P(ROW), P(None, ROW), P(), P()),
        out_specs=(P(None, ROW), P(), P()),
        check_vma=False,
    )
```

```python
import functools

import jax
import jax.numpy as jnp
from jax import lax
from jax.experimental import pallas as pl
from jax.experimental.pallas import tpu as pltpu
from jax.sharding import PartitionSpec as P

NUM_STEPS = 6
ROW = "rows"
NY, NX, NC = 4, 4, 2
NS = NY * NX
PAIR = 9
BW = 32
BLK = 72
HALVES = (slice(0, 32), slice(32, 72))
LANES = 128
TILE, ROWVEC = (8, LANES), (1, LANES)
PAIRED, QUAD = range(2), range(4)
MESH = pl.DeviceIdType.MESH
F32, BF16 = jnp.float32, jnp.bfloat16
OFFSETS = sorted(
    [(dy, dx) for dy in range(NY) for dx in range(NX) if (dy, dx) != (0, 0)],
    key=lambda o: (-(min(o[0], NY - o[0]) + min(o[1], NX - o[1])), o),
)


def span(k, width):
    return slice(k * width, k * width + width)


GROUPS = [(k, span(k, LANES)) for k in QUAD]
ROW0, ROW1, ROW2, ROW3, ROW4 = [span(k, 1) for k in range(5)]


def place():
    me = lax.axis_index(ROW)
    return me // (NS * NC), (me // (NX * NC)) % NY, (me // NC) % NX, me % NC


def device(z, y, x, core):
    return ((z * NY + y) * NX + x) * NC + core


def rcopy(src, dst, send_sem, recv_sem, dev):
    return pltpu.make_async_remote_copy(
        src_ref=src, dst_ref=dst, send_sem=send_sem, recv_sem=recv_sem, device_id=(dev,), device_id_type=MESH
    )


def knock(devs):
    for dev in devs:
        pl.semaphore_signal(pltpu.get_barrier_semaphore(), inc=1, device_id=(dev,), device_id_type=MESH)


def enter(devs):
    pl.semaphore_wait(pltpu.get_barrier_semaphore(), len(devs))


def plane_peers(z, y, x, core):
    out = []
    for dy, dx in OFFSETS:
        py, px = (y + dy) % NY, (x + dx) % NX
        out.append((py * NX + px, device(z, py, px, core)))
    return out


def swap4(a, b, c, d):
    lane = lax.broadcasted_iota(jnp.int32, a.shape, 1)
    low = lane < 64
    even = (lane // 32) % 2 == 0
    a, c = jnp.where(low, a, pltpu.roll(c, 64, 1)), jnp.where(low, pltpu.roll(a, 64, 1), c)
    b, d = jnp.where(low, b, pltpu.roll(d, 64, 1)), jnp.where(low, pltpu.roll(b, 64, 1), d)
    a, b = jnp.where(even, a, pltpu.roll(b, 32, 1)), jnp.where(even, pltpu.roll(a, 96, 1), b)
    c, d = jnp.where(even, c, pltpu.roll(d, 32, 1)), jnp.where(even, pltpu.roll(c, 96, 1), d)
    return a, b, c, d


def fold(val):
    return jnp.sum(val.reshape(BLK // 8, *TILE), axis=0)


def total(val):
    one = jnp.sum(jnp.sum(val, axis=0, keepdims=True), axis=1, keepdims=True)
    return jnp.broadcast_to(one, ROWVEC)


def block(main, last):
    return jnp.concatenate([main[0], main[1], last], axis=0)


def pack_last(rows):
    grp = lax.broadcasted_iota(jnp.int32, TILE, 1) // 32
    packed = rows[0:8]
    for t in range(1, 4):
        packed = jnp.where(grp == t, pltpu.roll(rows[span(t, 8)], 32 * t, 1), packed)
    return packed


def unpack_last(tile):
    return jnp.concatenate([tile if t == 0 else pltpu.roll(tile, 128 - 32 * t, 1) for t in QUAD], axis=0)


def rows5(vals):
    row = lax.broadcasted_iota(jnp.int32, TILE, 0)
    tile = vals[4]
    for k in (3, 2, 1, 0):
        tile = jnp.where(row == k, vals[k], tile)
    return jnp.broadcast_to(tile, TILE)


def ratio(num, den):
    some = den > 0.0
    return jnp.where(some, num / jnp.where(some, den, 1.0), 0.0)


def main_kernel(
    nz, count, psi_ref, left_ref, op_ref, right_ref, vec_ref, ab_ref,
    gbuf, vb, ut, xt, y2, sbuf, rbuf, abuf, asend, cbuf, lt, r2, wv, lf, lsend, lrecv, rt, psend, precv, osend, orecv, mt,
    g_ss, d_ss, g_rs, r_ss, r_rs, a_ss, a_rs, c_ss, c_rs, l_ss, l_rs, p_ss, p_rs, o_ss, o_rs, rt_sem,
):
    ng = nz * NC
    terms = left_ref.shape[0]
    left_dim = left_ref.shape[2]
    z, y, x, core = place()
    i, j = core * nz + z, y * NX + x
    peers = plane_peers(z, y, x, core)
    mate = device(z, y, x, 1 - core)
    zs = [((z + dz) % nz, dz) for dz in sorted(range(1, nz), key=lambda dz: (min(dz, nz - dz), dz))]
    line = [(core, pz, dz) for pz, dz in zs] + [(1 - core, pz, nz + dz) for pz, dz in zs] + [(1 - core, z, nz)]

    load_right = pltpu.make_async_copy(right_ref.at[:, pl.ds(pl.multiple_of(j * BW, BW), BW), :], rt, rt_sem)
    load_right.start()
    others = [dev for _, dev in peers] + [device(pz, y, x, pc) for pc, pz, _ in line]
    knock(others)

    def start_gather(par, half):
        own = gbuf.at[par, i, HALVES[half]]
        for pz, dz in reversed(zs):
            rcopy(own, own, g_ss.at[half, dz], g_rs.at[2 * par + half, i], device(pz, y, x, core)).start()
        rcopy(own, own, g_ss.at[half, 0], g_rs.at[2 * par + half, i], mate).start()

    def relay(par, half):
        for pz, dz in zs:
            slot = core * nz + pz
            ref = gbuf.at[par, slot, HALVES[half]]
            rcopy(ref, ref, g_ss.at[half, dz], g_rs.at[2 * par + half, slot], mate).wait_recv()
            rcopy(ref, ref, d_ss.at[half, dz], g_rs.at[2 * par + half, slot], mate).start()

    def finish_gather(par):
        for half in PAIRED:
            for dz in range(nz):
                slot = (1 - core) * nz + (z + dz) % nz
                ref = gbuf.at[par, slot, HALVES[half]]
                rcopy(ref, ref, g_ss.at[half, 0], g_rs.at[2 * par + half, slot], mate).wait_recv()
    def drain_gather(par):
        for half in PAIRED:
            own = gbuf.at[par, i, HALVES[half]]
            rcopy(own, own, g_ss.at[half, 0], g_rs.at[2 * par + half, i], mate).wait_send()
            for pz, dz in zs:
                ref = gbuf.at[par, core * nz + pz, HALVES[half]]
                rcopy(own, own, g_ss.at[half, dz], g_rs.at[2 * par + half, i], mate).wait_send()
                rcopy(ref, ref, d_ss.at[half, dz], g_rs.at[2 * par + half, i], mate).wait_send()

    def start_line(par, vals):
        lane = lax.broadcasted_iota(jnp.int32, ROWVEC, 1)
        line_row = vals[4]
        for k in reversed(QUAD):
            line_row = jnp.where(lane == k, vals[k], line_row)
        cbuf[par, pl.ds(i, 1)] = line_row[None]
        own = cbuf.at[par, i]
        for pc, pz, k in line:
            rcopy(own, own, c_ss.at[k], c_rs.at[par, i], device(pz, y, x, pc)).start()

    def finish_line(par):
        own = cbuf.at[par, i]
        for pc, pz, k in line:
            slot = pc * nz + pz
            rcopy(own, cbuf.at[par, slot], c_ss.at[k], c_rs.at[par, slot], mate).wait_recv()
        rows = jnp.concatenate([cbuf[par, s] for s in range(ng)], axis=0)
        lane = lax.broadcasted_iota(jnp.int32, rows.shape, 1)
        m, p, nn, ee, ev = [jnp.sum(jnp.where(lane == k, rows, 0.0), axis=1, keepdims=True) for k in range(5)]
        alpha = jnp.sum(m, axis=0, keepdims=True) / count
        off = p - alpha
        square = jnp.sum(ee + 2.0 * (off * ev) + (off * nn) * off, axis=0, keepdims=True)
        return jnp.broadcast_to(alpha, ROWVEC), jnp.broadcast_to(jnp.sqrt(square / count), ROWVEC)

    def start_plane(par, beta_prev):
        w, v, vp = gbuf[par, i], vb[1 - par, i], vb[par, i]
        rest = w - beta_prev * vp
        m, yv, nn = total(fold(w * v)), total(fold(rest * v)), total(fold(v * v))
        p = ratio(yv, nn)
        e = rest - p * v
        tile = rows5([m, p, nn, total(fold(e * e)), total(fold(e * v))])
        asend[...] = tile
        for pj, dev in peers:
            rcopy(asend, abuf.at[j], a_ss.at[pj], a_rs.at[j], dev).start()
        abuf[pl.ds(j, 1)] = tile[None]

    def finish_plane():
        for pj, dev in peers:
            rcopy(asend, abuf.at[pj], a_ss.at[pj], a_rs.at[pj], dev).wait_recv()
        zero = jnp.zeros(ROWVEC, F32)
        m, nn, pn, ee, ev = zero, zero, zero, zero, zero
        for s in range(NS):
            m, nn, pn = m + abuf[s, ROW0], nn + abuf[s, ROW2], pn + abuf[s, ROW1] * abuf[s, ROW2]
        p = ratio(pn, nn)
        for s in range(NS):
            off = abuf[s, ROW1] - p
            ee = ee + (abuf[s, ROW3] + 2.0 * (off * abuf[s, ROW4]) + (off * abuf[s, ROW2]) * off)
            ev = ev + (abuf[s, ROW4] + off * abuf[s, ROW2])
        return [m, p, nn, ee, ev]

    def start_out(par):
        blk = gbuf[par, i]
        last = unpack_last(blk[64:72])
        mt[...] = jnp.concatenate([blk[:64], last, jnp.zeros((32, 128), F32)], axis=0).T
        for pj in range(NS):
            for k in QUAD:
                osend[pj, span(k, 2)] = mt[span(k * NS + pj, 2)]
        for pj, dev in peers:
            rcopy(osend.at[pj], orecv.at[j], o_ss.at[pj], o_rs.at[j], dev).start()
        orecv[pl.ds(j, 1)] = osend[pl.ds(j, 1)]

    def finish_out(num):
        for pj, dev in peers:
            rcopy(osend.at[pj], orecv.at[pj], o_ss.at[pj], o_rs.at[pj], dev).wait_recv()
        for grp, lanes in GROUPS:
            outs = swap4(*[orecv[grp * 4 + k] for k in QUAD])
            for t in PAIRED:
                for k in QUAD:
                    vec_ref[num, 4 * t + k, :, lanes] = outs[t][span(k, 2)]
            vec_ref[num, 8, :, lanes] = outs[2][0:2]

    def own_rows(num, alpha, beta_prev, beta):
        older = num - 2 if isinstance(num, int) else jnp.maximum(num - 2, 0)
        for grp, lanes in GROUPS:
            for q in range(PAIR):
                w, v, vp = vec_ref[num, q, :, lanes], vec_ref[num - 1, q, :, lanes], vec_ref[older, q, :, lanes]
                vec_ref[num, q, :, lanes] = (w - alpha * v - beta_prev * vp) / beta

    def update(par, alpha, beta_prev, beta, first, size):
        def body(s, carry):
            w, v, vp = gbuf[par, s], vb[1 - par, s], vb[par, s]
            vb[par, pl.ds(s, 1)] = ((w - alpha * v - beta_prev * vp) / beta)[None]
            return carry

        lax.fori_loop(first, first + size, body, 0, unroll=4 if size > 1 else 1)

    def left_and_mix(par):
        for grp in range(ng // 4):
            lanes = span(grp, LANES)
            for t in PAIRED:
                outs = swap4(*[vb[par, grp * 4 + ii, span(t, BW)] for ii in QUAD])
                for k in QUAD:
                    q = 4 * t + k
                    ut[span(q, BW), lanes] = outs[k].astype(BF16)
            outs = swap4(*[vb[par, grp * 4 + ii, 64:72] for ii in QUAD])
            ut[256:272, lanes] = jnp.concatenate(outs[:2], axis=0).astype(BF16)
            ut[272:288, lanes] = jnp.concatenate(outs[2:], axis=0).astype(BF16)
        width = 256
        for part in range(terms * BW // width):
            cols = span(part, width)
            whole = jnp.dot(ut[...], lt[:, cols], preferred_element_type=F32).astype(BF16).astype(F32)
            xt[:, cols] = whole
            for sub in range(width // LANES):
                grp = part * (width // LANES) + sub
                mix(0, grp, [whole[span(r, BW), span(sub, LANES)] for r in range(PAIR)])

    def mix(half, grp, xs):
        lanes = span(grp, LANES)
        for part in PAIRED:
            some = [x_r[span(part, 16)] for x_r in xs]

            def one(q):
                acc = wv[q * 16 : q * 16 + 1, lanes] * some[0]
                for r in range(1, PAIR):
                    acc = acc + wv[q * 16 + r : q * 16 + r + 1, lanes] * some[r]
                return acc

            rows = [span(grp * 8 + 2 * k + part, 16) for k in QUAD]
            outs = swap4(*[one(4 * half + k) for k in QUAD])
            for k in QUAD:
                y2[rows[k], span(half, LANES)] = outs[k].astype(BF16)
            if half:
                last = one(8)
                for k in QUAD:
                    moved = last if k == 0 else pltpu.roll(last, LANES - BW * k, 1)
                    y2[rows[k], 2 * LANES :] = moved.astype(BF16)

    def mix_rest():
        for grp in range(terms * BW // LANES):
            mix(1, grp, [xt[span(r, BW), span(grp, LANES)] for r in range(PAIR)])

    def start_scatter(half):
        cols = slice(0, 128) if half == 0 else slice(128, 384)
        for dy in (2, 1, 3, 0):
            py = (y + dy) % NY
            part = jnp.dot(
                r2[pl.ds(pl.multiple_of(py * 128, 128), 128), :], y2[:, cols], preferred_element_type=F32
            )
            for px in range(NX):
                pj = py * NX + px
                rows = part[span(px, BW)]
                if half == 0:
                    sbuf[pj, 0:32] = rows
                else:
                    sbuf[pj, 32:64] = rows[:, 0:128]
                    sbuf[pj, 64:72] = pack_last(rows[:, 128:256])
                send = rcopy(
                    sbuf.at[pj, HALVES[half]], rbuf.at[j, HALVES[half]],
                    r_ss.at[half, pj], r_rs.at[half, j], device(z, py, px, core),
                )
                if dy:
                    send.start()
                else:

                    @pl.when(px != x)
                    def _():
                        send.start()

        rbuf[pl.ds(j, 1), HALVES[half]] = sbuf[pl.ds(j, 1), HALVES[half]]

    def finish_scatter(nxt, half):
        for pj, dev in reversed(peers):
            rcopy(
                sbuf.at[pj, HALVES[half]], rbuf.at[pj, HALVES[half]], r_ss.at[half, pj], r_rs.at[half, pj], dev
            ).wait_recv()
        w = rbuf[0, HALVES[half]]
        for s in range(1, NS):
            w = w + rbuf[s, HALVES[half]]
        gbuf[nxt, pl.ds(i, 1), HALVES[half]] = w[None]

    def drain_sums(par):
        for pj, dev in peers:
            rcopy(asend, abuf.at[pj], a_ss.at[pj], a_rs.at[pj], dev).wait_send()
            rcopy(osend.at[pj], orecv.at[pj], o_ss.at[pj], o_rs.at[pj], dev).wait_send()
        drain_line(par)

    def drain_line(par):
        own = cbuf.at[par, i]
        for pc, pz, k in line:
            rcopy(own, own, c_ss.at[k], c_rs.at[par, i], mate).wait_send()

    def drain_scatter():
        for half in PAIRED:
            for pj, dev in peers:
                ref = sbuf.at[pj, HALVES[half]]
                rcopy(ref, ref, r_ss.at[half, pj], r_rs.at[half, pj], dev).wait_send()

    def product(par, nxt, more, between):
        left_and_mix(par)
        start_scatter(0)
        mix_rest()
        start_scatter(1)
        drain_gather(par)
        between()
        for half in PAIRED:
            finish_scatter(nxt, half)
            if more is True:
                start_gather(nxt, half)
            else:

                @pl.when(more)
                def _(half=half):
                    start_gather(nxt, half)

    norm = jnp.zeros(ROWVEC, F32)
    for grp, lanes in GROUPS:
        for q in range(PAIR):
            norm = norm + jnp.sum(psi_ref[q, :, lanes] * psi_ref[q, :, lanes], axis=0, keepdims=True)
    norm = jnp.broadcast_to(jnp.sum(norm, axis=1, keepdims=True), TILE)
    for t in range(3):
        mt[span(t, 8)] = jnp.zeros(TILE, F32)
    for grp, lanes in GROUPS:
        for q in range(PAIR):
            mt[span(q, 2)] = psi_ref[q, :, lanes]
        outs = swap4(mt[0:8], mt[8:16], mt[16:24], norm)
        for k in QUAD:
            psend[grp * 4 + k] = outs[k]
    for k in range(terms):
        lf[span(k, 2)] = left_ref[k].astype(F32)
    row = lax.broadcasted_iota(jnp.int32, (left_dim, left_dim), 0)
    col = lax.broadcasted_iota(jnp.int32, (left_dim, left_dim), 1)
    goal = ((row >> 1) & 1) * (nz * BW) + (row >> 6) * BW + ((row >> 2) & 15) * 2 + (row & 1)
    perm = jnp.where(goal == col, 1.0, 0.0).astype(BF16)
    lsend[...] = jnp.dot(lf[...].astype(BF16), perm, preferred_element_type=F32).astype(BF16)
    enter(others)
    for pj, dev in peers:
        rcopy(psend.at[pj], precv.at[j], p_ss.at[pj], p_rs.at[j], dev).start()
    precv[pl.ds(j, 1)] = psend[pl.ds(j, 1)]
    for pj, dev in peers:
        rcopy(lsend, lrecv.at[j], l_ss.at[pj], l_rs.at[j], dev).start()
    lrecv[pl.ds(j, 1)] = lsend[...][None]

    term = lax.broadcasted_iota(jnp.int32, (terms, terms * BW), 0)
    lane = lax.broadcasted_iota(jnp.int32, (terms, terms * BW), 1)
    spread = jnp.where((lane >> 5) == term, 1.0, 0.0).astype(BF16)
    for q in range(PAIR):
        wv[q * 16 : q * 16 + PAIR] = jnp.dot(op_ref[q], spread, preferred_element_type=F32)
    vb[...] = jnp.zeros_like(vb)

    for pj, dev in peers:
        rcopy(psend.at[pj], precv.at[pj], p_ss.at[pj], p_rs.at[pj], dev).wait_recv()
    square = precv[0, ROW0]
    for s in range(1, NS):
        square = square + precv[s, ROW0]
    square = jnp.where(lax.broadcasted_iota(jnp.int32, ROWVEC, 1) >= 96, square, 0.0)
    square = square + pltpu.roll(square, 64, 1)
    square = square + pltpu.roll(square, 32, 1)
    for s in range(NS):
        for k in QUAD:
            mt[span(k * NS + s, 2)] = precv[s, span(k, 2)]
    flat = mt[...].T
    gbuf[0, pl.ds(i, 1)] = block((flat[span(0, BW)], flat[span(1, BW)]), pack_last(flat[span(2, BW)]))[None]
    start_gather(0, 0)
    start_gather(0, 1)
    zero = jnp.zeros(ROWVEC, F32)
    start_line(0, [zero, zero, zero, square, zero])

    load_right.wait()
    for part in range(terms * BW // 128):
        rows = rt[span(part, 4)].reshape(128, rt.shape[2])
        r2[:, span(part, LANES)] = rows.T

    relay(0, 0)
    relay(0, 1)
    for pj, dev in peers:
        rcopy(lsend, lrecv.at[pj], l_ss.at[pj], l_rs.at[pj], dev).wait_recv()
    mine = lrecv[...].reshape(NS * terms * 2, left_dim)
    width = 256
    row = lax.broadcasted_iota(jnp.int32, (NS * terms * 2, width), 0)
    col = lax.broadcasted_iota(jnp.int32, (NS * terms * 2, width), 1)
    shift = terms.bit_length()
    goal = ((row & (2 * terms - 1)) >> 1) * BW + (row >> shift) * 2 + (row & 1)
    for part in range(terms * BW // width):
        perm = jnp.where(goal == col + part * width, 1.0, 0.0).astype(BF16)
        lt[:, span(part, width)] = lax.dot_general(
            mine, perm, (((0,), (0,)), ((), ())), preferred_element_type=F32
        ).astype(BF16)
    finish_gather(0)
    alpha, beta = finish_line(0)
    update(0, zero, zero, beta, 0, ng)

    def first_rows():
        drain_line(0)
        for pj, dev in peers:
            rcopy(psend.at[pj], precv.at[pj], p_ss.at[pj], p_rs.at[pj], dev).wait_send()
            rcopy(lsend, lrecv.at[pj], l_ss.at[pj], l_rs.at[pj], dev).wait_send()
        for grp, lanes in GROUPS:
            for q in range(PAIR):
                vec_ref[0, q, :, lanes] = psi_ref[q, :, lanes] / beta

    product(0, 1, True, first_rows)

    def step(t, beta_prev):
        par = t % 2
        start_plane(par, beta_prev)
        start_out(par)
        drain_scatter()
        relay(par, 0)
        start_line(par, finish_plane())
        relay(par, 1)
        finish_out(t)
        finish_gather(par)
        alpha, beta = finish_line(par)
        update(par, alpha, beta_prev, beta, 0, ng)

        def rest():
            drain_sums(par)
            ab_ref[0, t - 1] = alpha[0, 0]
            ab_ref[1, t - 1] = beta[0, 0]
            own_rows(t, alpha, beta_prev, beta)

        product(par, 1 - par, t < NUM_STEPS - 1, rest)
        return beta

    beta_prev = lax.fori_loop(1, NUM_STEPS, step, zero)
    par = NUM_STEPS % 2
    start_plane(par, beta_prev)
    start_out(par)
    drain_scatter()
    start_line(par, finish_plane())
    finish_out(NUM_STEPS)
    alpha, beta = finish_line(par)
    ab_ref[0, NUM_STEPS - 1] = alpha[0, 0]
    ab_ref[1, NUM_STEPS - 1] = beta[0, 0]
    own_rows(NUM_STEPS, alpha, beta_prev, beta)
    drain_sums(par)


def end_kernel(vec_ref, ab_ref, vec_out, alpha_out, beta_out):
    vec_out[...] = vec_ref[...]
    for k in range(NUM_STEPS):
        alpha_out[k] = ab_ref[0, k]
        beta_out[k] = ab_ref[1, k]


def vmem(n):
    return [pl.BlockSpec(memory_space=pltpu.VMEM)] * n


def dma(*shape):
    return pltpu.SemaphoreType.DMA(shape)


def solution(mesh):
    nz = mesh.shape[ROW] // (NS * NC)
    ng = nz * NC

    def local_run(wave_rows, left_rows, op_pair, right_env):
        terms, rows, left_dim = left_rows.shape
        right_dim = right_env.shape[1]
        count = left_dim * right_dim * PAIR
        nv = NUM_STEPS + 1
        smem = pl.BlockSpec(memory_space=pltpu.SMEM)
        vecs, ab = pl.pallas_call(
            functools.partial(main_kernel, nz, float(count)),
            out_shape=(
                jax.ShapeDtypeStruct((nv, PAIR, rows, right_dim), F32),
                jax.ShapeDtypeStruct((2, NUM_STEPS), F32),
            ),
            in_specs=vmem(3) + [pl.BlockSpec(memory_space=pl.ANY)],
            out_specs=(vmem(1)[0], smem),
            scratch_shapes=[
                pltpu.VMEM((2, ng, BLK, LANES), F32),
                pltpu.VMEM((2, ng, BLK, LANES), F32),
                pltpu.VMEM((PAIR * BW, left_dim), BF16),
                pltpu.VMEM((PAIR * BW, terms * BW), F32),
                pltpu.VMEM((terms * BW, 384), BF16),
                pltpu.VMEM((NS, BLK, LANES), F32),
                pltpu.VMEM((NS, BLK, LANES), F32),
                pltpu.VMEM((NS, *TILE), F32),
                pltpu.VMEM(TILE, F32),
                pltpu.VMEM((2, ng, *ROWVEC), F32),
                pltpu.VMEM((left_dim, terms * BW), BF16),
                pltpu.VMEM((right_dim, terms * BW), BF16),
                pltpu.VMEM((PAIR * 16, terms * BW), F32),
                pltpu.VMEM((terms * rows, left_dim), F32),
                pltpu.VMEM((terms * rows, left_dim), BF16),
                pltpu.VMEM((NS, terms * rows, left_dim), BF16),
                pltpu.VMEM((terms, BW, right_dim), BF16),
                pltpu.VMEM((NS, *TILE), F32),
                pltpu.VMEM((NS, *TILE), F32),
                pltpu.VMEM((NS, *TILE), F32),
                pltpu.VMEM((NS, *TILE), F32),
                pltpu.VMEM((128, 128), F32),
                dma(2, nz), dma(2, nz), dma(4, ng), dma(2, NS), dma(2, NS), dma(NS), dma(NS), dma(ng), dma(2, ng),
                dma(NS), dma(NS), dma(NS), dma(NS), dma(NS), dma(NS), pltpu.SemaphoreType.DMA,
            ],
            compiler_params=pltpu.CompilerParams(
                collective_id=0, has_side_effects=True, vmem_limit_bytes=56 * 1024 * 1024
            ),
            name="lanczos",
        )(
            wave_rows.transpose(1, 2, 0, 3).reshape(PAIR, rows, right_dim),
            left_rows,
            op_pair.transpose(1, 2, 0),
            right_env,
        )
        short = jax.ShapeDtypeStruct((NUM_STEPS,), F32)
        vecs, alpha, beta = pl.pallas_call(
            end_kernel,
            out_shape=(jax.ShapeDtypeStruct(vecs.shape, F32), short, short),
            in_specs=vmem(1) + [smem],
            out_specs=(vmem(1)[0], smem, smem),
            name="result",
        )(vecs, ab)
        vecs = vecs.reshape(nv, 3, 3, rows, right_dim).transpose(0, 3, 1, 2, 4)
        return vecs, alpha, beta

    return jax.shard_map(
        local_run,
        mesh=mesh,
        in_specs=(P(ROW), P(None, ROW), P(), P()),
        out_specs=(P(None, ROW), P(), P()),
        check_vma=False,
    )
```

```python
import functools

import jax
import jax.numpy as jnp
from jax import lax
from jax.experimental import pallas as pl
from jax.experimental.pallas import tpu as pltpu
from jax.sharding import PartitionSpec as P

NUM_STEPS = 6
ROW = "rows"
NY, NX, NC = 4, 4, 2
NS = NY * NX
PAIR = 9
BW = 32
BLK = 72
HALVES = (slice(0, 32), slice(32, 72))
LANES = 128
TILE, ROWVEC = (8, LANES), (1, LANES)
PAIRED, QUAD = range(2), range(4)
MESH = pl.DeviceIdType.MESH
F32, BF16 = jnp.float32, jnp.bfloat16
OFFSETS = sorted(
    [(dy, dx) for dy in range(NY) for dx in range(NX) if (dy, dx) != (0, 0)],
    key=lambda o: (-(min(o[0], NY - o[0]) + min(o[1], NX - o[1])), o),
)


def span(k, width):
    return slice(k * width, k * width + width)


GROUPS = [(k, span(k, LANES)) for k in QUAD]
ROW0, ROW1, ROW2, ROW3, ROW4 = [span(k, 1) for k in range(5)]


def place():
    me = lax.axis_index(ROW)
    return me // (NS * NC), (me // (NX * NC)) % NY, (me // NC) % NX, me % NC


def device(z, y, x, core):
    return ((z * NY + y) * NX + x) * NC + core


def rcopy(src, dst, send_sem, recv_sem, dev):
    return pltpu.make_async_remote_copy(
        src_ref=src, dst_ref=dst, send_sem=send_sem, recv_sem=recv_sem, device_id=(dev,), device_id_type=MESH
    )


def knock(devs):
    for dev in devs:
        pl.semaphore_signal(pltpu.get_barrier_semaphore(), inc=1, device_id=(dev,), device_id_type=MESH)


def enter(devs):
    pl.semaphore_wait(pltpu.get_barrier_semaphore(), len(devs))


def plane_peers(z, y, x, core):
    out = []
    for dy, dx in OFFSETS:
        py, px = (y + dy) % NY, (x + dx) % NX
        out.append((py * NX + px, device(z, py, px, core)))
    return out


def swap4(a, b, c, d):
    lane = lax.broadcasted_iota(jnp.int32, a.shape, 1)
    low = lane < 64
    even = (lane // 32) % 2 == 0
    a, c = jnp.where(low, a, pltpu.roll(c, 64, 1)), jnp.where(low, pltpu.roll(a, 64, 1), c)
    b, d = jnp.where(low, b, pltpu.roll(d, 64, 1)), jnp.where(low, pltpu.roll(b, 64, 1), d)
    a, b = jnp.where(even, a, pltpu.roll(b, 32, 1)), jnp.where(even, pltpu.roll(a, 96, 1), b)
    c, d = jnp.where(even, c, pltpu.roll(d, 32, 1)), jnp.where(even, pltpu.roll(c, 96, 1), d)
    return a, b, c, d


def fold(val):
    return jnp.sum(val.reshape(BLK // 8, *TILE), axis=0)


def total(val):
    one = jnp.sum(jnp.sum(val, axis=0, keepdims=True), axis=1, keepdims=True)
    return jnp.broadcast_to(one, ROWVEC)


def block(main, last):
    return jnp.concatenate([main[0], main[1], last], axis=0)


def pack_last(rows):
    grp = lax.broadcasted_iota(jnp.int32, TILE, 1) // 32
    packed = rows[0:8]
    for t in range(1, 4):
        packed = jnp.where(grp == t, pltpu.roll(rows[span(t, 8)], 32 * t, 1), packed)
    return packed


def unpack_last(tile):
    return jnp.concatenate([tile if t == 0 else pltpu.roll(tile, 128 - 32 * t, 1) for t in QUAD], axis=0)


def rows5(vals):
    row = lax.broadcasted_iota(jnp.int32, TILE, 0)
    tile = vals[4]
    for k in (3, 2, 1, 0):
        tile = jnp.where(row == k, vals[k], tile)
    return jnp.broadcast_to(tile, TILE)


def ratio(num, den):
    some = den > 0.0
    return jnp.where(some, num / jnp.where(some, den, 1.0), 0.0)


def main_kernel(
    nz, count, psi_ref, left_ref, op_ref, right_ref, vec_ref, ab_ref,
    gbuf, vb, ut, xt, y2, sbuf, rbuf, abuf, asend, cbuf, lt, r2, wv, lf, lsend, lrecv, rt, psend, precv, osend, orecv, mt,
    g_ss, d_ss, g_rs, r_ss, r_rs, a_ss, a_rs, c_ss, c_rs, l_ss, l_rs, p_ss, p_rs, o_ss, o_rs, rt_sem,
):
    ng = nz * NC
    terms = left_ref.shape[0]
    left_dim = left_ref.shape[2]
    z, y, x, core = place()
    i, j = core * nz + z, y * NX + x
    peers = plane_peers(z, y, x, core)
    mate = device(z, y, x, 1 - core)
    zs = [((z + dz) % nz, dz) for dz in sorted(range(1, nz), key=lambda dz: (min(dz, nz - dz), dz))]
    line = [(core, pz, dz) for pz, dz in zs] + [(1 - core, pz, nz + dz) for pz, dz in zs] + [(1 - core, z, nz)]

    load_right = pltpu.make_async_copy(right_ref.at[:, pl.ds(pl.multiple_of(j * BW, BW), BW), :], rt, rt_sem)
    load_right.start()
    others = [dev for _, dev in peers] + [device(pz, y, x, pc) for pc, pz, _ in line]
    knock(others)

    def start_gather(par, half):
        own = gbuf.at[par, i, HALVES[half]]
        for pz, dz in reversed(zs):
            rcopy(own, own, g_ss.at[half, dz], g_rs.at[2 * par + half, i], device(pz, y, x, core)).start()
        rcopy(own, own, g_ss.at[half, 0], g_rs.at[2 * par + half, i], mate).start()

    def relay(par, half):
        for pz, dz in zs:
            slot = core * nz + pz
            ref = gbuf.at[par, slot, HALVES[half]]
            rcopy(ref, ref, g_ss.at[half, dz], g_rs.at[2 * par + half, slot], mate).wait_recv()
            rcopy(ref, ref, d_ss.at[half, dz], g_rs.at[2 * par + half, slot], mate).start()

    def finish_gather(par):
        for half in PAIRED:
            for dz in range(nz):
                slot = (1 - core) * nz + (z + dz) % nz
                ref = gbuf.at[par, slot, HALVES[half]]
                rcopy(ref, ref, g_ss.at[half, 0], g_rs.at[2 * par + half, slot], mate).wait_recv()
    def drain_gather(par):
        for half in PAIRED:
            own = gbuf.at[par, i, HALVES[half]]
            rcopy(own, own, g_ss.at[half, 0], g_rs.at[2 * par + half, i], mate).wait_send()
            for pz, dz in zs:
                ref = gbuf.at[par, core * nz + pz, HALVES[half]]
                rcopy(own, own, g_ss.at[half, dz], g_rs.at[2 * par + half, i], mate).wait_send()
                rcopy(ref, ref, d_ss.at[half, dz], g_rs.at[2 * par + half, i], mate).wait_send()

    def start_line(par, vals):
        lane = lax.broadcasted_iota(jnp.int32, ROWVEC, 1)
        line_row = vals[4]
        for k in reversed(QUAD):
            line_row = jnp.where(lane == k, vals[k], line_row)
        cbuf[par, pl.ds(i, 1)] = line_row[None]
        own = cbuf.at[par, i]
        for pc, pz, k in line:
            rcopy(own, own, c_ss.at[k], c_rs.at[par, i], device(pz, y, x, pc)).start()

    def finish_line(par):
        own = cbuf.at[par, i]
        for pc, pz, k in line:
            slot = pc * nz + pz
            rcopy(own, cbuf.at[par, slot], c_ss.at[k], c_rs.at[par, slot], mate).wait_recv()
        rows = jnp.concatenate([cbuf[par, s] for s in range(ng)], axis=0)
        lane = lax.broadcasted_iota(jnp.int32, rows.shape, 1)
        m, p, nn, ee, ev = [jnp.sum(jnp.where(lane == k, rows, 0.0), axis=1, keepdims=True) for k in range(5)]
        alpha = jnp.sum(m, axis=0, keepdims=True) / count
        off = p - alpha
        square = jnp.sum(ee + 2.0 * (off * ev) + (off * nn) * off, axis=0, keepdims=True)
        return jnp.broadcast_to(alpha, ROWVEC), jnp.broadcast_to(jnp.sqrt(square / count), ROWVEC)

    def start_plane(par, beta_prev):
        w, v, vp = gbuf[par, i], vb[1 - par, i], vb[par, i]
        rest = w - beta_prev * vp
        m, yv, nn = total(fold(w * v)), total(fold(rest * v)), total(fold(v * v))
        p = ratio(yv, nn)
        e = rest - p * v
        tile = rows5([m, p, nn, total(fold(e * e)), total(fold(e * v))])
        asend[...] = tile
        for pj, dev in peers:
            rcopy(asend, abuf.at[j], a_ss.at[pj], a_rs.at[j], dev).start()
        abuf[pl.ds(j, 1)] = tile[None]

    def finish_plane():
        for pj, dev in peers:
            rcopy(asend, abuf.at[pj], a_ss.at[pj], a_rs.at[pj], dev).wait_recv()
        zero = jnp.zeros(ROWVEC, F32)
        m, nn, pn, ee, ev = zero, zero, zero, zero, zero
        for s in range(NS):
            m, nn, pn = m + abuf[s, ROW0], nn + abuf[s, ROW2], pn + abuf[s, ROW1] * abuf[s, ROW2]
        p = ratio(pn, nn)
        for s in range(NS):
            off = abuf[s, ROW1] - p
            ee = ee + (abuf[s, ROW3] + 2.0 * (off * abuf[s, ROW4]) + (off * abuf[s, ROW2]) * off)
            ev = ev + (abuf[s, ROW4] + off * abuf[s, ROW2])
        return [m, p, nn, ee, ev]

    def start_out(par):
        blk = gbuf[par, i]
        last = unpack_last(blk[64:72])
        mt[...] = jnp.concatenate([blk[:64], last, jnp.zeros((32, 128), F32)], axis=0).T
        for pj in range(NS):
            for k in QUAD:
                osend[pj, span(k, 2)] = mt[span(k * NS + pj, 2)]
        for pj, dev in peers:
            rcopy(osend.at[pj], orecv.at[j], o_ss.at[pj], o_rs.at[j], dev).start()
        orecv[pl.ds(j, 1)] = osend[pl.ds(j, 1)]

    def finish_out(num):
        for pj, dev in peers:
            rcopy(osend.at[pj], orecv.at[pj], o_ss.at[pj], o_rs.at[pj], dev).wait_recv()
        for grp, lanes in GROUPS:
            outs = swap4(*[orecv[grp * 4 + k] for k in QUAD])
            for t in PAIRED:
                for k in QUAD:
                    vec_ref[num, 4 * t + k, :, lanes] = outs[t][span(k, 2)]
            vec_ref[num, 8, :, lanes] = outs[2][0:2]

    def own_rows(num, alpha, beta_prev, beta):
        older = num - 2 if isinstance(num, int) else jnp.maximum(num - 2, 0)
        for grp, lanes in GROUPS:
            for q in range(PAIR):
                w, v, vp = vec_ref[num, q, :, lanes], vec_ref[num - 1, q, :, lanes], vec_ref[older, q, :, lanes]
                vec_ref[num, q, :, lanes] = (w - alpha * v - beta_prev * vp) / beta

    def update(par, alpha, beta_prev, beta, first, size):
        def body(s, carry):
            w, v, vp = gbuf[par, s], vb[1 - par, s], vb[par, s]
            vb[par, pl.ds(s, 1)] = ((w - alpha * v - beta_prev * vp) / beta)[None]
            return carry

        lax.fori_loop(first, first + size, body, 0, unroll=4 if size > 1 else 1)

    def left_and_mix(par):
        for grp in range(ng // 4):
            lanes = span(grp, LANES)
            for t in PAIRED:
                outs = swap4(*[vb[par, grp * 4 + ii, span(t, BW)] for ii in QUAD])
                for k in QUAD:
                    q = 4 * t + k
                    ut[span(q, BW), lanes] = outs[k].astype(BF16)
            outs = swap4(*[vb[par, grp * 4 + ii, 64:72] for ii in QUAD])
            ut[256:272, lanes] = jnp.concatenate(outs[:2], axis=0).astype(BF16)
            ut[272:288, lanes] = jnp.concatenate(outs[2:], axis=0).astype(BF16)
        width = 256
        for part in range(terms * BW // width):
            cols = span(part, width)
            whole = jnp.dot(ut[...], lt[:, cols], preferred_element_type=F32).astype(BF16).astype(F32)
            xt[:, cols] = whole
            for sub in range(width // LANES):
                grp = part * (width // LANES) + sub
                mix(0, grp, [xt[span(r, BW), span(grp, LANES)] for r in range(PAIR)])

    def mix(half, grp, xs):
        lanes = span(grp, LANES)
        for part in PAIRED:
            some = [x_r[span(part, 16)] for x_r in xs]

            def one(q):
                acc = wv[q * 16 : q * 16 + 1, lanes] * some[0]
                for r in range(1, PAIR):
                    acc = acc + wv[q * 16 + r : q * 16 + r + 1, lanes] * some[r]
                return acc

            rows = [span(grp * 8 + 2 * k + part, 16) for k in QUAD]
            outs = swap4(*[one(4 * half + k) for k in QUAD])
            for k in QUAD:
                y2[rows[k], span(half, LANES)] = outs[k].astype(BF16)
            if half:
                last = one(8)
                for k in QUAD:
                    moved = last if k == 0 else pltpu.roll(last, LANES - BW * k, 1)
                    y2[rows[k], 2 * LANES :] = moved.astype(BF16)

    def mix_rest():
        for grp in range(terms * BW // LANES):
            mix(1, grp, [xt[span(r, BW), span(grp, LANES)] for r in range(PAIR)])

    def start_scatter(half):
        cols = slice(0, 128) if half == 0 else slice(128, 384)
        for dy in (2, 1, 3, 0):
            py = (y + dy) % NY
            part = jnp.dot(
                r2[pl.ds(pl.multiple_of(py * 128, 128), 128), :], y2[:, cols], preferred_element_type=F32
            )
            for px in range(NX):
                pj = py * NX + px
                rows = part[span(px, BW)]
                if half == 0:
                    sbuf[pj, 0:32] = rows
                else:
                    sbuf[pj, 32:64] = rows[:, 0:128]
                    sbuf[pj, 64:72] = pack_last(rows[:, 128:256])
                send = rcopy(
                    sbuf.at[pj, HALVES[half]], rbuf.at[j, HALVES[half]],
                    r_ss.at[half, pj], r_rs.at[half, j], device(z, py, px, core),
                )
                if dy:
                    send.start()
                else:

                    @pl.when(px != x)
                    def _():
                        send.start()

        rbuf[pl.ds(j, 1), HALVES[half]] = sbuf[pl.ds(j, 1), HALVES[half]]

    def finish_scatter(nxt, half):
        for pj, dev in reversed(peers):
            rcopy(
                sbuf.at[pj, HALVES[half]], rbuf.at[pj, HALVES[half]], r_ss.at[half, pj], r_rs.at[half, pj], dev
            ).wait_recv()
        w = rbuf[0, HALVES[half]]
        for s in range(1, NS):
            w = w + rbuf[s, HALVES[half]]
        gbuf[nxt, pl.ds(i, 1), HALVES[half]] = w[None]

    def drain_sums(par):
        for pj, dev in peers:
            rcopy(asend, abuf.at[pj], a_ss.at[pj], a_rs.at[pj], dev).wait_send()
            rcopy(osend.at[pj], orecv.at[pj], o_ss.at[pj], o_rs.at[pj], dev).wait_send()
        drain_line(par)

    def drain_line(par):
        own = cbuf.at[par, i]
        for pc, pz, k in line:
            rcopy(own, own, c_ss.at[k], c_rs.at[par, i], mate).wait_send()

    def drain_scatter():
        for half in PAIRED:
            for pj, dev in peers:
                ref = sbuf.at[pj, HALVES[half]]
                rcopy(ref, ref, r_ss.at[half, pj], r_rs.at[half, pj], dev).wait_send()

    def product(par, nxt, more, between):
        left_and_mix(par)
        start_scatter(0)
        mix_rest()
        start_scatter(1)
        drain_gather(par)
        between()
        for half in PAIRED:
            finish_scatter(nxt, half)
            if more is True:
                start_gather(nxt, half)
            else:

                @pl.when(more)
                def _(half=half):
                    start_gather(nxt, half)

    norm = jnp.zeros(ROWVEC, F32)
    for grp, lanes in GROUPS:
        for q in range(PAIR):
            norm = norm + jnp.sum(psi_ref[q, :, lanes] * psi_ref[q, :, lanes], axis=0, keepdims=True)
    norm = jnp.broadcast_to(jnp.sum(norm, axis=1, keepdims=True), TILE)
    for t in range(3):
        mt[span(t, 8)] = jnp.zeros(TILE, F32)
    for grp, lanes in GROUPS:
        for q in range(PAIR):
            mt[span(q, 2)] = psi_ref[q, :, lanes]
        outs = swap4(mt[0:8], mt[8:16], mt[16:24], norm)
        for k in QUAD:
            psend[grp * 4 + k] = outs[k]
    for k in range(terms):
        lf[span(k, 2)] = left_ref[k].astype(F32)
    row = lax.broadcasted_iota(jnp.int32, (left_dim, left_dim), 0)
    col = lax.broadcasted_iota(jnp.int32, (left_dim, left_dim), 1)
    goal = ((row >> 1) & 1) * (nz * BW) + (row >> 6) * BW + ((row >> 2) & 15) * 2 + (row & 1)
    perm = jnp.where(goal == col, 1.0, 0.0).astype(BF16)
    lsend[...] = jnp.dot(lf[...].astype(BF16), perm, preferred_element_type=F32).astype(BF16)
    enter(others)
    for pj, dev in peers:
        rcopy(psend.at[pj], precv.at[j], p_ss.at[pj], p_rs.at[j], dev).start()
    precv[pl.ds(j, 1)] = psend[pl.ds(j, 1)]
    lhalf = [span(k, terms) for k in PAIRED]
    for k in PAIRED:
        for pj, dev in peers:
            rcopy(lsend.at[lhalf[k]], lrecv.at[j, lhalf[k]], l_ss.at[k, pj], l_rs.at[k, j], dev).start()
    lrecv[pl.ds(j, 1)] = lsend[...][None]

    term = lax.broadcasted_iota(jnp.int32, (terms, terms * BW), 0)
    lane = lax.broadcasted_iota(jnp.int32, (terms, terms * BW), 1)
    spread = jnp.where((lane >> 5) == term, 1.0, 0.0).astype(BF16)
    for q in range(PAIR):
        wv[q * 16 : q * 16 + PAIR] = jnp.dot(op_ref[q], spread, preferred_element_type=F32)
    vb[...] = jnp.zeros_like(vb)

    for pj, dev in peers:
        rcopy(psend.at[pj], precv.at[pj], p_ss.at[pj], p_rs.at[pj], dev).wait_recv()
    square = precv[0, ROW0]
    for s in range(1, NS):
        square = square + precv[s, ROW0]
    square = jnp.where(lax.broadcasted_iota(jnp.int32, ROWVEC, 1) >= 96, square, 0.0)
    square = square + pltpu.roll(square, 64, 1)
    square = square + pltpu.roll(square, 32, 1)
    for s in range(NS):
        for k in QUAD:
            mt[span(k * NS + s, 2)] = precv[s, span(k, 2)]
    flat = mt[...].T
    gbuf[0, pl.ds(i, 1)] = block((flat[span(0, BW)], flat[span(1, BW)]), pack_last(flat[span(2, BW)]))[None]
    start_gather(0, 0)
    start_gather(0, 1)
    zero = jnp.zeros(ROWVEC, F32)
    start_line(0, [zero, zero, zero, square, zero])

    load_right.wait()
    for part in range(terms * BW // 128):
        rows = rt[span(part, 4)].reshape(128, rt.shape[2])
        r2[:, span(part, LANES)] = rows.T

    relay(0, 0)
    relay(0, 1)
    width = 8 * BW
    row = lax.broadcasted_iota(jnp.int32, (width, width), 0)
    col = lax.broadcasted_iota(jnp.int32, (width, width), 1)
    goal = ((row & 15) >> 1) * BW + (row >> 4) * 2 + (row & 1)
    perm = jnp.where(goal == col, 1.0, 0.0).astype(BF16)
    parts = terms // 8
    for part in range(parts):
        for k in PAIRED:
            if part == k * parts // 2:
                for pj, dev in peers:
                    rcopy(
                        lsend.at[lhalf[k]], lrecv.at[pj, lhalf[k]], l_ss.at[k, pj], l_rs.at[k, pj], dev
                    ).wait_recv()
        mine = lrecv[:, span(part, 16), :].reshape(width, left_dim)
        lt[:, span(part, width)] = lax.dot_general(
            mine, perm, (((0,), (0,)), ((), ())), preferred_element_type=F32
        ).astype(BF16)
    finish_gather(0)
    alpha, beta = finish_line(0)
    update(0, zero, zero, beta, 0, ng)

    def first_rows():
        drain_line(0)
        for pj, dev in peers:
            rcopy(psend.at[pj], precv.at[pj], p_ss.at[pj], p_rs.at[pj], dev).wait_send()
            for k in PAIRED:
                rcopy(lsend.at[lhalf[k]], lrecv.at[pj, lhalf[k]], l_ss.at[k, pj], l_rs.at[k, pj], dev).wait_send()
        for grp, lanes in GROUPS:
            for q in range(PAIR):
                vec_ref[0, q, :, lanes] = psi_ref[q, :, lanes] / beta

    product(0, 1, True, first_rows)

    def step(t, beta_prev):
        par = t % 2
        start_plane(par, beta_prev)
        start_out(par)
        drain_scatter()
        relay(par, 0)
        start_line(par, finish_plane())
        relay(par, 1)
        finish_out(t)
        finish_gather(par)
        alpha, beta = finish_line(par)
        update(par, alpha, beta_prev, beta, 0, ng)

        def rest():
            drain_sums(par)
            ab_ref[0, t - 1] = alpha[0, 0]
            ab_ref[1, t - 1] = beta[0, 0]
            own_rows(t, alpha, beta_prev, beta)

        product(par, 1 - par, t < NUM_STEPS - 1, rest)
        return beta

    beta_prev = lax.fori_loop(1, NUM_STEPS, step, zero)
    par = NUM_STEPS % 2
    start_plane(par, beta_prev)
    start_out(par)
    drain_scatter()
    start_line(par, finish_plane())
    finish_out(NUM_STEPS)
    alpha, beta = finish_line(par)
    ab_ref[0, NUM_STEPS - 1] = alpha[0, 0]
    ab_ref[1, NUM_STEPS - 1] = beta[0, 0]
    own_rows(NUM_STEPS, alpha, beta_prev, beta)
    drain_sums(par)


def end_kernel(vec_ref, ab_ref, vec_out, alpha_out, beta_out):
    vec_out[...] = vec_ref[...]
    for k in range(NUM_STEPS):
        alpha_out[k] = ab_ref[0, k]
        beta_out[k] = ab_ref[1, k]


def vmem(n):
    return [pl.BlockSpec(memory_space=pltpu.VMEM)] * n


def dma(*shape):
    return pltpu.SemaphoreType.DMA(shape)


def solution(mesh):
    nz = mesh.shape[ROW] // (NS * NC)
    ng = nz * NC

    def local_run(wave_rows, left_rows, op_pair, right_env):
        terms, rows, left_dim = left_rows.shape
        right_dim = right_env.shape[1]
        count = left_dim * right_dim * PAIR
        nv = NUM_STEPS + 1
        smem = pl.BlockSpec(memory_space=pltpu.SMEM)
        vecs, ab = pl.pallas_call(
            functools.partial(main_kernel, nz, float(count)),
            out_shape=(
                jax.ShapeDtypeStruct((nv, PAIR, rows, right_dim), F32),
                jax.ShapeDtypeStruct((2, NUM_STEPS), F32),
            ),
            in_specs=vmem(3) + [pl.BlockSpec(memory_space=pl.ANY)],
            out_specs=(vmem(1)[0], smem),
            scratch_shapes=[
                pltpu.VMEM((2, ng, BLK, LANES), F32),
                pltpu.VMEM((2, ng, BLK, LANES), F32),
                pltpu.VMEM((PAIR * BW, left_dim), BF16),
                pltpu.VMEM((PAIR * BW, terms * BW), F32),
                pltpu.VMEM((terms * BW, 384), BF16),
                pltpu.VMEM((NS, BLK, LANES), F32),
                pltpu.VMEM((NS, BLK, LANES), F32),
                pltpu.VMEM((NS, *TILE), F32),
                pltpu.VMEM(TILE, F32),
                pltpu.VMEM((2, ng, *ROWVEC), F32),
                pltpu.VMEM((left_dim, terms * BW), BF16),
                pltpu.VMEM((right_dim, terms * BW), BF16),
                pltpu.VMEM((PAIR * 16, terms * BW), F32),
                pltpu.VMEM((terms * rows, left_dim), F32),
                pltpu.VMEM((terms * rows, left_dim), BF16),
                pltpu.VMEM((NS, terms * rows, left_dim), BF16),
                pltpu.VMEM((terms, BW, right_dim), BF16),
                pltpu.VMEM((NS, *TILE), F32),
                pltpu.VMEM((NS, *TILE), F32),
                pltpu.VMEM((NS, *TILE), F32),
                pltpu.VMEM((NS, *TILE), F32),
                pltpu.VMEM((128, 128), F32),
                dma(2, nz), dma(2, nz), dma(4, ng), dma(2, NS), dma(2, NS), dma(NS), dma(NS), dma(ng), dma(2, ng),
                dma(2, NS), dma(2, NS), dma(NS), dma(NS), dma(NS), dma(NS), pltpu.SemaphoreType.DMA,
            ],
            compiler_params=pltpu.CompilerParams(
                collective_id=0, has_side_effects=True, vmem_limit_bytes=56 * 1024 * 1024
            ),
            name="lanczos",
        )(
            wave_rows.transpose(1, 2, 0, 3).reshape(PAIR, rows, right_dim),
            left_rows,
            op_pair.transpose(1, 2, 0),
            right_env,
        )
        short = jax.ShapeDtypeStruct((NUM_STEPS,), F32)
        vecs, alpha, beta = pl.pallas_call(
            end_kernel,
            out_shape=(jax.ShapeDtypeStruct(vecs.shape, F32), short, short),
            in_specs=vmem(1) + [smem],
            out_specs=(vmem(1)[0], smem, smem),
            name="result",
        )(vecs, ab)
        vecs = vecs.reshape(nv, 3, 3, rows, right_dim).transpose(0, 3, 1, 2, 4)
        return vecs, alpha, beta

    return jax.shard_map(
        local_run,
        mesh=mesh,
        in_specs=(P(ROW), P(None, ROW), P(), P()),
        out_specs=(P(None, ROW), P(), P()),
        check_vma=False,
    )
```

```python
import functools

import jax
import jax.numpy as jnp
from jax import lax
from jax.experimental import pallas as pl
from jax.experimental.pallas import tpu as pltpu
from jax.sharding import PartitionSpec as P

NUM_STEPS = 6
ROW = "rows"
NY, NX, NC = 4, 4, 2
NS = NY * NX
PAIR = 9
BW = 32
BLK = 72
HALVES = (slice(0, 32), slice(32, 72))
LANES = 128
TILE, ROWVEC = (8, LANES), (1, LANES)
PAIRED, QUAD = range(2), range(4)
MESH = pl.DeviceIdType.MESH
F32, BF16 = jnp.float32, jnp.bfloat16
OFFSETS = sorted(
    [(dy, dx) for dy in range(NY) for dx in range(NX) if (dy, dx) != (0, 0)],
    key=lambda o: (-(min(o[0], NY - o[0]) + min(o[1], NX - o[1])), o),
)


def span(k, width):
    return slice(k * width, k * width + width)


GROUPS = [(k, span(k, LANES)) for k in QUAD]
ROW0, ROW1, ROW2, ROW3, ROW4 = [span(k, 1) for k in range(5)]


def place():
    me = lax.axis_index(ROW)
    return me // (NS * NC), (me // (NX * NC)) % NY, (me // NC) % NX, me % NC


def device(z, y, x, core):
    return ((z * NY + y) * NX + x) * NC + core


def rcopy(src, dst, send_sem, recv_sem, dev):
    return pltpu.make_async_remote_copy(
        src_ref=src, dst_ref=dst, send_sem=send_sem, recv_sem=recv_sem, device_id=(dev,), device_id_type=MESH
    )


def knock(devs):
    for dev in devs:
        pl.semaphore_signal(pltpu.get_barrier_semaphore(), inc=1, device_id=(dev,), device_id_type=MESH)


def enter(devs):
    pl.semaphore_wait(pltpu.get_barrier_semaphore(), len(devs))


def plane_peers(z, y, x, core):
    out = []
    for dy, dx in OFFSETS:
        py, px = (y + dy) % NY, (x + dx) % NX
        out.append((py * NX + px, device(z, py, px, core)))
    return out


def swap4(a, b, c, d):
    lane = lax.broadcasted_iota(jnp.int32, a.shape, 1)
    low = lane < 64
    even = (lane // 32) % 2 == 0
    a, c = jnp.where(low, a, pltpu.roll(c, 64, 1)), jnp.where(low, pltpu.roll(a, 64, 1), c)
    b, d = jnp.where(low, b, pltpu.roll(d, 64, 1)), jnp.where(low, pltpu.roll(b, 64, 1), d)
    a, b = jnp.where(even, a, pltpu.roll(b, 32, 1)), jnp.where(even, pltpu.roll(a, 96, 1), b)
    c, d = jnp.where(even, c, pltpu.roll(d, 32, 1)), jnp.where(even, pltpu.roll(c, 96, 1), d)
    return a, b, c, d


def fold(val):
    return jnp.sum(val.reshape(BLK // 8, *TILE), axis=0)


def total(val):
    one = jnp.sum(jnp.sum(val, axis=0, keepdims=True), axis=1, keepdims=True)
    return jnp.broadcast_to(one, ROWVEC)


def block(main, last):
    return jnp.concatenate([main[0], main[1], last], axis=0)


def pack_last(rows):
    grp = lax.broadcasted_iota(jnp.int32, TILE, 1) // 32
    packed = rows[0:8]
    for t in range(1, 4):
        packed = jnp.where(grp == t, pltpu.roll(rows[span(t, 8)], 32 * t, 1), packed)
    return packed


def unpack_last(tile):
    return jnp.concatenate([tile if t == 0 else pltpu.roll(tile, 128 - 32 * t, 1) for t in QUAD], axis=0)


def pack_sums(vals):
    lane = lax.broadcasted_iota(jnp.int32, ROWVEC, 1)
    row = vals[4]
    for k in reversed(QUAD):
        row = jnp.where(lane == k, vals[k], row)
    return row


def unpack_sums(rows):
    rows = jnp.concatenate(rows, axis=0)
    lane = lax.broadcasted_iota(jnp.int32, rows.shape, 1)
    return [jnp.sum(jnp.where(lane == k, rows, 0.0), axis=1, keepdims=True) for k in range(5)]


def down(val):
    return jnp.sum(val, axis=0, keepdims=True)


def ratio(num, den):
    some = den > 0.0
    return jnp.where(some, num / jnp.where(some, den, 1.0), 0.0)


def main_kernel(
    nz, count, psi_ref, left_ref, op_ref, right_ref, vec_ref, ab_ref,
    gbuf, vb, ut, xt, y2, sbuf, rbuf, abuf, asend, cbuf, lt, r2, wv, lf, lsend, lrecv, rt, psend, precv, osend, orecv, mt,
    g_ss, d_ss, g_rs, r_ss, r_rs, a_ss, a_rs, c_ss, c_rs, l_ss, l_rs, p_ss, p_rs, o_ss, o_rs, rt_sem,
):
    ng = nz * NC
    terms = left_ref.shape[0]
    left_dim = left_ref.shape[2]
    z, y, x, core = place()
    i, j = core * nz + z, y * NX + x
    peers = plane_peers(z, y, x, core)
    mate = device(z, y, x, 1 - core)
    zs = [((z + dz) % nz, dz) for dz in sorted(range(1, nz), key=lambda dz: (min(dz, nz - dz), dz))]
    line = [(core, pz, dz) for pz, dz in zs] + [(1 - core, pz, nz + dz) for pz, dz in zs] + [(1 - core, z, nz)]

    load_right = pltpu.make_async_copy(right_ref.at[:, pl.ds(pl.multiple_of(j * BW, BW), BW), :], rt, rt_sem)
    load_right.start()
    others = [dev for _, dev in peers] + [device(pz, y, x, pc) for pc, pz, _ in line]
    knock(others)

    def start_gather(par, half):
        own = gbuf.at[par, i, HALVES[half]]
        for pz, dz in reversed(zs):
            rcopy(own, own, g_ss.at[half, dz], g_rs.at[2 * par + half, i], device(pz, y, x, core)).start()
        rcopy(own, own, g_ss.at[half, 0], g_rs.at[2 * par + half, i], mate).start()

    def relay(par, half):
        for pz, dz in zs:
            slot = core * nz + pz
            ref = gbuf.at[par, slot, HALVES[half]]
            rcopy(ref, ref, g_ss.at[half, dz], g_rs.at[2 * par + half, slot], mate).wait_recv()
            rcopy(ref, ref, d_ss.at[half, dz], g_rs.at[2 * par + half, slot], mate).start()

    def finish_gather(par):
        for half in PAIRED:
            for dz in range(nz):
                slot = (1 - core) * nz + (z + dz) % nz
                ref = gbuf.at[par, slot, HALVES[half]]
                rcopy(ref, ref, g_ss.at[half, 0], g_rs.at[2 * par + half, slot], mate).wait_recv()
    def drain_gather(par):
        for half in PAIRED:
            own = gbuf.at[par, i, HALVES[half]]
            rcopy(own, own, g_ss.at[half, 0], g_rs.at[2 * par + half, i], mate).wait_send()
            for pz, dz in zs:
                ref = gbuf.at[par, core * nz + pz, HALVES[half]]
                rcopy(own, own, g_ss.at[half, dz], g_rs.at[2 * par + half, i], mate).wait_send()
                rcopy(ref, ref, d_ss.at[half, dz], g_rs.at[2 * par + half, i], mate).wait_send()

    def start_line(par, vals):
        cbuf[par, pl.ds(i, 1)] = pack_sums(vals)[None]
        own = cbuf.at[par, i]
        for pc, pz, k in line:
            rcopy(own, own, c_ss.at[k], c_rs.at[par, i], device(pz, y, x, pc)).start()

    def finish_line(par):
        own = cbuf.at[par, i]
        for pc, pz, k in line:
            slot = pc * nz + pz
            rcopy(own, cbuf.at[par, slot], c_ss.at[k], c_rs.at[par, slot], mate).wait_recv()
        m, p, nn, ee, ev = unpack_sums([cbuf[par, s] for s in range(ng)])
        alpha = down(m) / count
        off = p - alpha
        square = down(ee + 2.0 * (off * ev) + (off * nn) * off)
        return jnp.broadcast_to(alpha, ROWVEC), jnp.broadcast_to(jnp.sqrt(square / count), ROWVEC)

    def start_plane(par, beta_prev):
        w, v, vp = gbuf[par, i], vb[1 - par, i], vb[par, i]
        rest = w - beta_prev * vp
        m, yv, nn = total(fold(w * v)), total(fold(rest * v)), total(fold(v * v))
        p = ratio(yv, nn)
        e = rest - p * v
        tile = pack_sums([m, p, nn, total(fold(e * e)), total(fold(e * v))])
        asend[...] = tile
        for pj, dev in peers:
            rcopy(asend, abuf.at[j], a_ss.at[pj], a_rs.at[j], dev).start()
        abuf[pl.ds(j, 1)] = tile[None]

    def finish_plane():
        for pj, dev in peers:
            rcopy(asend, abuf.at[pj], a_ss.at[pj], a_rs.at[pj], dev).wait_recv()
        m, p, nn, ee, ev = unpack_sums([abuf[s] for s in range(NS)])
        whole = ratio(down(p * nn), down(nn))
        off = p - whole
        sums = [down(m), whole, down(nn), down(ee + 2.0 * (off * ev) + (off * nn) * off), down(ev + off * nn)]
        return [jnp.broadcast_to(val, ROWVEC) for val in sums]

    def start_out(par):
        blk = gbuf[par, i]
        last = unpack_last(blk[64:72])
        mt[...] = jnp.concatenate([blk[:64], last, jnp.zeros((32, 128), F32)], axis=0).T
        for pj in range(NS):
            for k in QUAD:
                osend[pj, span(k, 2)] = mt[span(k * NS + pj, 2)]
        for pj, dev in peers:
            rcopy(osend.at[pj], orecv.at[j], o_ss.at[pj], o_rs.at[j], dev).start()
        orecv[pl.ds(j, 1)] = osend[pl.ds(j, 1)]

    def finish_out(num):
        for pj, dev in peers:
            rcopy(osend.at[pj], orecv.at[pj], o_ss.at[pj], o_rs.at[pj], dev).wait_recv()
        for grp, lanes in GROUPS:
            outs = swap4(*[orecv[grp * 4 + k] for k in QUAD])
            for t in PAIRED:
                for k in QUAD:
                    vec_ref[num, 4 * t + k, :, lanes] = outs[t][span(k, 2)]
            vec_ref[num, 8, :, lanes] = outs[2][0:2]

    def own_rows(num, alpha, beta_prev, beta):
        older = num - 2 if isinstance(num, int) else jnp.maximum(num - 2, 0)
        for grp, lanes in GROUPS:
            for q in range(PAIR):
                w, v, vp = vec_ref[num, q, :, lanes], vec_ref[num - 1, q, :, lanes], vec_ref[older, q, :, lanes]
                vec_ref[num, q, :, lanes] = (w - alpha * v - beta_prev * vp) / beta

    def update(par, alpha, beta_prev, beta, first, size):
        def body(s, carry):
            w, v, vp = gbuf[par, s], vb[1 - par, s], vb[par, s]
            vb[par, pl.ds(s, 1)] = ((w - alpha * v - beta_prev * vp) / beta)[None]
            return carry

        lax.fori_loop(first, first + size, body, 0, unroll=4 if size > 1 else 1)

    def left_and_mix(par):
        for grp in range(ng // 4):
            lanes = span(grp, LANES)
            for t in PAIRED:
                outs = swap4(*[vb[par, grp * 4 + ii, span(t, BW)] for ii in QUAD])
                for k in QUAD:
                    q = 4 * t + k
                    ut[span(q, BW), lanes] = outs[k].astype(BF16)
            outs = swap4(*[vb[par, grp * 4 + ii, 64:72] for ii in QUAD])
            ut[256:272, lanes] = jnp.concatenate(outs[:2], axis=0).astype(BF16)
            ut[272:288, lanes] = jnp.concatenate(outs[2:], axis=0).astype(BF16)
        width = 256
        for part in range(terms * BW // width):
            cols = span(part, width)
            whole = jnp.dot(ut[...], lt[:, cols], preferred_element_type=F32).astype(BF16).astype(F32)
            xt[:, cols] = whole
            for sub in range(width // LANES):
                grp = part * (width // LANES) + sub
                mix(0, grp, [xt[span(r, BW), span(grp, LANES)] for r in range(PAIR)])

    def mix(half, grp, xs):
        lanes = span(grp, LANES)
        for part in PAIRED:
            some = [x_r[span(part, 16)] for x_r in xs]

            def one(q):
                acc = wv[q * 16 : q * 16 + 1, lanes] * some[0]
                for r in range(1, PAIR):
                    acc = acc + wv[q * 16 + r : q * 16 + r + 1, lanes] * some[r]
                return acc

            rows = [span(grp * 8 + 2 * k + part, 16) for k in QUAD]
            outs = swap4(*[one(4 * half + k) for k in QUAD])
            for k in QUAD:
                y2[rows[k], span(half, LANES)] = outs[k].astype(BF16)
            if half:
                last = one(8)
                for k in QUAD:
                    moved = last if k == 0 else pltpu.roll(last, LANES - BW * k, 1)
                    y2[rows[k], 2 * LANES :] = moved.astype(BF16)

    def mix_rest():
        for grp in range(terms * BW // LANES):
            mix(1, grp, [xt[span(r, BW), span(grp, LANES)] for r in range(PAIR)])

    def start_scatter(half):
        cols = slice(0, 128) if half == 0 else slice(128, 384)
        for dy in (2, 1, 3, 0):
            py = (y + dy) % NY
            part = jnp.dot(
                r2[pl.ds(pl.multiple_of(py * 128, 128), 128), :], y2[:, cols], preferred_element_type=F32
            )
            for px in range(NX):
                pj = py * NX + px
                rows = part[span(px, BW)]
                if half == 0:
                    sbuf[pj, 0:32] = rows
                else:
                    sbuf[pj, 32:64] = rows[:, 0:128]
                    sbuf[pj, 64:72] = pack_last(rows[:, 128:256])
                send = rcopy(
                    sbuf.at[pj, HALVES[half]], rbuf.at[j, HALVES[half]],
                    r_ss.at[half, pj], r_rs.at[half, j], device(z, py, px, core),
                )
                if dy:
                    send.start()
                else:

                    @pl.when(px != x)
                    def _():
                        send.start()

        rbuf[pl.ds(j, 1), HALVES[half]] = sbuf[pl.ds(j, 1), HALVES[half]]

    def finish_scatter(nxt, half):
        for pj, dev in reversed(peers):
            rcopy(
                sbuf.at[pj, HALVES[half]], rbuf.at[pj, HALVES[half]], r_ss.at[half, pj], r_rs.at[half, pj], dev
            ).wait_recv()
        w = rbuf[0, HALVES[half]]
        for s in range(1, NS):
            w = w + rbuf[s, HALVES[half]]
        gbuf[nxt, pl.ds(i, 1), HALVES[half]] = w[None]

    def drain_sums(par):
        for pj, dev in peers:
            rcopy(asend, abuf.at[pj], a_ss.at[pj], a_rs.at[pj], dev).wait_send()
            rcopy(osend.at[pj], orecv.at[pj], o_ss.at[pj], o_rs.at[pj], dev).wait_send()
        drain_line(par)

    def drain_line(par):
        own = cbuf.at[par, i]
        for pc, pz, k in line:
            rcopy(own, own, c_ss.at[k], c_rs.at[par, i], mate).wait_send()

    def drain_scatter():
        for half in PAIRED:
            for pj, dev in peers:
                ref = sbuf.at[pj, HALVES[half]]
                rcopy(ref, ref, r_ss.at[half, pj], r_rs.at[half, pj], dev).wait_send()

    def product(par, nxt, more, between):
        left_and_mix(par)
        start_scatter(0)
        mix_rest()
        start_scatter(1)
        drain_gather(par)
        between()
        for half in PAIRED:
            finish_scatter(nxt, half)
            if more is True:
                start_gather(nxt, half)
            else:

                @pl.when(more)
                def _(half=half):
                    start_gather(nxt, half)

    norm = jnp.zeros(ROWVEC, F32)
    for grp, lanes in GROUPS:
        for q in range(PAIR):
            norm = norm + jnp.sum(psi_ref[q, :, lanes] * psi_ref[q, :, lanes], axis=0, keepdims=True)
    norm = jnp.broadcast_to(jnp.sum(norm, axis=1, keepdims=True), TILE)
    for t in range(3):
        mt[span(t, 8)] = jnp.zeros(TILE, F32)
    for grp, lanes in GROUPS:
        for q in range(PAIR):
            mt[span(q, 2)] = psi_ref[q, :, lanes]
        outs = swap4(mt[0:8], mt[8:16], mt[16:24], norm)
        for k in QUAD:
            psend[grp * 4 + k] = outs[k]
    for k in range(terms):
        lf[span(k, 2)] = left_ref[k].astype(F32)
    row = lax.broadcasted_iota(jnp.int32, (left_dim, left_dim), 0)
    col = lax.broadcasted_iota(jnp.int32, (left_dim, left_dim), 1)
    goal = ((row >> 1) & 1) * (nz * BW) + (row >> 6) * BW + ((row >> 2) & 15) * 2 + (row & 1)
    perm = jnp.where(goal == col, 1.0, 0.0).astype(BF16)
    lsend[...] = jnp.dot(lf[...].astype(BF16), perm, preferred_element_type=F32).astype(BF16)
    enter(others)
    for pj, dev in peers:
        rcopy(psend.at[pj], precv.at[j], p_ss.at[pj], p_rs.at[j], dev).start()
    precv[pl.ds(j, 1)] = psend[pl.ds(j, 1)]
    lhalf = [span(k, terms) for k in PAIRED]
    for k in PAIRED:
        for pj, dev in peers:
            rcopy(lsend.at[lhalf[k]], lrecv.at[j, lhalf[k]], l_ss.at[k, pj], l_rs.at[k, j], dev).start()
    lrecv[pl.ds(j, 1)] = lsend[...][None]

    term = lax.broadcasted_iota(jnp.int32, (terms, terms * BW), 0)
    lane = lax.broadcasted_iota(jnp.int32, (terms, terms * BW), 1)
    spread = jnp.where((lane >> 5) == term, 1.0, 0.0).astype(BF16)
    for q in range(PAIR):
        wv[q * 16 : q * 16 + PAIR] = jnp.dot(op_ref[q], spread, preferred_element_type=F32)
    vb[...] = jnp.zeros_like(vb)

    for pj, dev in peers:
        rcopy(psend.at[pj], precv.at[pj], p_ss.at[pj], p_rs.at[pj], dev).wait_recv()
    square = precv[0, ROW0]
    for s in range(1, NS):
        square = square + precv[s, ROW0]
    square = jnp.where(lax.broadcasted_iota(jnp.int32, ROWVEC, 1) >= 96, square, 0.0)
    square = square + pltpu.roll(square, 64, 1)
    square = square + pltpu.roll(square, 32, 1)
    for s in range(NS):
        for k in QUAD:
            mt[span(k * NS + s, 2)] = precv[s, span(k, 2)]
    flat = mt[...].T
    gbuf[0, pl.ds(i, 1)] = block((flat[span(0, BW)], flat[span(1, BW)]), pack_last(flat[span(2, BW)]))[None]
    start_gather(0, 0)
    start_gather(0, 1)
    zero = jnp.zeros(ROWVEC, F32)
    start_line(0, [zero, zero, zero, square, zero])

    load_right.wait()
    for part in range(terms * BW // 128):
        rows = rt[span(part, 4)].reshape(128, rt.shape[2])
        r2[:, span(part, LANES)] = rows.T

    relay(0, 0)
    relay(0, 1)
    width = 8 * BW
    row = lax.broadcasted_iota(jnp.int32, (width, width), 0)
    col = lax.broadcasted_iota(jnp.int32, (width, width), 1)
    goal = ((row & 15) >> 1) * BW + (row >> 4) * 2 + (row & 1)
    perm = jnp.where(goal == col, 1.0, 0.0).astype(BF16)
    parts = terms // 8
    for part in range(parts):
        for k in PAIRED:
            if part == k * parts // 2:
                for pj, dev in peers:
                    rcopy(
                        lsend.at[lhalf[k]], lrecv.at[pj, lhalf[k]], l_ss.at[k, pj], l_rs.at[k, pj], dev
                    ).wait_recv()
        mine = lrecv[:, span(part, 16), :].reshape(width, left_dim)
        lt[:, span(part, width)] = lax.dot_general(
            mine, perm, (((0,), (0,)), ((), ())), preferred_element_type=F32
        ).astype(BF16)
    finish_gather(0)
    alpha, beta = finish_line(0)
    update(0, zero, zero, beta, 0, ng)

    def first_rows():
        drain_line(0)
        for pj, dev in peers:
            rcopy(psend.at[pj], precv.at[pj], p_ss.at[pj], p_rs.at[pj], dev).wait_send()
            for k in PAIRED:
                rcopy(lsend.at[lhalf[k]], lrecv.at[pj, lhalf[k]], l_ss.at[k, pj], l_rs.at[k, pj], dev).wait_send()
        for grp, lanes in GROUPS:
            for q in range(PAIR):
                vec_ref[0, q, :, lanes] = psi_ref[q, :, lanes] / beta

    product(0, 1, True, first_rows)

    def step(t, beta_prev):
        par = t % 2
        start_plane(par, beta_prev)
        drain_scatter()
        relay(par, 0)
        start_line(par, finish_plane())
        start_out(par)
        relay(par, 1)
        finish_gather(par)
        alpha, beta = finish_line(par)
        update(par, alpha, beta_prev, beta, 0, ng)

        def rest():
            finish_out(t)
            drain_sums(par)
            ab_ref[0, t - 1] = alpha[0, 0]
            ab_ref[1, t - 1] = beta[0, 0]
            own_rows(t, alpha, beta_prev, beta)

        product(par, 1 - par, t < NUM_STEPS - 1, rest)
        return beta

    beta_prev = lax.fori_loop(1, NUM_STEPS, step, zero)
    par = NUM_STEPS % 2
    start_plane(par, beta_prev)
    drain_scatter()
    start_line(par, finish_plane())
    start_out(par)
    finish_out(NUM_STEPS)
    alpha, beta = finish_line(par)
    ab_ref[0, NUM_STEPS - 1] = alpha[0, 0]
    ab_ref[1, NUM_STEPS - 1] = beta[0, 0]
    own_rows(NUM_STEPS, alpha, beta_prev, beta)
    drain_sums(par)


def end_kernel(vec_ref, ab_ref, vec_out, alpha_out, beta_out):
    vec_out[...] = vec_ref[...]
    for k in range(NUM_STEPS):
        alpha_out[k] = ab_ref[0, k]
        beta_out[k] = ab_ref[1, k]


def vmem(n):
    return [pl.BlockSpec(memory_space=pltpu.VMEM)] * n


def dma(*shape):
    return pltpu.SemaphoreType.DMA(shape)


def solution(mesh):
    nz = mesh.shape[ROW] // (NS * NC)
    ng = nz * NC

    def local_run(wave_rows, left_rows, op_pair, right_env):
        terms, rows, left_dim = left_rows.shape
        right_dim = right_env.shape[1]
        count = left_dim * right_dim * PAIR
        nv = NUM_STEPS + 1
        smem = pl.BlockSpec(memory_space=pltpu.SMEM)
        vecs, ab = pl.pallas_call(
            functools.partial(main_kernel, nz, float(count)),
            out_shape=(
                jax.ShapeDtypeStruct((nv, PAIR, rows, right_dim), F32),
                jax.ShapeDtypeStruct((2, NUM_STEPS), F32),
            ),
            in_specs=vmem(3) + [pl.BlockSpec(memory_space=pl.ANY)],
            out_specs=(vmem(1)[0], smem),
            scratch_shapes=[
                pltpu.VMEM((2, ng, BLK, LANES), F32),
                pltpu.VMEM((2, ng, BLK, LANES), F32),
                pltpu.VMEM((PAIR * BW, left_dim), BF16),
                pltpu.VMEM((PAIR * BW, terms * BW), F32),
                pltpu.VMEM((terms * BW, 384), BF16),
                pltpu.VMEM((NS, BLK, LANES), F32),
                pltpu.VMEM((NS, BLK, LANES), F32),
                pltpu.VMEM((NS, *ROWVEC), F32),
                pltpu.VMEM(ROWVEC, F32),
                pltpu.VMEM((2, ng, *ROWVEC), F32),
                pltpu.VMEM((left_dim, terms * BW), BF16),
                pltpu.VMEM((right_dim, terms * BW), BF16),
                pltpu.VMEM((PAIR * 16, terms * BW), F32),
                pltpu.VMEM((terms * rows, left_dim), F32),
                pltpu.VMEM((terms * rows, left_dim), BF16),
                pltpu.VMEM((NS, terms * rows, left_dim), BF16),
                pltpu.VMEM((terms, BW, right_dim), BF16),
                pltpu.VMEM((NS, *TILE), F32),
                pltpu.VMEM((NS, *TILE), F32),
                pltpu.VMEM((NS, *TILE), F32),
                pltpu.VMEM((NS, *TILE), F32),
                pltpu.VMEM((128, 128), F32),
                dma(2, nz), dma(2, nz), dma(4, ng), dma(2, NS), dma(2, NS), dma(NS), dma(NS), dma(ng), dma(2, ng),
                dma(2, NS), dma(2, NS), dma(NS), dma(NS), dma(NS), dma(NS), pltpu.SemaphoreType.DMA,
            ],
            compiler_params=pltpu.CompilerParams(
                collective_id=0, has_side_effects=True, vmem_limit_bytes=56 * 1024 * 1024
            ),
            name="lanczos",
        )(
            wave_rows.transpose(1, 2, 0, 3).reshape(PAIR, rows, right_dim),
            left_rows,
            op_pair.transpose(1, 2, 0),
            right_env,
        )
        short = jax.ShapeDtypeStruct((NUM_STEPS,), F32)
        vecs, alpha, beta = pl.pallas_call(
            end_kernel,
            out_shape=(jax.ShapeDtypeStruct(vecs.shape, F32), short, short),
            in_specs=vmem(1) + [smem],
            out_specs=(vmem(1)[0], smem, smem),
            name="result",
        )(vecs, ab)
        vecs = vecs.reshape(nv, 3, 3, rows, right_dim).transpose(0, 3, 1, 2, 4)
        return vecs, alpha, beta

    return jax.shard_map(
        local_run,
        mesh=mesh,
        in_specs=(P(ROW), P(None, ROW), P(), P()),
        out_specs=(P(None, ROW), P(), P()),
        check_vma=False,
    )
```

```python
import functools

import jax
import jax.numpy as jnp
from jax import lax
from jax.experimental import pallas as pl
from jax.experimental.pallas import tpu as pltpu
from jax.sharding import PartitionSpec as P

NUM_STEPS = 6
ROW = "rows"
NY, NX, NC = 4, 4, 2
NS = NY * NX
PAIR = 9
BW = 32
BLK = 72
HALVES = (slice(0, 32), slice(32, 72))
LANES = 128
TILE, ROWVEC = (8, LANES), (1, LANES)
PAIRED, QUAD = range(2), range(4)
MESH = pl.DeviceIdType.MESH
F32, BF16 = jnp.float32, jnp.bfloat16
OFFSETS = sorted(
    [(dy, dx) for dy in range(NY) for dx in range(NX) if (dy, dx) != (0, 0)],
    key=lambda o: (-(min(o[0], NY - o[0]) + min(o[1], NX - o[1])), o),
)


def span(k, width):
    return slice(k * width, k * width + width)


GROUPS = [(k, span(k, LANES)) for k in QUAD]
ROW0, ROW1, ROW2, ROW3, ROW4 = [span(k, 1) for k in range(5)]


def place():
    me = lax.axis_index(ROW)
    return me // (NS * NC), (me // (NX * NC)) % NY, (me // NC) % NX, me % NC


def device(z, y, x, core):
    return ((z * NY + y) * NX + x) * NC + core


def rcopy(src, dst, send_sem, recv_sem, dev):
    return pltpu.make_async_remote_copy(
        src_ref=src, dst_ref=dst, send_sem=send_sem, recv_sem=recv_sem, device_id=(dev,), device_id_type=MESH
    )


def knock(devs):
    for dev in devs:
        pl.semaphore_signal(pltpu.get_barrier_semaphore(), inc=1, device_id=(dev,), device_id_type=MESH)


def enter(devs):
    pl.semaphore_wait(pltpu.get_barrier_semaphore(), len(devs))


def plane_peers(z, y, x, core):
    out = []
    for dy, dx in OFFSETS:
        py, px = (y + dy) % NY, (x + dx) % NX
        out.append((py * NX + px, device(z, py, px, core)))
    return out


def swap4(a, b, c, d):
    lane = lax.broadcasted_iota(jnp.int32, a.shape, 1)
    low = lane < 64
    even = (lane // 32) % 2 == 0
    a, c = jnp.where(low, a, pltpu.roll(c, 64, 1)), jnp.where(low, pltpu.roll(a, 64, 1), c)
    b, d = jnp.where(low, b, pltpu.roll(d, 64, 1)), jnp.where(low, pltpu.roll(b, 64, 1), d)
    a, b = jnp.where(even, a, pltpu.roll(b, 32, 1)), jnp.where(even, pltpu.roll(a, 96, 1), b)
    c, d = jnp.where(even, c, pltpu.roll(d, 32, 1)), jnp.where(even, pltpu.roll(c, 96, 1), d)
    return a, b, c, d


def fold(val):
    return jnp.sum(val.reshape(BLK // 8, *TILE), axis=0)


def total(val):
    one = jnp.sum(jnp.sum(val, axis=0, keepdims=True), axis=1, keepdims=True)
    return jnp.broadcast_to(one, ROWVEC)


def block(main, last):
    return jnp.concatenate([main[0], main[1], last], axis=0)


def pack_last(rows):
    grp = lax.broadcasted_iota(jnp.int32, TILE, 1) // 32
    packed = rows[0:8]
    for t in range(1, 4):
        packed = jnp.where(grp == t, pltpu.roll(rows[span(t, 8)], 32 * t, 1), packed)
    return packed


def unpack_last(tile):
    return jnp.concatenate([tile if t == 0 else pltpu.roll(tile, 128 - 32 * t, 1) for t in QUAD], axis=0)


def rows5(vals):
    row = lax.broadcasted_iota(jnp.int32, TILE, 0)
    tile = vals[4]
    for k in (3, 2, 1, 0):
        tile = jnp.where(row == k, vals[k], tile)
    return jnp.broadcast_to(tile, TILE)


def ratio(num, den):
    some = den > 0.0
    return jnp.where(some, num / jnp.where(some, den, 1.0), 0.0)


def main_kernel(
    nz, count, psi_ref, left_ref, op_ref, right_ref, vec_ref, ab_ref,
    gbuf, vb, ut, xt, y2, sbuf, rbuf, abuf, asend, cbuf, lt, r2, wv, lf, lsend, lrecv, rt, psend, precv, osend, orecv, mt,
    g_ss, d_ss, g_rs, r_ss, r_rs, a_ss, a_rs, c_ss, c_rs, l_ss, l_rs, p_ss, p_rs, o_ss, o_rs, rt_sem,
):
    ng = nz * NC
    terms = left_ref.shape[0]
    left_dim = left_ref.shape[2]
    z, y, x, core = place()
    i, j = core * nz + z, y * NX + x
    peers = plane_peers(z, y, x, core)
    mate = device(z, y, x, 1 - core)
    zs = [((z + dz) % nz, dz) for dz in sorted(range(1, nz), key=lambda dz: (min(dz, nz - dz), dz))]
    line = [(core, pz, dz) for pz, dz in zs] + [(1 - core, pz, nz + dz) for pz, dz in zs] + [(1 - core, z, nz)]

    load_right = pltpu.make_async_copy(right_ref.at[:, pl.ds(pl.multiple_of(j * BW, BW), BW), :], rt, rt_sem)
    load_right.start()
    others = [dev for _, dev in peers] + [device(pz, y, x, pc) for pc, pz, _ in line]
    knock(others)

    def start_gather(par, half):
        own = gbuf.at[par, i, HALVES[half]]
        for pz, dz in reversed(zs):
            rcopy(own, own, g_ss.at[half, dz], g_rs.at[2 * par + half, i], device(pz, y, x, core)).start()
        rcopy(own, own, g_ss.at[half, 0], g_rs.at[2 * par + half, i], mate).start()

    def relay(par, half):
        for pz, dz in zs:
            slot = core * nz + pz
            ref = gbuf.at[par, slot, HALVES[half]]
            rcopy(ref, ref, g_ss.at[half, dz], g_rs.at[2 * par + half, slot], mate).wait_recv()
            rcopy(ref, ref, d_ss.at[half, dz], g_rs.at[2 * par + half, slot], mate).start()

    def finish_gather(par):
        for half in PAIRED:
            for dz in range(nz):
                slot = (1 - core) * nz + (z + dz) % nz
                ref = gbuf.at[par, slot, HALVES[half]]
                rcopy(ref, ref, g_ss.at[half, 0], g_rs.at[2 * par + half, slot], mate).wait_recv()
    def drain_gather(par):
        for half in PAIRED:
            own = gbuf.at[par, i, HALVES[half]]
            rcopy(own, own, g_ss.at[half, 0], g_rs.at[2 * par + half, i], mate).wait_send()
            for pz, dz in zs:
                ref = gbuf.at[par, core * nz + pz, HALVES[half]]
                rcopy(own, own, g_ss.at[half, dz], g_rs.at[2 * par + half, i], mate).wait_send()
                rcopy(ref, ref, d_ss.at[half, dz], g_rs.at[2 * par + half, i], mate).wait_send()

    def start_line(par, vals):
        lane = lax.broadcasted_iota(jnp.int32, ROWVEC, 1)
        line_row = vals[4]
        for k in reversed(QUAD):
            line_row = jnp.where(lane == k, vals[k], line_row)
        cbuf[par, pl.ds(i, 1)] = line_row[None]
        own = cbuf.at[par, i]
        for pc, pz, k in line:
            rcopy(own, own, c_ss.at[k], c_rs.at[par, i], device(pz, y, x, pc)).start()

    def finish_line(par):
        own = cbuf.at[par, i]
        for pc, pz, k in line:
            slot = pc * nz + pz
            rcopy(own, cbuf.at[par, slot], c_ss.at[k], c_rs.at[par, slot], mate).wait_recv()
        rows = jnp.concatenate([cbuf[par, s] for s in range(ng)], axis=0)
        lane = lax.broadcasted_iota(jnp.int32, rows.shape, 1)
        m, p, nn, ee, ev = [jnp.sum(jnp.where(lane == k, rows, 0.0), axis=1, keepdims=True) for k in range(5)]
        alpha = jnp.sum(m, axis=0, keepdims=True) / count
        off = p - alpha
        square = jnp.sum(ee + 2.0 * (off * ev) + (off * nn) * off, axis=0, keepdims=True)
        return jnp.broadcast_to(alpha, ROWVEC), jnp.broadcast_to(jnp.sqrt(square / count), ROWVEC)

    def start_plane(par, beta_prev):
        w, v, vp = gbuf[par, i], vb[1 - par, i], vb[par, i]
        rest = w - beta_prev * vp
        m, yv, nn = total(fold(w * v)), total(fold(rest * v)), total(fold(v * v))
        p = ratio(yv, nn)
        e = rest - p * v
        tile = rows5([m, p, nn, total(fold(e * e)), total(fold(e * v))])
        asend[...] = tile
        for pj, dev in peers:
            rcopy(asend, abuf.at[j], a_ss.at[pj], a_rs.at[j], dev).start()
        abuf[pl.ds(j, 1)] = tile[None]

    def finish_plane():
        for pj, dev in peers:
            rcopy(asend, abuf.at[pj], a_ss.at[pj], a_rs.at[pj], dev).wait_recv()
        zero = jnp.zeros(ROWVEC, F32)
        m, nn, pn, ee, ev = zero, zero, zero, zero, zero
        for s in range(NS):
            m, nn, pn = m + abuf[s, ROW0], nn + abuf[s, ROW2], pn + abuf[s, ROW1] * abuf[s, ROW2]
        p = ratio(pn, nn)
        for s in range(NS):
            off = abuf[s, ROW1] - p
            ee = ee + (abuf[s, ROW3] + 2.0 * (off * abuf[s, ROW4]) + (off * abuf[s, ROW2]) * off)
            ev = ev + (abuf[s, ROW4] + off * abuf[s, ROW2])
        return [m, p, nn, ee, ev]

    def start_out(par):
        blk = gbuf[par, i]
        last = unpack_last(blk[64:72])
        mt[...] = jnp.concatenate([blk[:64], last, jnp.zeros((32, 128), F32)], axis=0).T
        for pj in range(NS):
            for k in QUAD:
                osend[pj, span(k, 2)] = mt[span(k * NS + pj, 2)]
        for pj, dev in peers:
            rcopy(osend.at[pj], orecv.at[j], o_ss.at[pj], o_rs.at[j], dev).start()
        orecv[pl.ds(j, 1)] = osend[pl.ds(j, 1)]

    def finish_out(num):
        for pj, dev in peers:
            rcopy(osend.at[pj], orecv.at[pj], o_ss.at[pj], o_rs.at[pj], dev).wait_recv()
        for grp, lanes in GROUPS:
            outs = swap4(*[orecv[grp * 4 + k] for k in QUAD])
            for t in PAIRED:
                for k in QUAD:
                    vec_ref[num, 4 * t + k, :, lanes] = outs[t][span(k, 2)]
            vec_ref[num, 8, :, lanes] = outs[2][0:2]

    def own_rows(num, alpha, beta_prev, beta):
        older = num - 2 if isinstance(num, int) else jnp.maximum(num - 2, 0)
        for grp, lanes in GROUPS:
            for q in range(PAIR):
                w, v, vp = vec_ref[num, q, :, lanes], vec_ref[num - 1, q, :, lanes], vec_ref[older, q, :, lanes]
                vec_ref[num, q, :, lanes] = (w - alpha * v - beta_prev * vp) / beta

    def update(par, alpha, beta_prev, beta, first, size):
        def body(s, carry):
            w, v, vp = gbuf[par, s], vb[1 - par, s], vb[par, s]
            vb[par, pl.ds(s, 1)] = ((w - alpha * v - beta_prev * vp) / beta)[None]
            return carry

        lax.fori_loop(first, first + size, body, 0, unroll=4 if size > 1 else 1)

    def left_and_mix(par):
        for grp in range(ng // 4):
            lanes = span(grp, LANES)
            for t in PAIRED:
                outs = swap4(*[vb[par, grp * 4 + ii, span(t, BW)] for ii in QUAD])
                for k in QUAD:
                    q = 4 * t + k
                    ut[span(q, BW), lanes] = outs[k].astype(BF16)
            outs = swap4(*[vb[par, grp * 4 + ii, 64:72] for ii in QUAD])
            ut[256:272, lanes] = jnp.concatenate(outs[:2], axis=0).astype(BF16)
            ut[272:288, lanes] = jnp.concatenate(outs[2:], axis=0).astype(BF16)
        width = 256
        for part in range(terms * BW // width):
            cols = span(part, width)
            whole = jnp.dot(ut[...], lt[:, cols], preferred_element_type=F32).astype(BF16).astype(F32)
            xt[:, cols] = whole
            for sub in range(width // LANES):
                grp = part * (width // LANES) + sub
                mix(0, grp, [xt[span(r, BW), span(grp, LANES)] for r in range(PAIR)])

    def mix(half, grp, xs):
        lanes = span(grp, LANES)
        for part in PAIRED:
            some = [x_r[span(part, 16)] for x_r in xs]

            def one(q):
                acc = wv[q * 16 : q * 16 + 1, lanes] * some[0]
                for r in range(1, PAIR):
                    acc = acc + wv[q * 16 + r : q * 16 + r + 1, lanes] * some[r]
                return acc

            rows = [span(grp * 8 + 2 * k + part, 16) for k in QUAD]
            outs = swap4(*[one(4 * half + k) for k in QUAD])
            for k in QUAD:
                y2[rows[k], span(half, LANES)] = outs[k].astype(BF16)
            if half:
                last = one(8)
                for k in QUAD:
                    moved = last if k == 0 else pltpu.roll(last, LANES - BW * k, 1)
                    y2[rows[k], 2 * LANES :] = moved.astype(BF16)

    def mix_rest():
        for grp in range(terms * BW // LANES):
            mix(1, grp, [xt[span(r, BW), span(grp, LANES)] for r in range(PAIR)])

    def start_scatter(half):
        cols = slice(0, 128) if half == 0 else slice(128, 384)
        for dy in (2, 1, 3, 0):
            py = (y + dy) % NY
            part = jnp.dot(
                r2[pl.ds(pl.multiple_of(py * 128, 128), 128), :], y2[:, cols], preferred_element_type=F32
            )
            for px in range(NX):
                pj = py * NX + px
                rows = part[span(px, BW)]
                if half == 0:
                    sbuf[pj, 0:32] = rows
                else:
                    sbuf[pj, 32:64] = rows[:, 0:128]
                    sbuf[pj, 64:72] = pack_last(rows[:, 128:256])
                send = rcopy(
                    sbuf.at[pj, HALVES[half]], rbuf.at[j, HALVES[half]],
                    r_ss.at[half, pj], r_rs.at[half, j], device(z, py, px, core),
                )
                if dy:
                    send.start()
                else:

                    @pl.when(px != x)
                    def _():
                        send.start()

        rbuf[pl.ds(j, 1), HALVES[half]] = sbuf[pl.ds(j, 1), HALVES[half]]

    def finish_scatter(nxt, half):
        for pj, dev in reversed(peers):
            rcopy(
                sbuf.at[pj, HALVES[half]], rbuf.at[pj, HALVES[half]], r_ss.at[half, pj], r_rs.at[half, pj], dev
            ).wait_recv()
        w = rbuf[0, HALVES[half]]
        for s in range(1, NS):
            w = w + rbuf[s, HALVES[half]]
        gbuf[nxt, pl.ds(i, 1), HALVES[half]] = w[None]

    def drain_sums(par):
        for pj, dev in peers:
            rcopy(asend, abuf.at[pj], a_ss.at[pj], a_rs.at[pj], dev).wait_send()
            rcopy(osend.at[pj], orecv.at[pj], o_ss.at[pj], o_rs.at[pj], dev).wait_send()
        drain_line(par)

    def drain_line(par):
        own = cbuf.at[par, i]
        for pc, pz, k in line:
            rcopy(own, own, c_ss.at[k], c_rs.at[par, i], mate).wait_send()

    def drain_scatter():
        for half in PAIRED:
            for pj, dev in peers:
                ref = sbuf.at[pj, HALVES[half]]
                rcopy(ref, ref, r_ss.at[half, pj], r_rs.at[half, pj], dev).wait_send()

    def product(par, nxt, more, between):
        left_and_mix(par)
        start_scatter(0)
        mix_rest()
        start_scatter(1)
        drain_gather(par)
        between()
        for half in PAIRED:
            finish_scatter(nxt, half)
            if more is True:
                start_gather(nxt, half)
            else:

                @pl.when(more)
                def _(half=half):
                    start_gather(nxt, half)

    norm = jnp.zeros(ROWVEC, F32)
    for grp, lanes in GROUPS:
        for q in range(PAIR):
            norm = norm + jnp.sum(psi_ref[q, :, lanes] * psi_ref[q, :, lanes], axis=0, keepdims=True)
    norm = jnp.broadcast_to(jnp.sum(norm, axis=1, keepdims=True), TILE)
    for t in range(3):
        mt[span(t, 8)] = jnp.zeros(TILE, F32)
    for grp, lanes in GROUPS:
        for q in range(PAIR):
            mt[span(q, 2)] = psi_ref[q, :, lanes]
        outs = swap4(mt[0:8], mt[8:16], mt[16:24], norm)
        for k in QUAD:
            psend[grp * 4 + k] = outs[k]
    for k in range(terms):
        lf[span(k, 2)] = left_ref[k].astype(F32)
    row = lax.broadcasted_iota(jnp.int32, (left_dim, left_dim), 0)
    col = lax.broadcasted_iota(jnp.int32, (left_dim, left_dim), 1)
    goal = ((row >> 1) & 1) * (nz * BW) + (row >> 6) * BW + ((row >> 2) & 15) * 2 + (row & 1)
    perm = jnp.where(goal == col, 1.0, 0.0).astype(BF16)
    lsend[...] = jnp.dot(lf[...].astype(BF16), perm, preferred_element_type=F32).astype(BF16)
    enter(others)
    for pj, dev in peers:
        rcopy(psend.at[pj], precv.at[j], p_ss.at[pj], p_rs.at[j], dev).start()
    precv[pl.ds(j, 1)] = psend[pl.ds(j, 1)]
    lhalf = [span(k, terms) for k in PAIRED]
    for k in PAIRED:
        for pj, dev in peers:
            rcopy(lsend.at[lhalf[k]], lrecv.at[j, lhalf[k]], l_ss.at[k, pj], l_rs.at[k, j], dev).start()
    lrecv[pl.ds(j, 1)] = lsend[...][None]

    term = lax.broadcasted_iota(jnp.int32, (terms, terms * BW), 0)
    lane = lax.broadcasted_iota(jnp.int32, (terms, terms * BW), 1)
    spread = jnp.where((lane >> 5) == term, 1.0, 0.0).astype(BF16)
    for q in range(PAIR):
        wv[q * 16 : q * 16 + PAIR] = jnp.dot(op_ref[q], spread, preferred_element_type=F32)
    vb[...] = jnp.zeros_like(vb)

    for pj, dev in peers:
        rcopy(psend.at[pj], precv.at[pj], p_ss.at[pj], p_rs.at[pj], dev).wait_recv()
    square = precv[0, ROW0]
    for s in range(1, NS):
        square = square + precv[s, ROW0]
    square = jnp.where(lax.broadcasted_iota(jnp.int32, ROWVEC, 1) >= 96, square, 0.0)
    square = square + pltpu.roll(square, 64, 1)
    square = square + pltpu.roll(square, 32, 1)
    for s in range(NS):
        for k in QUAD:
            mt[span(k * NS + s, 2)] = precv[s, span(k, 2)]
    flat = mt[...].T
    gbuf[0, pl.ds(i, 1)] = block((flat[span(0, BW)], flat[span(1, BW)]), pack_last(flat[span(2, BW)]))[None]
    start_gather(0, 0)
    start_gather(0, 1)
    zero = jnp.zeros(ROWVEC, F32)
    start_line(0, [zero, zero, zero, square, zero])

    load_right.wait()
    for part in range(terms * BW // 128):
        rows = rt[span(part, 4)].reshape(128, rt.shape[2])
        r2[:, span(part, LANES)] = rows.T

    relay(0, 0)
    relay(0, 1)
    width = 8 * BW
    row = lax.broadcasted_iota(jnp.int32, (width, width), 0)
    col = lax.broadcasted_iota(jnp.int32, (width, width), 1)
    goal = ((row & 15) >> 1) * BW + (row >> 4) * 2 + (row & 1)
    perm = jnp.where(goal == col, 1.0, 0.0).astype(BF16)
    parts = terms // 8
    for part in range(parts):
        for k in PAIRED:
            if part == k * parts // 2:
                for pj, dev in peers:
                    rcopy(
                        lsend.at[lhalf[k]], lrecv.at[pj, lhalf[k]], l_ss.at[k, pj], l_rs.at[k, pj], dev
                    ).wait_recv()
        mine = lrecv[:, span(part, 16), :].reshape(width, left_dim)
        lt[:, span(part, width)] = lax.dot_general(
            mine, perm, (((0,), (0,)), ((), ())), preferred_element_type=F32
        ).astype(BF16)
    finish_gather(0)
    alpha, beta = finish_line(0)
    update(0, zero, zero, beta, 0, ng)

    def first_rows():
        drain_line(0)
        for pj, dev in peers:
            rcopy(psend.at[pj], precv.at[pj], p_ss.at[pj], p_rs.at[pj], dev).wait_send()
            for k in PAIRED:
                rcopy(lsend.at[lhalf[k]], lrecv.at[pj, lhalf[k]], l_ss.at[k, pj], l_rs.at[k, pj], dev).wait_send()
        for grp, lanes in GROUPS:
            for q in range(PAIR):
                vec_ref[0, q, :, lanes] = psi_ref[q, :, lanes] / beta

    product(0, 1, True, first_rows)

    def step(t, beta_prev):
        par = t % 2
        start_plane(par, beta_prev)
        start_out(par)
        drain_scatter()
        start_line(par, finish_plane())
        relay(par, 0)
        relay(par, 1)
        finish_out(t)
        finish_gather(par)
        alpha, beta = finish_line(par)
        update(par, alpha, beta_prev, beta, 0, ng)

        def rest():
            drain_sums(par)
            ab_ref[0, t - 1] = alpha[0, 0]
            ab_ref[1, t - 1] = beta[0, 0]
            own_rows(t, alpha, beta_prev, beta)

        product(par, 1 - par, t < NUM_STEPS - 1, rest)
        return beta

    beta_prev = lax.fori_loop(1, NUM_STEPS, step, zero)
    par = NUM_STEPS % 2
    start_plane(par, beta_prev)
    start_out(par)
    drain_scatter()
    start_line(par, finish_plane())
    finish_out(NUM_STEPS)
    alpha, beta = finish_line(par)
    ab_ref[0, NUM_STEPS - 1] = alpha[0, 0]
    ab_ref[1, NUM_STEPS - 1] = beta[0, 0]
    own_rows(NUM_STEPS, alpha, beta_prev, beta)
    drain_sums(par)


def end_kernel(vec_ref, ab_ref, vec_out, alpha_out, beta_out):
    vec_out[...] = vec_ref[...]
    for k in range(NUM_STEPS):
        alpha_out[k] = ab_ref[0, k]
        beta_out[k] = ab_ref[1, k]


def vmem(n):
    return [pl.BlockSpec(memory_space=pltpu.VMEM)] * n


def dma(*shape):
    return pltpu.SemaphoreType.DMA(shape)


def solution(mesh):
    nz = mesh.shape[ROW] // (NS * NC)
    ng = nz * NC

    def local_run(wave_rows, left_rows, op_pair, right_env):
        terms, rows, left_dim = left_rows.shape
        right_dim = right_env.shape[1]
        count = left_dim * right_dim * PAIR
        nv = NUM_STEPS + 1
        smem = pl.BlockSpec(memory_space=pltpu.SMEM)
        vecs, ab = pl.pallas_call(
            functools.partial(main_kernel, nz, float(count)),
            out_shape=(
                jax.ShapeDtypeStruct((nv, PAIR, rows, right_dim), F32),
                jax.ShapeDtypeStruct((2, NUM_STEPS), F32),
            ),
            in_specs=vmem(3) + [pl.BlockSpec(memory_space=pl.ANY)],
            out_specs=(vmem(1)[0], smem),
            scratch_shapes=[
                pltpu.VMEM((2, ng, BLK, LANES), F32),
                pltpu.VMEM((2, ng, BLK, LANES), F32),
                pltpu.VMEM((PAIR * BW, left_dim), BF16),
                pltpu.VMEM((PAIR * BW, terms * BW), F32),
                pltpu.VMEM((terms * BW, 384), BF16),
                pltpu.VMEM((NS, BLK, LANES), F32),
                pltpu.VMEM((NS, BLK, LANES), F32),
                pltpu.VMEM((NS, *TILE), F32),
                pltpu.VMEM(TILE, F32),
                pltpu.VMEM((2, ng, *ROWVEC), F32),
                pltpu.VMEM((left_dim, terms * BW), BF16),
                pltpu.VMEM((right_dim, terms * BW), BF16),
                pltpu.VMEM((PAIR * 16, terms * BW), F32),
                pltpu.VMEM((terms * rows, left_dim), F32),
                pltpu.VMEM((terms * rows, left_dim), BF16),
                pltpu.VMEM((NS, terms * rows, left_dim), BF16),
                pltpu.VMEM((terms, BW, right_dim), BF16),
                pltpu.VMEM((NS, *TILE), F32),
                pltpu.VMEM((NS, *TILE), F32),
                pltpu.VMEM((NS, *TILE), F32),
                pltpu.VMEM((NS, *TILE), F32),
                pltpu.VMEM((128, 128), F32),
                dma(2, nz), dma(2, nz), dma(4, ng), dma(2, NS), dma(2, NS), dma(NS), dma(NS), dma(ng), dma(2, ng),
                dma(2, NS), dma(2, NS), dma(NS), dma(NS), dma(NS), dma(NS), pltpu.SemaphoreType.DMA,
            ],
            compiler_params=pltpu.CompilerParams(
                collective_id=0, has_side_effects=True, vmem_limit_bytes=56 * 1024 * 1024
            ),
            name="lanczos",
        )(
            wave_rows.transpose(1, 2, 0, 3).reshape(PAIR, rows, right_dim),
            left_rows,
            op_pair.transpose(1, 2, 0),
            right_env,
        )
        short = jax.ShapeDtypeStruct((NUM_STEPS,), F32)
        vecs, alpha, beta = pl.pallas_call(
            end_kernel,
            out_shape=(jax.ShapeDtypeStruct(vecs.shape, F32), short, short),
            in_specs=vmem(1) + [smem],
            out_specs=(vmem(1)[0], smem, smem),
            name="result",
        )(vecs, ab)
        vecs = vecs.reshape(nv, 3, 3, rows, right_dim).transpose(0, 3, 1, 2, 4)
        return vecs, alpha, beta

    return jax.shard_map(
        local_run,
        mesh=mesh,
        in_specs=(P(ROW), P(None, ROW), P(), P()),
        out_specs=(P(None, ROW), P(), P()),
        check_vma=False,
    )
```
